8 devices in a mesh: dp: 2 (over z, y), tp: 4 (over x, core).
Axes of the slice: x: 2, y: 2, z: 1, core: 2. Of those that a mesh axis runs over, the one named last changes fastest.
Arguments:
- hidden: bfloat16 [4, 256, 7168], P('dp', 'tp'), parts along dimension 0
- lengths: int32 [4], P('dp'), parts along dimension 0
- rope_cos: float32 [4, 256, 32], P('dp'), parts along dimension 0
- rope_sin: float32 [4, 256, 32], P('dp'), parts along dimension 0
- cache_lat: bfloat16 [4, 2304, 512], P('dp'), parts along dimension 0
- cache_pe: bfloat16 [4, 2304, 64], P('dp'), parts along dimension 0
- norm_in: float32 [7168], replicated
- w_dq: bfloat16 [7168, 1536], replicated
- norm_q: float32 [1536], replicated
- w_dkv: bfloat16 [7168, 576], replicated
- norm_kv: float32 [512], replicated
- w_uq: bfloat16 [1536, 64, 192], P(None, 'tp')
- w_uk: bfloat16 [512, 64, 128], P(None, 'tp')
- w_uv: bfloat16 [512, 64, 128], P(None, 'tp')
- w_out: bfloat16 [8192, 7168], P('tp')
Outputs:
- output 1: bfloat16 [4, 256, 7168], P('dp', 'tp'), parts along dimension 0
- output 2: bfloat16 [4, 2304, 512], P('dp'), parts along dimension 0
- output 3: bfloat16 [4, 2304, 64], P('dp'), parts along dimension 0
There are 2 independent parts. The reference program is written for one: setup_inputs(seed, part) draws one part's arguments, and reference() takes and returns one part's arrays. A program takes and returns all parts, laid end to end along the dimension named above; an argument that names none is the same for every part.
All inputs are finite; a program needn't handle non-finite values.
Results may differ from the reference program's by a relative error of at most 0.0160033.
Values are sent between devices in bfloat16 or wider.
A program may use at most 1 GiB of HBM per device.

```python
import jax
import jax.numpy as jnp
from jax import lax

MODEL_DIM = 7168
NUM_HEADS = 64
Q_RANK = 1536
KV_RANK = 512
NOPE_DIM = 128
ROPE_DIM = 64
VALUE_DIM = 128
SEQ_COUNT = 2
CHUNK_LEN = 256
PREFIX_MAX = 2048
CACHE_LEN = 2304

HEAD_BLOCK = min(8, NUM_HEADS)


def rms_norm(values, gain_vec):
    inv_rms = lax.rsqrt(jnp.mean(values * values, axis=-1, keepdims=True) + 1e-6)
    return values * inv_rms * gain_vec


def apply_rope(values, cos_tab, sin_tab):
    half_dim = values.shape[-1] // 2
    lower_half = values[..., :half_dim]
    upper_half = values[..., half_dim:]
    return jnp.concatenate([lower_half * cos_tab - upper_half * sin_tab, upper_half * cos_tab + lower_half * sin_tab], axis=-1)


def write_rows(old_rows, new_rows, start_row):
    zero_col = jnp.zeros((), start_row.dtype)
    return lax.dynamic_update_slice(old_rows, new_rows.astype(old_rows.dtype), (start_row, zero_col))


def rope_tables(lengths):
    positions = (lengths[:, None] + jnp.arange(CHUNK_LEN)[None, :]).astype(jnp.float32)
    inv_freq = 10000.0 ** (-2.0 * jnp.arange(ROPE_DIM // 2).astype(jnp.float32) / ROPE_DIM)
    angles = positions[:, :, None] * inv_freq[None, None, :]
    return jnp.cos(angles), jnp.sin(angles)


def normal_draw(key_in, array_shape, std_scale):
    return jax.random.normal(key_in, array_shape, jnp.float32) * std_scale


def setup_inputs(seed: int = 0, part: int = 0) -> dict:
    base_key = jax.random.key(seed)
    part_keys = jax.random.split(jax.random.fold_in(base_key, part), 5)
    weight_keys = jax.random.split(base_key, 9)
    draw_vals = jax.random.randint(part_keys[0], (SEQ_COUNT,), PREFIX_MAX // 4, PREFIX_MAX + 1)
    top_slot = jax.random.randint(part_keys[1], (), 0, SEQ_COUNT)
    lengths = jnp.where(jnp.arange(SEQ_COUNT) == top_slot, PREFIX_MAX, draw_vals).astype(jnp.int32)
    rope_cos, rope_sin = rope_tables(lengths)
    out_scale = (NUM_HEADS * VALUE_DIM) ** -0.5 * (CACHE_LEN / 4.0) ** 0.5
    return {
        "hidden": normal_draw(part_keys[2], (SEQ_COUNT, CHUNK_LEN, MODEL_DIM), 1.0).astype(jnp.bfloat16),
        "lengths": lengths,
        "rope_cos": rope_cos,
        "rope_sin": rope_sin,
        "cache_lat": normal_draw(part_keys[3], (SEQ_COUNT, CACHE_LEN, KV_RANK), 1.0).astype(jnp.bfloat16),
        "cache_pe": normal_draw(part_keys[4], (SEQ_COUNT, CACHE_LEN, ROPE_DIM), 1.0).astype(jnp.bfloat16),
        "norm_in": jax.random.uniform(weight_keys[0], (MODEL_DIM,), jnp.float32, 0.5, 1.5),
        "w_dq": normal_draw(weight_keys[1], (MODEL_DIM, Q_RANK), MODEL_DIM ** -0.5).astype(jnp.bfloat16),
        "norm_q": jax.random.uniform(weight_keys[2], (Q_RANK,), jnp.float32, 0.5, 1.5),
        "w_dkv": normal_draw(weight_keys[3], (MODEL_DIM, KV_RANK + ROPE_DIM), MODEL_DIM ** -0.5).astype(jnp.bfloat16),
        "norm_kv": jax.random.uniform(weight_keys[4], (KV_RANK,), jnp.float32, 0.5, 1.5),
        "w_uq": normal_draw(weight_keys[5], (Q_RANK, NUM_HEADS, NOPE_DIM + ROPE_DIM), Q_RANK ** -0.5).astype(jnp.bfloat16),
        "w_uk": normal_draw(weight_keys[6], (KV_RANK, NUM_HEADS, NOPE_DIM), KV_RANK ** -0.5).astype(jnp.bfloat16),
        "w_uv": normal_draw(weight_keys[7], (KV_RANK, NUM_HEADS, VALUE_DIM), KV_RANK ** -0.5).astype(jnp.bfloat16),
        "w_out": normal_draw(weight_keys[8], (NUM_HEADS * VALUE_DIM, MODEL_DIM), out_scale).astype(jnp.bfloat16),
    }


def reference(hidden, lengths, rope_cos, rope_sin, cache_lat, cache_pe, norm_in, w_dq, norm_q, w_dkv, norm_kv, w_uq, w_uk, w_uv, w_out):
    hidden_f = hidden.astype(jnp.float32)
    normed = rms_norm(hidden_f, norm_in).astype(jnp.bfloat16).reshape(SEQ_COUNT * CHUNK_LEN, MODEL_DIM)
    q_latent = rms_norm(jnp.dot(normed, w_dq, preferred_element_type=jnp.float32), norm_q).astype(jnp.bfloat16)
    kv_proj = jnp.dot(normed, w_dkv, preferred_element_type=jnp.float32).reshape(SEQ_COUNT, CHUNK_LEN, KV_RANK + ROPE_DIM)
    new_lat = rms_norm(kv_proj[..., :KV_RANK], norm_kv).astype(jnp.bfloat16)
    new_pe = apply_rope(kv_proj[..., KV_RANK:], rope_cos, rope_sin).astype(jnp.bfloat16)
    lat_all = jax.vmap(write_rows)(cache_lat, new_lat, lengths)
    pe_all = jax.vmap(write_rows)(cache_pe, new_pe, lengths)
    q_full = jnp.einsum("nc,chd->nhd", q_latent.astype(jnp.float32), w_uq.astype(jnp.float32)).reshape(SEQ_COUNT, CHUNK_LEN, NUM_HEADS, NOPE_DIM + ROPE_DIM)
    q_nope = q_full[..., :NOPE_DIM].astype(jnp.bfloat16)
    q_pe = apply_rope(q_full[..., NOPE_DIM:], rope_cos[:, :, None, :], rope_sin[:, :, None, :]).astype(jnp.bfloat16)
    block_count = NUM_HEADS // HEAD_BLOCK
    uk_blocks = w_uk.reshape(KV_RANK, block_count, HEAD_BLOCK, NOPE_DIM).transpose(1, 0, 2, 3)
    uv_blocks = w_uv.reshape(KV_RANK, block_count, HEAD_BLOCK, VALUE_DIM).transpose(1, 0, 2, 3)
    score_scale = (NOPE_DIM + ROPE_DIM) ** -0.5
    query_pos = jnp.arange(CHUNK_LEN)[:, None]
    key_pos = jnp.arange(CACHE_LEN)[None, :]

    def one_sequence(seq_args):
        qn_seq, qp_seq, lat_seq, pe_seq, length = seq_args
        visible = key_pos < length + query_pos + 1
        qn_blocks = qn_seq.reshape(CHUNK_LEN, block_count, HEAD_BLOCK, NOPE_DIM).transpose(1, 0, 2, 3)
        qp_blocks = qp_seq.reshape(CHUNK_LEN, block_count, HEAD_BLOCK, ROPE_DIM).transpose(1, 0, 2, 3)
        lat_f = lat_seq.astype(jnp.float32)
        pe_f = pe_seq.astype(jnp.float32)

        def one_block(blk_args):
            qn_blk, qp_blk, uk_blk, uv_blk = blk_args
            keys_nope = jnp.einsum("sc,chd->shd", lat_f, uk_blk.astype(jnp.float32)).astype(jnp.bfloat16)
            values_blk = jnp.einsum("sc,chv->shv", lat_f, uv_blk.astype(jnp.float32)).astype(jnp.bfloat16)
            scores = jnp.einsum("thd,shd->hts", qn_blk.astype(jnp.float32), keys_nope.astype(jnp.float32))
            scores = scores + jnp.einsum("thr,sr->hts", qp_blk.astype(jnp.float32), pe_f)
            scores = jnp.where(visible[None], scores * score_scale, -1e30)
            attn_probs = jax.nn.softmax(scores, axis=-1).astype(jnp.bfloat16)
            return jnp.einsum("hts,shv->thv", attn_probs.astype(jnp.float32), values_blk.astype(jnp.float32)).astype(jnp.bfloat16)

        out_blocks = lax.map(one_block, (qn_blocks, qp_blocks, uk_blocks, uv_blocks))
        return out_blocks.transpose(1, 0, 2, 3).reshape(CHUNK_LEN, NUM_HEADS * VALUE_DIM)

    attn_out = lax.map(one_sequence, (q_nope, q_pe, lat_all, pe_all, lengths))
    out_proj = jnp.dot(attn_out.reshape(SEQ_COUNT * CHUNK_LEN, NUM_HEADS * VALUE_DIM), w_out, preferred_element_type=jnp.float32)
    block_out = (out_proj.reshape(SEQ_COUNT, CHUNK_LEN, MODEL_DIM) + hidden_f).astype(jnp.bfloat16)
    return (block_out, lat_all, pe_all)
```

```python
import functools

import jax
import jax.numpy as jnp
from jax import lax
from jax.experimental import pallas as pl
from jax.experimental.pallas import tpu as pltpu
from jax.sharding import PartitionSpec as P

F32 = jnp.float32
BF16 = jnp.bfloat16
EPS = 1e-6
MIB = 1 << 20
LAT_W = 2176
PREFIX = 2048
ROW_BLK = 512
SCALE = 192.0 ** -0.5
LOG2E = 1.4426950408889634
NT = (((1,), (1,)), ((), ()))


def dot(lhs, rhs):
    return jnp.dot(lhs, rhs, preferred_element_type=F32)


def dot_nt(lhs, rhs):
    return lax.dot_general(lhs, rhs, NT, preferred_element_type=F32)


def cost(flops, nbytes):
    return pl.CostEstimate(flops=int(flops), bytes_accessed=int(nbytes), transcendentals=0)


def proj_kernel(x_ref, g1_ref, wq_ref, wkvt_ref, gq_ref, gkv_ref, cos_ref, sin_ref, out_ref, a_s, q_acc, kv_acc):
    step = pl.program_id(0)
    depth = wq_ref.shape[0]

    @pl.when(step == 0)
    def _():
        xf = x_ref[...].astype(F32)
        inv = lax.rsqrt(jnp.mean(xf * xf, axis=-1, keepdims=True) + EPS)
        a_s[...] = (x_ref[...].astype(F32) * inv * g1_ref[...]).astype(BF16)
        q_acc[...] = jnp.zeros_like(q_acc)
        kv_acc[...] = jnp.zeros_like(kv_acc)

    a_blk = a_s[:, pl.ds(pl.multiple_of(step * depth, 128), depth)]
    q_acc[...] += dot(a_blk, wq_ref[...])
    kv_acc[...] += dot_nt(a_blk, wkvt_ref[...])

    @pl.when(step == pl.num_programs(0) - 1)
    def _():
        q = q_acc[...]
        inv = lax.rsqrt(jnp.mean(q * q, axis=-1, keepdims=True) + EPS)
        out_ref[:, :1536] = (q * inv * gq_ref[...]).astype(BF16)
        c = kv_acc[:, :512]
        inv = lax.rsqrt(jnp.mean(c * c, axis=-1, keepdims=True) + EPS)
        out_ref[:, 1536:2048] = (c * inv * gkv_ref[...]).astype(BF16)
        v1 = kv_acc[:, 512:544]
        v2 = kv_acc[:, 544:576]
        cos = cos_ref[...]
        sin = sin_ref[...]
        rot = jnp.concatenate([v1 * cos - v2 * sin, v2 * cos + v1 * sin, jnp.zeros((v1.shape[0], 64), F32)], axis=1)
        out_ref[:, 2048:] = rot.astype(BF16)


def project(x, g1, w_dq, w_dkvt, g_q, g_kv, cos, sin):
    rows, dim = x.shape
    depth = 1024
    const = lambda shape: pl.BlockSpec(shape, lambda k: (0,) * len(shape))
    return pl.pallas_call(
        proj_kernel,
        grid=(dim // depth,),
        in_specs=[
            const((rows, dim)),
            const((1, dim)),
            pl.BlockSpec((depth, 1536), lambda k: (k, 0)),
            pl.BlockSpec((576, depth), lambda k: (0, k)),
            const((1, 1536)),
            const((1, 512)),
            const((rows, 32)),
            const((rows, 32)),
        ],
        out_specs=const((rows, LAT_W)),
        out_shape=jax.ShapeDtypeStruct((rows, LAT_W), BF16),
        scratch_shapes=[pltpu.VMEM((rows, dim), BF16), pltpu.VMEM((rows, 1536), F32), pltpu.VMEM((rows, 576), F32)],
        compiler_params=pltpu.CompilerParams(vmem_limit_bytes=40 * MIB),
        cost_estimate=cost(2 * rows * dim * 2112 * 3, dim * 2112 * 2),
        name="project",
    )(x, g1, w_dq, w_dkvt, g_q, g_kv, cos, sin)


def prep_kernel(wuk_ref, wuv_ref, wk_ref, wvt_ref):
    wk_ref[...] = wuk_ref[...].reshape(wk_ref.shape)
    wvt_ref[...] = wuv_ref[...].reshape(wk_ref.shape).T


def prep_weights(w_uk, w_uv):
    rank, heads, dim = w_uk.shape
    blk = 256
    spec = pl.BlockSpec((blk, heads, dim), lambda i: (i, 0, 0))
    return pl.pallas_call(
        prep_kernel,
        grid=(rank // blk,),
        in_specs=[spec, spec],
        out_specs=[pl.BlockSpec((blk, heads * dim), lambda i: (i, 0)), pl.BlockSpec((heads * dim, blk), lambda i: (0, i))],
        out_shape=[jax.ShapeDtypeStruct((rank, heads * dim), BF16), jax.ShapeDtypeStruct((heads * dim, rank), BF16)],
        compiler_params=pltpu.CompilerParams(vmem_limit_bytes=40 * MIB),
        cost_estimate=cost(4e9, 8 * MIB),
        name="prep",
    )(w_uk, w_uv)


def kv_kernel(seq, len_ref, c_ref, wk_ref, wvt_ref, k_ref, vt_ref):
    @pl.when(pl.program_id(0) * ROW_BLK < len_ref[seq])
    def _():
        c = c_ref[...]
        k_ref[...] = dot(c, wk_ref[...]).astype(BF16)
        vt_ref[...] = dot_nt(wvt_ref[...], c).astype(BF16)

    @pl.when(pl.program_id(0) * ROW_BLK >= len_ref[seq])
    def _():
        vt_ref[...] = jnp.zeros_like(vt_ref)


def kv_up(seq, lengths, cache_lat, wk, wvt):
    rank, width = wk.shape
    blocks = PREFIX // ROW_BLK
    last = lambda r, n: jnp.minimum(r, (n[seq] + ROW_BLK - 1) // ROW_BLK - 1)
    grid_spec = pltpu.PrefetchScalarGridSpec(
        num_scalar_prefetch=1,
        grid=(blocks,),
        in_specs=[
            pl.BlockSpec((None, ROW_BLK, rank), lambda r, n: (seq, last(r, n), 0)),
            pl.BlockSpec((rank, width), lambda r, n: (0, 0)),
            pl.BlockSpec((width, rank), lambda r, n: (0, 0)),
        ],
        out_specs=[
            pl.BlockSpec((ROW_BLK, width), lambda r, n: (last(r, n), 0)),
            pl.BlockSpec((width, ROW_BLK), lambda r, n: (0, r)),
        ],
    )
    return pl.pallas_call(
        functools.partial(kv_kernel, seq),
        grid_spec=grid_spec,
        out_shape=[jax.ShapeDtypeStruct((PREFIX, width), BF16), jax.ShapeDtypeStruct((width, PREFIX), BF16)],
        compiler_params=pltpu.CompilerParams(vmem_limit_bytes=48 * MIB),
        cost_estimate=cost(4 * PREFIX * rank * width * 2, 20 * MIB),
        name="kv_up",
    )(lengths, cache_lat, wk, wvt)


def attn_kernel(seq, len_ref, place_ref, b0, b1, b2, b3, cos_ref, sin_ref, pet_ref, wuqt_ref, wk_ref, wvt_ref, k_ref, vt_ref,
                o_ref, cnew_ref, knewt_ref, cqt, cn, cnt, kn, pe):
    step = pl.program_id(0)

    @pl.when(step == 0)
    def _():
        for k, blk in enumerate((b0, b1, b2, b3)):
            rows = pl.ds(pl.multiple_of(place_ref[k], 64), 64)
            cnew_ref[rows, :] = blk[:, 1536:2048]
            cn[rows, :] = blk[:, 1536:2048]
            kn[rows, :] = blk[:, 2048:]
            cqt[rows, :] = blk[:, :1536]
        cnt[...] = cn[...].T
        knewt_ref[...] = kn[...].T[:64]
        pe[...] = pet_ref[:, :PREFIX].T

    @pl.when(len_ref[seq] >= 0)
    def _():
        length = len_ref[seq]
        cos = cos_ref[...]
        sin = sin_ref[...]
        row_old = lax.broadcasted_iota(jnp.int32, (PREFIX, 256), 0)
        row_new = lax.broadcasted_iota(jnp.int32, (256, 256), 0)
        col_new = lax.broadcasted_iota(jnp.int32, (256, 256), 1)
        c2 = SCALE * LOG2E
        for h in range(2):
            d = slice(128 * h, 128 * h + 128)
            q = dot_nt(wuqt_ref[h], cqt[...])
            v1 = q[128:160]
            v2 = q[160:192]
            qt = jnp.concatenate([q[:128], v1 * cos - v2 * sin, v2 * cos + v1 * sin], axis=0).astype(BF16)
            k_new = dot(cn[...], wk_ref[:, d]).astype(BF16)
            vt_new = dot(wvt_ref[d, :], cnt[...]).astype(BF16)
            s_old = dot(jnp.concatenate([k_ref[:, d], pe[...]], axis=1), qt)
            s_new = dot(jnp.concatenate([k_new, kn[:, :64]], axis=1), qt)
            s_old = jnp.where(row_old < length, s_old * c2, -1e30)
            s_new = jnp.where(row_new <= col_new, s_new * c2, -1e30)
            m = jnp.maximum(jnp.max(s_old, axis=0, keepdims=True), jnp.max(s_new, axis=0, keepdims=True))
            p_old = jnp.exp2(s_old - m)
            p_new = jnp.exp2(s_new - m)
            inv = 1.0 / (jnp.sum(p_old, axis=0, keepdims=True) + jnp.sum(p_new, axis=0, keepdims=True))
            p_old = jnp.where(row_old < length, p_old * inv, 0.0).astype(BF16)
            ot = dot(vt_ref[d, :], p_old) + dot(vt_new, (p_new * inv).astype(BF16))
            o_ref[:, d] = ot.T.astype(BF16)


def attend(seq, lengths, place, blocks, cos_t, sin_t, pe_t, w_uqt, wk, wvt, k_old, vt_old):
    lat_spec = pl.BlockSpec((None, 64, LAT_W), lambda h, n, p: (seq, 0, 0))
    grid_spec = pltpu.PrefetchScalarGridSpec(
        num_scalar_prefetch=2,
        grid=(8,),
        in_specs=[lat_spec] * 4 + [
            pl.BlockSpec((None, 32, 256), lambda h, n, p: (seq, 0, 0)),
            pl.BlockSpec((None, 32, 256), lambda h, n, p: (seq, 0, 0)),
            pl.BlockSpec((None, 64, 2304), lambda h, n, p: (seq, 0, 0)),
            pl.BlockSpec((2, 192, 1536), lambda h, n, p: (h, 0, 0)),
            pl.BlockSpec((512, 256), lambda h, n, p: (0, h)),
            pl.BlockSpec((256, 512), lambda h, n, p: (h, 0)),
            pl.BlockSpec((PREFIX, 256), lambda h, n, p: (0, h)),
            pl.BlockSpec((256, PREFIX), lambda h, n, p: (h, 0)),
        ],
        out_specs=[
            pl.BlockSpec((256, 256), lambda h, n, p: (0, h)),
            pl.BlockSpec((256, 512), lambda h, n, p: (0, 0)),
            pl.BlockSpec((64, 256), lambda h, n, p: (0, 0)),
        ],
        scratch_shapes=[
            pltpu.VMEM((256, 1536), BF16),
            pltpu.VMEM((256, 512), BF16),
            pltpu.VMEM((512, 256), BF16),
            pltpu.VMEM((256, 128), BF16),
            pltpu.VMEM((PREFIX, 64), BF16),
        ],
    )
    return pl.pallas_call(
        functools.partial(attn_kernel, seq),
        grid_spec=grid_spec,
        out_shape=[
            jax.ShapeDtypeStruct((256, 2048), BF16),
            jax.ShapeDtypeStruct((256, 512), BF16),
            jax.ShapeDtypeStruct((64, 256), BF16),
        ],
        compiler_params=pltpu.CompilerParams(vmem_limit_bytes=56 * MIB),
        cost_estimate=cost(16 * 256 * 2304 * 1024 * 2, 32 * MIB),
        name="attend",
    )(lengths, place, *blocks, cos_t, sin_t, pe_t, w_uqt, wk, wvt, k_old, vt_old)


def out_kernel(rows_ref, o_ref, w_ref, mine_ref, sib_ref):
    r0 = pl.multiple_of(rows_ref[0], 64)
    r1 = pl.multiple_of(rows_ref[1], 64)
    lhs = jnp.concatenate([o_ref[pl.ds(r0, 64), :], o_ref[pl.ds(r1, 64), :]], axis=0)
    y = dot(lhs, w_ref[...])
    mine_ref[...] = y[:64]
    sib_ref[...] = y[64:]


def out_proj(rows, o, w_out, half):
    cols = 512
    steps = 7
    grid_spec = pltpu.PrefetchScalarGridSpec(
        num_scalar_prefetch=1,
        grid=(steps,),
        in_specs=[
            pl.BlockSpec((256, 2048), lambda n, r: (0, 0)),
            pl.BlockSpec((2048, cols), lambda n, r: (0, n + half * steps)),
        ],
        out_specs=[pl.BlockSpec((64, cols), lambda n, r: (0, n))] * 2,
    )
    shape = jax.ShapeDtypeStruct((64, cols * steps), F32)
    return pl.pallas_call(
        out_kernel,
        grid_spec=grid_spec,
        out_shape=[shape, shape],
        compiler_params=pltpu.CompilerParams(vmem_limit_bytes=40 * MIB),
        cost_estimate=cost(2 * 128 * 2048 * 3584 * 3, 16 * MIB),
        name="out_proj",
    )(rows, o, w_out)


def solution(mesh):
    def local_step(hidden, lengths, rope_cos, rope_sin, cache_lat, cache_pe, norm_in, w_dq, norm_q, w_dkv, norm_kv, w_uq, w_uk, w_uv, w_out):
        me = lax.axis_index("tp")
        swap = lambda v, bit: lax.ppermute(v, "tp", [(i, i ^ bit) for i in range(4)])
        cos_t = jnp.swapaxes(rope_cos, 1, 2)
        sin_t = jnp.swapaxes(rope_sin, 1, 2)
        pe_t = jnp.swapaxes(cache_pe, 1, 2)
        w_uqt = jnp.transpose(w_uq, (1, 2, 0))
        own = lambda tab: lax.dynamic_slice_in_dim(tab, me * 64, 64, axis=1).reshape(128, 32)
        lat = project(hidden.reshape(128, -1), norm_in[None], w_dq, w_dkv.T, norm_q[None], norm_kv[None], own(rope_cos), own(rope_sin))
        lat = lat.reshape(2, 64, LAT_W)
        far = swap(lat, 2)
        near = swap(lat, 1)
        wk, wvt = prep_weights(w_uk, w_uv)
        k_old, vt_old = kv_up(0, lengths, cache_lat, wk, wvt)
        diag = swap(far, 1)
        place = jnp.stack([me, me ^ 1, me ^ 2, me ^ 3]).astype(jnp.int32) * 64
        rows_far = place[2:]
        rows_own = place[:2]
        blocks = (lat, near, far, diag)
        o0, c0, p0 = attend(0, lengths, place, blocks, cos_t, sin_t, pe_t, w_uqt, wk, wvt, k_old, vt_old)

        def far_sum(o):
            got = []
            for half in range(2):
                mine, sib = out_proj(rows_far, o, w_out, half)
                got.append(swap(mine + swap(sib, 1), 2))
            return got

        got0 = far_sum(o0)
        lengths_b, _ = lax.optimization_barrier((lengths, o0[0, 0]))
        k_old, vt_old = kv_up(1, lengths_b, cache_lat, wk, wvt)
        o1, c1, p1 = attend(1, lengths, place, blocks, cos_t, sin_t, pe_t, w_uqt, wk, wvt, k_old, vt_old)
        got1 = far_sum(o1)

        def own_sum(o, x, got):
            parts = []
            for half in range(2):
                mine, sib = out_proj(rows_own, o, w_out, half)
                cols = slice(half * 3584, half * 3584 + 3584)
                parts.append((x[:, cols].astype(F32) + (mine + swap(sib, 1) + got[half])).astype(BF16))
            return jnp.concatenate(parts, axis=1)

        y = jnp.stack([own_sum(o0, hidden[0], got0), own_sum(o1, hidden[1], got1)])
        zero = jnp.zeros((), jnp.int32)
        lat_new = cache_lat
        pe_new = pe_t
        for b, (c, p) in enumerate(((c0, p0), (c1, p1))):
            lat_new = lax.dynamic_update_slice(lat_new, c[None], (jnp.int32(b), lengths[b], zero))
            pe_new = lax.dynamic_update_slice(pe_new, p[None], (jnp.int32(b), zero, lengths[b]))
        return y, lat_new, jnp.swapaxes(pe_new, 1, 2)

    spec_tok = P("dp", "tp", None)
    spec_len = P("dp")
    spec_seq = P("dp", None, None)
    spec_vec = P(None)
    spec_mat = P(None, None)
    spec_head = P(None, "tp", None)
    spec_rows = P("tp", None)
    in_specs = (spec_tok, spec_len, spec_seq, spec_seq, spec_seq, spec_seq, spec_vec, spec_mat, spec_vec, spec_mat, spec_vec, spec_head, spec_head, spec_head, spec_rows)
    return jax.shard_map(local_step, mesh=mesh, in_specs=in_specs, out_specs=(spec_tok, spec_seq, spec_seq), check_vma=False)
```

```python
import functools

import jax
import jax.numpy as jnp
from jax import lax
from jax.experimental import pallas as pl
from jax.experimental.pallas import tpu as pltpu
from jax.sharding import PartitionSpec as P

F32 = jnp.float32
BF16 = jnp.bfloat16
EPS = 1e-6
MIB = 1 << 20
LAT_W = 2176
PREFIX = 2048
ROW_BLK = 512
CHUNK = 512
CHUNKS = 7168 // CHUNK
C2 = 192.0 ** -0.5 * 1.4426950408889634
NEG = -1e30
NT = (((1,), (1,)), ((), ()))


def dot(lhs, rhs):
    return jnp.dot(lhs, rhs, preferred_element_type=F32)


def dot_nt(lhs, rhs):
    return lax.dot_general(lhs, rhs, NT, preferred_element_type=F32)


def cost(flops, nbytes):
    return pl.CostEstimate(flops=int(flops), bytes_accessed=int(nbytes), transcendentals=0)


def proj_kernel(x_ref, g1_ref, wq_ref, wkvt_ref, gq_ref, gkv_ref, cos_ref, sin_ref, out_ref, a_s, q_acc, kv_acc):
    step = pl.program_id(0)
    depth = wq_ref.shape[0]

    @pl.when(step == 0)
    def _():
        xf = x_ref[...].astype(F32)
        inv = lax.rsqrt(jnp.mean(xf * xf, axis=-1, keepdims=True) + EPS)
        a_s[...] = (x_ref[...].astype(F32) * inv * g1_ref[...]).astype(BF16)
        q_acc[...] = jnp.zeros_like(q_acc)
        kv_acc[...] = jnp.zeros_like(kv_acc)

    a_blk = a_s[:, pl.ds(pl.multiple_of(step * depth, 128), depth)]
    q_acc[...] += dot(a_blk, wq_ref[...])
    kv_acc[...] += dot_nt(a_blk, wkvt_ref[...])

    @pl.when(step == pl.num_programs(0) - 1)
    def _():
        q = q_acc[...]
        inv = lax.rsqrt(jnp.mean(q * q, axis=-1, keepdims=True) + EPS)
        out_ref[:, :1536] = (q * inv * gq_ref[...]).astype(BF16)
        c = kv_acc[:, :512]
        inv = lax.rsqrt(jnp.mean(c * c, axis=-1, keepdims=True) + EPS)
        out_ref[:, 1536:2048] = (c * inv * gkv_ref[...]).astype(BF16)
        v1 = kv_acc[:, 512:544]
        v2 = kv_acc[:, 544:576]
        cos = cos_ref[...]
        sin = sin_ref[...]
        rot = jnp.concatenate([v1 * cos - v2 * sin, v2 * cos + v1 * sin, jnp.zeros((v1.shape[0], 64), F32)], axis=1)
        out_ref[:, 2048:] = rot.astype(BF16)


def project(x, g1, w_dq, w_dkvt, g_q, g_kv, cos, sin):
    rows, dim = x.shape
    depth = 1024
    const = lambda shape: pl.BlockSpec(shape, lambda k: (0,) * len(shape))
    return pl.pallas_call(
        proj_kernel,
        grid=(dim // depth,),
        in_specs=[
            const((rows, dim)),
            const((1, dim)),
            pl.BlockSpec((depth, 1536), lambda k: (k, 0)),
            pl.BlockSpec((576, depth), lambda k: (0, k)),
            const((1, 1536)),
            const((1, 512)),
            const((rows, 32)),
            const((rows, 32)),
        ],
        out_specs=const((rows, LAT_W)),
        out_shape=jax.ShapeDtypeStruct((rows, LAT_W), BF16),
        scratch_shapes=[pltpu.VMEM((rows, dim), BF16), pltpu.VMEM((rows, 1536), F32), pltpu.VMEM((rows, 576), F32)],
        compiler_params=pltpu.CompilerParams(vmem_limit_bytes=60 * MIB),
        cost_estimate=cost(2 * rows * dim * 2112 * 3, dim * 2112 * 2),
        name="project",
    )(x, g1, w_dq, w_dkvt, g_q, g_kv, cos, sin)


def prep_kernel(wuk_ref, wuv_ref, wk_ref, wvt_ref):
    wk_ref[...] = wuk_ref[...].reshape(wk_ref.shape)
    wvt_ref[...] = wuv_ref[...].reshape(wk_ref.shape).T


def prep_weights(w_uk, w_uv):
    rank, heads, dim = w_uk.shape
    blk = 256
    spec = pl.BlockSpec((blk, heads, dim), lambda i: (i, 0, 0))
    return pl.pallas_call(
        prep_kernel,
        grid=(rank // blk,),
        in_specs=[spec, spec],
        out_specs=[pl.BlockSpec((blk, heads * dim), lambda i: (i, 0)), pl.BlockSpec((heads * dim, blk), lambda i: (0, i))],
        out_shape=[jax.ShapeDtypeStruct((rank, heads * dim), BF16), jax.ShapeDtypeStruct((heads * dim, rank), BF16)],
        compiler_params=pltpu.CompilerParams(vmem_limit_bytes=40 * MIB),
        cost_estimate=cost(4e9, 8 * MIB),
        name="prep",
    )(w_uk, w_uv)


def cache_kernel(len_ref, c_ref, pe_ref, cn_ref, kn_ref, co_ref, po_ref):
    length = len_ref[pl.program_id(0)]
    base = pl.program_id(1) * 768
    row = lax.broadcasted_iota(jnp.int32, (768, 256), 0) + (base - length)
    hot = (row == lax.broadcasted_iota(jnp.int32, (768, 256), 1)).astype(F32).astype(BF16)
    row_c = lax.broadcasted_iota(jnp.int32, (768, 512), 0) + (base - length)
    new_c = dot(hot, cn_ref[...])
    co_ref[...] = jnp.where((row_c >= 0) & (row_c < 256), new_c, c_ref[...].astype(F32)).astype(BF16)
    col = lax.broadcasted_iota(jnp.int32, (64, 768), 1) + (base - length)
    new_p = dot_nt(kn_ref[...], hot)
    po_ref[...] = jnp.where((col >= 0) & (col < 256), new_p, pe_ref[...].astype(F32)).astype(BF16)


def update_caches(lengths, cache_lat, pe_t, c_new, k_newt):
    lat_spec = pl.BlockSpec((None, 768, 512), lambda b, r, n: (b, r, 0))
    pe_spec = pl.BlockSpec((None, 64, 768), lambda b, r, n: (b, 0, r))
    grid_spec = pltpu.PrefetchScalarGridSpec(
        num_scalar_prefetch=1,
        grid=(2, 3),
        in_specs=[
            lat_spec,
            pe_spec,
            pl.BlockSpec((None, 256, 512), lambda b, r, n: (b, 0, 0)),
            pl.BlockSpec((None, 64, 256), lambda b, r, n: (b, 0, 0)),
        ],
        out_specs=[lat_spec, pe_spec],
    )
    return pl.pallas_call(
        cache_kernel,
        grid_spec=grid_spec,
        out_shape=[jax.ShapeDtypeStruct(cache_lat.shape, BF16), jax.ShapeDtypeStruct(pe_t.shape, BF16)],
        compiler_params=pltpu.CompilerParams(vmem_limit_bytes=40 * MIB),
        cost_estimate=cost(4e9, 12 * MIB),
        name="caches",
    )(lengths, cache_lat, pe_t, c_new, k_newt)


def at(start, size, unit):
    return pl.ds(pl.multiple_of(start, unit), size)


def main_kernel(len_ref, lat, cos, sin, pet, c_hbm, wk_hbm, wvt_hbm, wq_hbm, wo_hbm, x_hbm,
                y_hbm, cnew_hbm, knewt_hbm,
                latb, cqa, cqt, cn, cnt, kn, knt, pe, mask, aug, cbuf, kb, vtb, wkb, wvtb, wqb, sb, mb, vb, ob, lhsb, wob,
                stage_d, xbuf, stage_x, rbuf, ownb, xres, ybuf,
                lat_send, lat_recv, c_sem, wk_sem, wvt_sem, wq_sem, wo_sem, x_sem, out_sem, y_sem,
                d_send, d_recv, i_send, i_recv, free_sem):
    me = lax.axis_index("tp")
    chip = me // 2
    core = me % 2
    sib = 2 * chip + (1 - core)
    far = 2 * (1 - chip) + core
    diag = 2 * (1 - chip) + (1 - core)

    def remote(src, dst, send, recv, peer):
        return pltpu.make_async_remote_copy(src_ref=src, dst_ref=dst, send_sem=send, recv_sem=recv, device_id={"tp": peer}, device_id_type=pl.DeviceIdType.MESH)

    def fetch_c(b):
        return pltpu.make_async_copy(c_hbm.at[b, pl.ds(0, PREFIX), :], cbuf, c_sem)

    def fetch_wq(h):
        return pltpu.make_async_copy(wq_hbm.at[h], wqb.at[h % 4], wq_sem.at[h % 4])

    def fetch_wo(g, n):
        return pltpu.make_async_copy(wo_hbm.at[:, at(n * CHUNK, CHUNK, CHUNK)], wob.at[g % 3], wo_sem.at[g % 3])

    copy_wk = pltpu.make_async_copy(wk_hbm, wkb, wk_sem)
    copy_wvt = pltpu.make_async_copy(wvt_hbm, wvtb, wvt_sem)
    copy_x = pltpu.make_async_copy(x_hbm, xres, x_sem)
    fetch_c(0).start()
    copy_wk.start()
    copy_wvt.start()

    barrier = pltpu.get_barrier_semaphore()
    for peer in (sib, far):
        pl.semaphore_signal(barrier, inc=1, device_id={"tp": peer}, device_id_type=pl.DeviceIdType.MESH)
    pl.semaphore_wait(barrier, 2)

    to_far = [remote(lat.at[b], latb.at[b, 1], lat_send.at[b, 1], lat_recv.at[b, 1], far) for b in range(2)]
    to_sib = [remote(lat.at[b], latb.at[b, 0], lat_send.at[b, 0], lat_recv.at[b, 0], sib) for b in range(2)]
    onward = [remote(latb.at[b, 1], latb.at[b, 2], lat_send.at[b, 2], lat_recv.at[b, 2], sib) for b in range(2)]
    to_far[0].start()
    to_sib[0].start()
    to_far[1].start()
    to_sib[1].start()
    for h in range(3):
        fetch_wq(h).start()
    for n in range(3):
        fetch_wo(n, n).start()
    copy_x.start()

    aug[...] = jnp.where(lax.broadcasted_iota(jnp.int32, (64, 256), 0) == 0, 1.0, 0.0).astype(BF16)
    causal = lax.broadcasted_iota(jnp.int32, (256, 256), 0) <= lax.broadcasted_iota(jnp.int32, (256, 256), 1)

    def keys_values(b, forward):
        length = len_ref[b]
        row = lax.broadcasted_iota(jnp.int32, (PREFIX, 128), 0)
        lane = lax.broadcasted_iota(jnp.int32, (PREFIX, 128), 1)
        old = row < length
        mask[...] = jnp.where(old, 1.0, 0.0).astype(BF16)
        rot = pet[b, :, :PREFIX].astype(F32).T
        rot = jnp.concatenate([rot, jnp.zeros_like(rot)], axis=1)
        pe[...] = jnp.where(old, rot, jnp.where(lane == 64, NEG, 0.0)).astype(BF16)
        fetch_c(b).wait()

        def block(r, carry):
            if forward is not None:
                @pl.when(r == 3)
                def _():
                    forward()
            rows = at(r * ROW_BLK, ROW_BLK, ROW_BLK)
            m = mask[rows, :]
            c = cbuf[rows, :] * jnp.concatenate([m, m, m, m], axis=1)
            kb[rows, :] = dot(c, wkb[...]).astype(BF16)
            vtb[:, rows] = dot_nt(wvtb[...], c).astype(BF16)
            return carry

        lax.fori_loop(0, PREFIX // ROW_BLK, block, 0)

    def assemble(b):
        for src, owner in ((lat.at[b], me), (latb.at[b, 0], sib), (latb.at[b, 1], far), (latb.at[b, 2], diag)):
            rows = at(owner * 64, 64, 64)
            cqa[rows, :] = src[:, :1536]
            cn[b, rows, :] = src[:, 1536:2048]
            kn[rows, :] = src[:, 2048:]
        cqt[...] = cqa[...].T
        cnt[...] = cn[b].T
        knt[b] = kn[...].T[:64]

    def attend(b):
        def head(h, carry):
            d = at(h * 128, 128, 128)
            fetch_wq(h).wait()
            cos_b = cos[b]
            sin_b = sin[b]
            q = dot(wqb[h % 4], cqt[...])
            v1 = q[128:160]
            v2 = q[160:192]
            qt = jnp.concatenate([q[:128].astype(BF16), (v1 * cos_b - v2 * sin_b).astype(BF16), (v2 * cos_b + v1 * sin_b).astype(BF16), aug[...]], axis=0)
            k_new = dot(cn[b], wkb[:, d]).astype(BF16)
            vb[...] = dot(wvtb[d, :], cnt[...]).astype(BF16)
            s = dot(jnp.concatenate([k_new, kn[...]], axis=1), qt)
            s = jnp.where(causal, s, NEG)
            sb[PREFIX:, :] = s
            m8 = jnp.max(s.reshape(32, 8, 256), axis=0)
            for c in range(PREFIX // 256):
                rows = slice(c * 256, c * 256 + 256)
                s = dot(jnp.concatenate([kb[rows, d], pe[rows, :]], axis=1), qt)
                sb[rows, :] = s
                m8 = jnp.maximum(m8, jnp.max(s.reshape(32, 8, 256), axis=0))
            mb[...] = m8

            @pl.when(h + 3 < 16)
            def _():
                fetch_wq(h + 3).start()

            m = jnp.max(mb[...], axis=0, keepdims=True) * C2
            l8 = jnp.zeros((8, 256), F32)
            for c in range(9):
                rows = slice(c * 256, c * 256 + 256)
                p = jnp.exp2(sb[rows, :] * C2 - m)
                sb[rows, :] = p
                l8 = l8 + jnp.sum(p.reshape(32, 8, 256), axis=0)
            inv = 1.0 / jnp.sum(l8, axis=0, keepdims=True)
            acc = None
            for c in range(9):
                rows = slice(c * 256, c * 256 + 256)
                p = (sb[rows, :] * inv).astype(BF16)
                t = dot(vtb[d, rows] if c < 8 else vb[...], p)
                acc = t if acc is None else acc + t
            ob[b, :, d] = acc.T.astype(BF16)
            return carry

        lax.fori_loop(0, 16, head, 0)

    def to_sibling(b, n):
        return remote(stage_d.at[n % 4], xbuf.at[b, n], d_send.at[n % 4], d_recv.at[b, n], sib)

    def over_link(b, n):
        return remote(stage_x.at[b, n], rbuf.at[b, n], i_send.at[b, n], i_recv.at[b, n], far)

    def put_y(b, n):
        return pltpu.make_async_copy(ybuf.at[b, n], y_hbm.at[b, :, at(n * CHUNK, CHUNK, CHUNK)], y_sem.at[b, n])

    def product(b, unit, first, second, n):
        g = unit * CHUNKS + n
        fetch_wo(g, n).wait()
        y = dot(lhsb[...], wob[g % 3])
        return y, g

    def next_wo(g):
        @pl.when(g + 3 < 4 * CHUNKS)
        def _():
            fetch_wo(g + 3, (g + 3) % CHUNKS).start()

    def load_lhs(b, first, second):
        lhsb[:64, :] = ob[b, at(first * 64, 64, 64), :]
        lhsb[64:, :] = ob[b, at(second * 64, 64, 64), :]

    def far_unit(b, unit):
        load_lhs(b, far, diag)

        def pass_on(n):
            to_sibling(b, n).wait_recv()
            stage_x[b, n] = stage_x[b, n] + xbuf[b, n]
            over_link(b, n).start()

        def chunk(n, carry):
            y, g = product(b, unit, far, diag, n)

            @pl.when(n >= 4)
            def _():
                to_sibling(b, n - 4).wait_send()

            stage_d[n % 4] = y[64:]
            stage_x[b, n] = y[:64]
            to_sibling(b, n).start()
            next_wo(g)

            @pl.when(n >= 1)
            def _():
                pass_on(n - 1)

            return carry

        lax.fori_loop(0, CHUNKS, chunk, 0)
        pass_on(CHUNKS - 1)
        for n in range(CHUNKS - 4, CHUNKS):
            to_sibling(b, n).wait_send()

    def own_unit(b, unit):
        load_lhs(b, me, sib)

        def finish(n):
            to_sibling(b, n).wait_recv()
            over_link(b, n).wait_recv()
            total = ownb[n % 2] + xbuf[b, n] + rbuf[b, n]
            ybuf[b, n] = (xres[b, :, at(n * CHUNK, CHUNK, CHUNK)].astype(F32) + total).astype(BF16)
            put_y(b, n).start()

        def chunk(n, carry):
            y, g = product(b, unit, me, sib, n)

            @pl.when(n >= 4)
            def _():
                to_sibling(b, n - 4).wait_send()

            stage_d[n % 4] = y[64:]
            ownb[n % 2] = y[:64]
            to_sibling(b, n).start()
            next_wo(g)

            @pl.when(n >= 1)
            def _():
                finish(n - 1)

            return carry

        lax.fori_loop(0, CHUNKS, chunk, 0)
        finish(CHUNKS - 1)
        for n in range(CHUNKS - 4, CHUNKS):
            to_sibling(b, n).wait_send()

    def forward_first():
        to_far[0].wait_recv()
        onward[0].start()

    copy_wk.wait()
    copy_wvt.wait()
    keys_values(0, forward_first)
    fetch_c(1).start()
    to_sib[0].wait_recv()
    onward[0].wait_recv()
    assemble(0)
    attend(0)
    for h in range(3):
        fetch_wq(h).start()
    to_far[1].wait_recv()
    onward[1].start()
    far_unit(0, 0)
    keys_values(1, None)
    to_sib[1].wait_recv()
    onward[1].wait_recv()
    assemble(1)
    put_c = pltpu.make_async_copy(cn, cnew_hbm, out_sem.at[0])
    put_k = pltpu.make_async_copy(knt, knewt_hbm, out_sem.at[1])
    put_c.start()
    put_k.start()
    attend(1)
    far_unit(1, 1)
    pl.semaphore_signal(free_sem, inc=1, device_id={"tp": sib}, device_id_type=pl.DeviceIdType.MESH)
    copy_x.wait()
    pl.semaphore_wait(free_sem, 1)
    own_unit(0, 2)
    own_unit(1, 3)
    for b in range(2):
        to_far[b].wait_send()
        to_sib[b].wait_send()
        onward[b].wait_send()

        def drain(n, carry):
            over_link(b, n).wait_send()
            put_y(b, n).wait()
            return carry

        lax.fori_loop(0, CHUNKS, drain, 0)
    put_c.wait()
    put_k.wait()


def main_call(lengths, lat, cos_t, sin_t, pe_t, cache_lat, wk, wvt, w_uqt, w_out, hidden):
    vmem = pl.BlockSpec(memory_space=pltpu.VMEM)
    hbm = pl.BlockSpec(memory_space=pl.ANY)
    dma = pltpu.SemaphoreType.DMA
    return pl.pallas_call(
        main_kernel,
        in_specs=[pl.BlockSpec(memory_space=pltpu.SMEM)] + [vmem] * 4 + [hbm] * 6,
        out_specs=[hbm] * 3,
        out_shape=[
            jax.ShapeDtypeStruct((2, 64, 7168), BF16),
            jax.ShapeDtypeStruct((2, 256, 512), BF16),
            jax.ShapeDtypeStruct((2, 64, 256), BF16),
        ],
        scratch_shapes=[
            pltpu.VMEM((2, 3, 64, LAT_W), BF16),
            pltpu.VMEM((256, 1536), BF16),
            pltpu.VMEM((1536, 256), BF16),
            pltpu.VMEM((2, 256, 512), BF16),
            pltpu.VMEM((512, 256), BF16),
            pltpu.VMEM((256, 128), BF16),
            pltpu.VMEM((2, 64, 256), BF16),
            pltpu.VMEM((PREFIX, 128), BF16),
            pltpu.VMEM((PREFIX, 128), BF16),
            pltpu.VMEM((64, 256), BF16),
            pltpu.VMEM((PREFIX, 512), BF16),
            pltpu.VMEM((PREFIX, 2048), BF16),
            pltpu.VMEM((2048, PREFIX), BF16),
            pltpu.VMEM((512, 2048), BF16),
            pltpu.VMEM((2048, 512), BF16),
            pltpu.VMEM((4, 192, 1536), BF16),
            pltpu.VMEM((PREFIX + 256, 256), F32),
            pltpu.VMEM((8, 256), F32),
            pltpu.VMEM((128, 256), BF16),
            pltpu.VMEM((2, 256, 2048), BF16),
            pltpu.VMEM((128, 2048), BF16),
            pltpu.VMEM((3, 2048, CHUNK), BF16),
            pltpu.VMEM((4, 64, CHUNK), F32),
            pltpu.VMEM((2, CHUNKS, 64, CHUNK), F32),
            pltpu.VMEM((2, CHUNKS, 64, CHUNK), F32),
            pltpu.VMEM((2, CHUNKS, 64, CHUNK), F32),
            pltpu.VMEM((2, 64, CHUNK), F32),
            pltpu.VMEM((2, 64, 7168), BF16),
            pltpu.VMEM((2, CHUNKS, 64, CHUNK), BF16),
            dma((2, 3)),
            dma((2, 3)),
            dma,
            dma,
            dma,
            dma((4,)),
            dma((3,)),
            dma,
            dma((2,)),
            dma((2, CHUNKS)),
            dma((4,)),
            dma((2, CHUNKS)),
            dma((2, CHUNKS)),
            dma((2, CHUNKS)),
            pltpu.SemaphoreType.REGULAR,
        ],
        compiler_params=pltpu.CompilerParams(vmem_limit_bytes=67043328, collective_id=0, has_side_effects=True),
        cost_estimate=cost(1e11, 200 * MIB),
        name="main",
    )(lengths, lat, cos_t, sin_t, pe_t, cache_lat, wk, wvt, w_uqt, w_out, hidden)


def solution(mesh):
    def local_step(hidden, lengths, rope_cos, rope_sin, cache_lat, cache_pe, norm_in, w_dq, norm_q, w_dkv, norm_kv, w_uq, w_uk, w_uv, w_out):
        me = lax.axis_index("tp")
        cos_t = jnp.swapaxes(rope_cos, 1, 2)
        sin_t = jnp.swapaxes(rope_sin, 1, 2)
        pe_t = jnp.swapaxes(cache_pe, 1, 2)
        w_uqt = jnp.transpose(w_uq, (1, 2, 0))
        own = lambda tab: lax.dynamic_slice_in_dim(tab, me * 64, 64, axis=1).reshape(128, 32)
        wk, wvt = prep_weights(w_uk, w_uv)
        lat = project(hidden.reshape(128, -1), norm_in[None], w_dq, w_dkv.T, norm_q[None], norm_kv[None], own(rope_cos), own(rope_sin))
        y, c_new, k_newt = main_call(lengths, lat.reshape(2, 64, LAT_W), cos_t, sin_t, pe_t, cache_lat, wk, wvt, w_uqt, w_out, hidden)
        lat_new, pe_new = update_caches(lengths, cache_lat, pe_t, c_new, k_newt)
        return y, lat_new, jnp.swapaxes(pe_new, 1, 2)

    spec_tok = P("dp", "tp", None)
    spec_len = P("dp")
    spec_seq = P("dp", None, None)
    spec_vec = P(None)
    spec_mat = P(None, None)
    spec_head = P(None, "tp", None)
    spec_rows = P("tp", None)
    in_specs = (spec_tok, spec_len, spec_seq, spec_seq, spec_seq, spec_seq, spec_vec, spec_mat, spec_vec, spec_mat, spec_vec, spec_head, spec_head, spec_head, spec_rows)
    return jax.shard_map(local_step, mesh=mesh, in_specs=in_specs, out_specs=(spec_tok, spec_seq, spec_seq), check_vma=False)
```

```python
import functools

import jax
import jax.numpy as jnp
from jax import lax
from jax.experimental import pallas as pl
from jax.experimental.pallas import tpu as pltpu
from jax.sharding import PartitionSpec as P

F32 = jnp.float32
BF16 = jnp.bfloat16
EPS = 1e-6
MIB = 1 << 20
VMEM_ALL = 67043328
MESH = pl.DeviceIdType.MESH
LAT_W = 2176
PREFIX = 2048
ROW_BLK = 512
CHUNK = 512
DEPTH = 512
CHUNKS = 7168 // CHUNK
C2 = 192.0 ** -0.5 * 1.4426950408889634
NEG = -1e30
LOC = 64
HD = 128
NEW = 256
QR = 1536
WID = 2048
CB = 768
KVR = 512
NT = (((1,), (1,)), ((), ()))


def dot(lhs, rhs):
    return jnp.dot(lhs, rhs, preferred_element_type=F32)


def dot_nt(lhs, rhs):
    return lax.dot_general(lhs, rhs, NT, preferred_element_type=F32)


def cost(flops, nbytes):
    return pl.CostEstimate(flops=int(flops), bytes_accessed=int(nbytes), transcendentals=0)


def cache_kernel(len_ref, c_hbm, pe_hbm, cn_hbm, kn_hbm, co_hbm, po_hbm, rows, cols, cn, kn, in_sem, out_sem, side_sem):
    blocks = rows.shape[1] // NEW
    span = lambda r: pl.ds(r * NEW, NEW)
    lat_in = lambda b, r: pltpu.make_async_copy(c_hbm.at[b, span(r)], rows.at[b, span(r)], in_sem.at[b, r])
    lat_out = lambda b, r: pltpu.make_async_copy(rows.at[b, span(r)], co_hbm.at[b, span(r)], out_sem.at[b, r])
    pe_in = lambda b: pltpu.make_async_copy(pe_hbm.at[b], cols.at[b], in_sem.at[b, blocks])
    pe_out = lambda b: pltpu.make_async_copy(cols.at[b], po_hbm.at[b], out_sem.at[b, blocks])
    new_in = [pltpu.make_async_copy(cn_hbm, cn, side_sem.at[0]), pltpu.make_async_copy(kn_hbm, kn, side_sem.at[1])]
    places = [(b, r) for b in range(2) for r in range(blocks)]
    for copy in new_in:
        copy.start()
    for b, r in places:
        lat_in(b, r).start()
    for b in range(2):
        pe_in(b).start()
    for copy in new_in:
        copy.wait()
    for b, r in places:
        shift = r * NEW - len_ref[b]
        lat_in(b, r).wait()

        @pl.when((shift < NEW) & (shift > -NEW))
        def _():
            row = lax.broadcasted_iota(jnp.int32, (NEW, NEW), 0) + shift
            hot = (row == lax.broadcasted_iota(jnp.int32, (NEW, NEW), 1)).astype(F32).astype(BF16)
            row = lax.broadcasted_iota(jnp.int32, (NEW, KVR), 0) + shift
            old = rows[b, span(r), :].astype(F32)
            rows[b, span(r), :] = jnp.where((row >= 0) & (row < NEW), dot(hot, cn[b]), old).astype(BF16)

        lat_out(b, r).start()
    for b in range(2):
        pe_in(b).wait()
        for r in range(blocks):
            shift = r * NEW - len_ref[b]

            @pl.when((shift < NEW) & (shift > -NEW))
            def _():
                row = lax.broadcasted_iota(jnp.int32, (NEW, NEW), 0) + shift
                hot = (row == lax.broadcasted_iota(jnp.int32, (NEW, NEW), 1)).astype(F32).astype(BF16)
                col = lax.broadcasted_iota(jnp.int32, (LOC, NEW), 1) + shift
                old = cols[b, :, span(r)].astype(F32)
                cols[b, :, span(r)] = jnp.where((col >= 0) & (col < NEW), dot_nt(kn[b], hot), old).astype(BF16)

        pe_out(b).start()
    for b, r in places:
        lat_out(b, r).wait()
    for b in range(2):
        pe_out(b).wait()


def update_caches(lengths, cache_lat, pe_t, c_new, k_newt):
    hbm = pl.BlockSpec(memory_space=pl.ANY)
    sems = pltpu.SemaphoreType.DMA((2, cache_lat.shape[1] // NEW + 1))
    return pl.pallas_call(
        cache_kernel,
        in_specs=[pl.BlockSpec(memory_space=pltpu.SMEM)] + [hbm] * 4,
        out_specs=[hbm] * 2,
        out_shape=[jax.ShapeDtypeStruct(v.shape, BF16) for v in (cache_lat, pe_t)],
        scratch_shapes=[*[pltpu.VMEM(v.shape, BF16) for v in (cache_lat, pe_t, c_new, k_newt)], sems, sems, pltpu.SemaphoreType.DMA((2,))],
        compiler_params=pltpu.CompilerParams(vmem_limit_bytes=VMEM_ALL),
        cost_estimate=cost(4e9, 12 * MIB),
        name="caches",
    )(lengths, cache_lat, pe_t, c_new, k_newt)


def at(start, size):
    return pl.ds(pl.multiple_of(start, size), size)


def main_kernel(len_ref, cos, sin, pet, g1, gq, gkv, x_hbm, wdq_hbm, wdkvt_hbm, c_hbm, wuk_hbm, wuv_hbm, wq_hbm, wo_hbm,
                y_hbm, cnew_hbm, knewt_hbm,
                lat, qa, kva, latb, cqt, cn, kn, knt, pe, mask, cbuf, kb, vtb, wkb, wvtb, wqb, q_lo, q_hi, sb, mb, ob, lhsb, wob,
                stage_d, xbuf, stage_x, rbuf, ownb, ybuf,
                lat_send, lat_recv, dq_sem, dkv_sem, c_sem, wk_sem, wvt_sem, wq_sem, wo_sem, x_sem, out_sem, y_sem,
                d_send, d_recv, i_send, i_recv, free_sem):
    me = lax.axis_index("tp")
    chip = me // 2
    core = me % 2
    sib = 2 * chip + (1 - core)
    far = 2 * (1 - chip) + core
    diag = 2 * (1 - chip) + (1 - core)

    def remote(src, dst, send, recv, peer):
        return pltpu.make_async_remote_copy(src_ref=src, dst_ref=dst, send_sem=send, recv_sem=recv, device_id={"tp": peer}, device_id_type=MESH)

    def fetch_rows(src, dst, sem, parts):
        size = dst.shape[0] // parts
        for k in range(parts):
            rows = pl.ds(k * size, size)
            pltpu.make_async_copy(src.at[rows], dst.at[rows], sem).start()

    def c_refs(b):
        return c_hbm.at[b, pl.ds(0, PREFIX), :], cbuf, c_sem

    def wq_refs(h):
        return wq_hbm.at[pl.ds(2 * h, 2)], wqb.at[h % 3], wq_sem.at[h % 3]

    def fetch_wq(i):
        src, dst, sem = wq_refs(i)
        for k in range(2):
            fetch_rows(src.at[k], dst.at[k], sem, 2)

    def wo_refs(g, n):
        return wo_hbm.at[:, at(n * CHUNK, CHUNK)], wob.at[g % 3], wo_sem.at[g % 3]

    def dq_refs(n):
        return wdq_hbm.at[at(n * DEPTH, DEPTH), :], kb.at[at((n % 4) * DEPTH, DEPTH), pl.ds(0, QR)], dq_sem.at[n % 4]

    def dkv_refs(n):
        return wdkvt_hbm.at[:, at(n * DEPTH, DEPTH)], vtb.at[pl.ds(0, 576), at((n % 4) * DEPTH, DEPTH)], dkv_sem.at[n % 4]

    def uk_copy(j):
        return pltpu.make_async_copy(wuk_hbm.at[pl.ds(WID * j, WID), :], kb.at[pl.ds(0, WID), pl.ds(QR + HD * j, HD)], wk_sem.at[j])

    def uv_copy(j):
        return pltpu.make_async_copy(wuv_hbm.at[pl.ds(1024 * j, 1024), :], vtb.at[pl.ds(1024, 1024), pl.ds(HD * j, HD)], wvt_sem.at[j])

    def piece(j):
        return at(HD * (j + 8), HD), pl.ds(1024, 1024)

    def x_copy(j):
        return pltpu.make_async_copy(x_hbm.at[:, at(1024 * j, 1024)], vtb.at[piece(j)], x_sem.at[j])

    def x_again(j):
        return pltpu.make_async_copy(x_hbm.at[:, at(1024 * j, 1024)], kb.at[at(HD * j, HD), pl.ds(0, 1024)], x_sem.at[j])

    for j in range(7):
        x_copy(j).start()
    for n in range(3):
        fetch_rows(*dq_refs(n), 2)
        fetch_rows(*dkv_refs(n), 2)

    barrier = pltpu.get_barrier_semaphore()
    for peer in (sib, far):
        pl.semaphore_signal(barrier, inc=1, device_id={"tp": peer}, device_id_type=MESH)

    aug = jnp.where(lax.broadcasted_iota(jnp.int32, (LOC, NEW), 0) == 0, 1.0, 0.0).astype(BF16)
    causal = lax.broadcasted_iota(jnp.int32, (NEW, NEW), 0) <= lax.broadcasted_iota(jnp.int32, (NEW, NEW), 1)
    for b in range(2):
        sb[pl.ds(NEW * b, NEW), :32] = cos[b].T
        sb[pl.ds(KVR + NEW * b, NEW), :32] = sin[b].T
    qa[...] = jnp.zeros_like(qa)
    kva[...] = jnp.zeros_like(kva)
    for j in range(7):
        x_copy(j).wait()

    def squares(j, acc):
        v = vtb[piece(j)].astype(F32)
        v = v * v
        return acc + sum(v[:, HD * k:HD * k + HD] for k in range(8))

    total = lax.fori_loop(0, 7, squares, jnp.zeros((HD, HD), F32))
    inv_x = lax.rsqrt(jnp.sum(total, axis=-1, keepdims=True) / 7168.0 + EPS)

    def scaled(j, carry):
        vtb[piece(j)] = (vtb[piece(j)].astype(F32) * inv_x * g1[:, at(1024 * j, 1024)]).astype(BF16)
        return carry

    lax.fori_loop(0, 7, scaled, 0)

    def project(n, carry):
        @pl.when(n + 3 < CHUNKS)
        def _():
            fetch_rows(*dq_refs(n + 3), 2)
            fetch_rows(*dkv_refs(n + 3), 2)

        pltpu.make_async_copy(*dq_refs(n)).wait()
        pltpu.make_async_copy(*dkv_refs(n)).wait()

        @pl.when(n == 7)
        def _():
            for j in range(4):
                uk_copy(j).start()
            for j in range(8):
                uv_copy(j).start()

        a = vtb[at(HD * (n // 2 + 8), HD), at(1024 + DEPTH * (n % 2), DEPTH)]
        slot = at((n % 4) * DEPTH, DEPTH)
        qa[...] += dot(a, kb[slot, :QR])
        kva[...] += dot_nt(a, vtb[:576, slot])
        return carry

    lax.fori_loop(0, CHUNKS, project, 0)
    fetch_rows(*c_refs(0), 4)
    for b in range(2):
        rows = slice(LOC * b, LOC * b + LOC)
        q = qa[rows, :]
        inv_q = lax.rsqrt(jnp.mean(q * q, axis=-1, keepdims=True) + EPS)
        lat[b, :, :QR] = (q * inv_q * gq[...]).astype(BF16)
        c = kva[rows, :KVR]
        inv_c = lax.rsqrt(jnp.mean(c * c, axis=-1, keepdims=True) + EPS)
        lat[b, :, QR:WID] = (c * inv_c * gkv[...]).astype(BF16)
        v1 = kva[rows, KVR:544]
        v2 = kva[rows, 544:576]
        own_cos = sb[at(NEW * b + me * LOC, LOC), :32]
        own_sin = sb[at(KVR + NEW * b + me * LOC, LOC), :32]
        rot = jnp.concatenate([v1 * own_cos - v2 * own_sin, v2 * own_cos + v1 * own_sin, jnp.zeros((LOC, LOC), F32)], axis=1)
        lat[b, :, WID:] = rot.astype(BF16)

    pl.semaphore_wait(barrier, 2)
    to_far = [remote(lat.at[b], latb.at[b, 1], lat_send.at[b, 1], lat_recv.at[b, 1], far) for b in range(2)]
    to_sib = [remote(lat.at[b], latb.at[b, 0], lat_send.at[b, 0], lat_recv.at[b, 0], sib) for b in range(2)]
    onward = [remote(latb.at[b, 1], latb.at[b, 2], lat_send.at[b, 2], lat_recv.at[b, 2], sib) for b in range(2)]
    to_far[0].start()
    to_sib[0].start()
    to_far[1].start()
    to_sib[1].start()
    fetch_wq(0)
    fetch_wq(1)
    for n in range(3):
        fetch_rows(*wo_refs(n, n), 4)
    for j in range(4):
        uk_copy(j).wait()
        wkb[HD * j:HD * j + HD, :] = kb[:WID, QR + HD * j:1664 + HD * j].reshape(HD, WID)
    for j in range(8):
        uv_copy(j).wait()
    for j in range(4):
        pair = [vtb[1024:, HD * k:HD * k + HD].reshape(LOC, WID) for k in (2 * j, 2 * j + 1)]
        wvtb[:, HD * j:HD * j + HD] = jnp.concatenate(pair, axis=0).T

    def keys_values(b, forward):
        length = len_ref[b]
        row = lax.broadcasted_iota(jnp.int32, (PREFIX, HD), 0)
        lane = lax.broadcasted_iota(jnp.int32, (PREFIX, HD), 1)
        old = row < length
        mask[...] = jnp.where(old, 1.0, 0.0).astype(BF16)
        rot = pet[b, :, :PREFIX].astype(F32).T
        rot = jnp.concatenate([rot, jnp.zeros_like(rot)], axis=1)
        pe[:PREFIX, :] = jnp.where(old, rot, jnp.where(lane == LOC, NEG, 0.0)).astype(BF16)
        pltpu.make_async_copy(*c_refs(b)).wait()

        def block(r, carry):
            if forward is not None:
                @pl.when(r == 3)
                def _():
                    forward()
            rows = at(r * ROW_BLK, ROW_BLK)
            m = mask[rows, :]
            c = cbuf[rows, :] * jnp.concatenate([m, m, m, m], axis=1)
            kb[rows, :] = dot(c, wkb[...]).astype(BF16)
            vtb[:, rows] = dot_nt(wvtb[...], c).astype(BF16)
            return carry

        lax.fori_loop(0, PREFIX // ROW_BLK, block, 0)

    def assemble(b):
        for src, owner in ((lat.at[b], me), (latb.at[b, 0], sib), (latb.at[b, 1], far), (latb.at[b, 2], diag)):
            rows = at(owner * LOC, LOC)
            lhsb[rows, :QR] = src[:, :QR]
            cn[b, rows, :] = src[:, QR:WID]
            kn[rows, :] = src[:, WID:]
        cqt[...] = lhsb[:, :QR].T
        knt[b] = kn[...].T[:LOC]
        pe[PREFIX:, :] = kn[...]
        kb[PREFIX:, :] = dot(cn[b], wkb[...]).astype(BF16)
        vtb[:, PREFIX:] = dot_nt(wvtb[...], cn[b]).astype(BF16)

    def queries(b):
        def pair(i, carry):
            @pl.when(i + 2 < 8)
            def _():
                fetch_wq(i + 2)

            pltpu.make_async_copy(*wq_refs(i)).wait()
            cos_b = cos[b]
            sin_b = sin[b]
            for k in range(2):
                q = dot(wqb[i % 3, k], cqt[...])
                v1 = q[HD:160]
                v2 = q[160:]
                qt = jnp.concatenate([q[:HD].astype(BF16), (v1 * cos_b - v2 * sin_b).astype(BF16), (v2 * cos_b + v1 * sin_b).astype(BF16), aug], axis=0)
                q_lo[2 * i + k] = qt
            return carry

        lax.fori_loop(0, 8, pair, 0)
        q_hi[0] = q_lo[0]

    def attend(b):
        halves = ((q_lo, range(5)), (q_hi, range(5, 9)))
        order = [(side, c) for c in range(5) for side, (_, blocks) in enumerate(halves) if c < len(blocks)]

        def head(h, carry):
            d = at(h * HD, HD)
            best = [jnp.full((8, NEW), NEG, F32)] * 2
            for side, k in order:
                c = halves[side][1][k]
                rows = pl.ds(c * NEW, NEW)
                s = dot(jnp.concatenate([kb[rows, d], pe[rows, :]], axis=1), halves[side][0][(h, h % 2)[side]])
                if c == 8:
                    s = jnp.where(causal, s, NEG)
                sb[rows, :] = s
                best[side] = jnp.maximum(best[side], jnp.max(s.reshape(32, 8, NEW), axis=0))
            mb[...] = jnp.maximum(*best)

            @pl.when(h >= 0)
            def _():
                m = jnp.max(mb[...], axis=0, keepdims=True) * C2
                l8 = jnp.zeros((8, NEW), F32)
                for c in range(9):
                    rows = pl.ds(c * NEW, NEW)
                    p = jnp.exp2(sb[rows, :] * C2 - m)
                    sb[rows, :] = p
                    l8 = l8 + jnp.sum(p.reshape(32, 8, NEW), axis=0)
                inv = 1.0 / jnp.sum(l8, axis=0, keepdims=True)
                acc = [jnp.zeros((HD, NEW), F32)] * 2
                for side, k in order:
                    rows = pl.ds(halves[side][1][k] * NEW, NEW)
                    acc[side] = acc[side] + dot(vtb[d, rows], (sb[rows, :] * inv).astype(BF16))
                ob[b, :, d] = (acc[0] + acc[1]).T.astype(BF16)
                q_hi[(h + 1) % 2] = q_lo[jnp.minimum(h + 1, 15)]

            return carry

        lax.fori_loop(0, 16, head, 0)

    def to_sibling(b, n):
        return remote(stage_d.at[n % 4, 0], xbuf.at[b, n], d_send.at[n % 4], d_recv.at[b, n], sib)

    def over_link(b, n):
        return remote(stage_x.at[b, n], rbuf.at[b, n], i_send.at[b, n], i_recv.at[b, n], far)

    def put_y(n):
        return pltpu.make_async_copy(ybuf.at[n % 4], y_hbm.at[:, at(n * CHUNK, CHUNK)], y_sem.at[n % 4])

    def product(rows, g, n):
        pltpu.make_async_copy(*wo_refs(g, n)).wait()
        return dot(lhsb[:rows, :], wob[g % 3])

    def next_wo(g):
        @pl.when(g + 3 < 3 * CHUNKS)
        def _():
            fetch_rows(*wo_refs(g + 3, (g + 3) % CHUNKS), 4)

    def load_lhs(k, b, owner):
        lhsb[LOC * k:LOC * k + LOC, :] = ob[b, at(owner * LOC, LOC), :]

    def far_unit(b, unit):
        load_lhs(0, b, far)
        load_lhs(1, b, diag)

        def pass_on(n):
            to_sibling(b, n).wait_recv()
            stage_x[b, n] = stage_x[b, n] + xbuf[b, n]
            over_link(b, n).start()

        def chunk(n, carry):
            g = unit * CHUNKS + n
            y = product(HD, g, n)

            @pl.when(n >= 4)
            def _():
                to_sibling(b, n - 4).wait_send()

            stage_d[n % 4, 0] = y[LOC:]
            stage_x[b, n] = y[:LOC]
            to_sibling(b, n).start()
            next_wo(g)

            @pl.when(n >= 1)
            def _():
                pass_on(n - 1)

            return carry

        lax.fori_loop(0, CHUNKS, chunk, 0)
        pass_on(CHUNKS - 1)
        for n in range(CHUNKS - 4, CHUNKS):
            to_sibling(b, n).wait_send()

    def own_unit(unit):
        for b in range(2):
            load_lhs(b, b, me)
            load_lhs(2 + b, b, sib)

        def both(n):
            return remote(stage_d.at[n % 4], xbuf.at[:, n], d_send.at[n % 4], d_recv.at[0, n], sib)

        def finish(n):
            both(n).wait_recv()

            @pl.when(n >= 4)
            def _():
                put_y(n - 4).wait()

            for b in range(2):
                over_link(b, n).wait_recv()
                total = ownb[n % 2, b] + xbuf[b, n] + rbuf[b, n]
                x = kb[at(HD * (n // 2) + LOC * b, LOC), at(CHUNK * (n % 2), CHUNK)]
                ybuf[n % 4, pl.ds(LOC * b, LOC), :] = (x.astype(F32) + total).astype(BF16)
            put_y(n).start()

        def chunk(n, carry):
            g = unit * CHUNKS + n
            y = product(NEW, g, n)

            @pl.when(n >= 4)
            def _():
                both(n - 4).wait_send()

            for b in range(2):
                ownb[n % 2, b] = y[LOC * b:LOC * b + LOC]
                stage_d[n % 4, b] = y[HD + LOC * b:192 + LOC * b]
            both(n).start()
            next_wo(g)

            @pl.when(n >= 1)
            def _():
                finish(n - 1)

            return carry

        lax.fori_loop(0, CHUNKS, chunk, 0)
        finish(CHUNKS - 1)
        for n in range(CHUNKS - 4, CHUNKS):
            both(n).wait_send()
            put_y(n).wait()

    def forward_first():
        to_far[0].wait_recv()
        onward[0].start()

    keys_values(0, forward_first)
    fetch_rows(*c_refs(1), 4)
    to_sib[0].wait_recv()
    onward[0].wait_recv()
    assemble(0)
    queries(0)
    fetch_wq(0)
    fetch_wq(1)
    attend(0)
    to_far[1].wait_recv()
    onward[1].start()
    far_unit(0, 0)
    keys_values(1, None)
    to_sib[1].wait_recv()
    onward[1].wait_recv()
    assemble(1)
    put_c = pltpu.make_async_copy(cn, cnew_hbm, out_sem.at[0])
    put_k = pltpu.make_async_copy(knt, knewt_hbm, out_sem.at[1])
    put_c.start()
    put_k.start()
    queries(1)
    attend(1)
    for j in range(7):
        x_again(j).start()
    far_unit(1, 1)
    pl.semaphore_signal(free_sem, inc=1, device_id={"tp": sib}, device_id_type=MESH)
    pl.semaphore_wait(free_sem, 1)
    for j in range(7):
        x_again(j).wait()
    own_unit(2)
    for b in range(2):
        to_far[b].wait_send()
        to_sib[b].wait_send()
        onward[b].wait_send()

        def drain(n, carry):
            over_link(b, n).wait_send()
            return carry

        lax.fori_loop(0, CHUNKS, drain, 0)
    put_c.wait()
    put_k.wait()


def main_call(lengths, *arrays):
    vmem = pl.BlockSpec(memory_space=pltpu.VMEM)
    hbm = pl.BlockSpec(memory_space=pl.ANY)
    dma = pltpu.SemaphoreType.DMA
    return pl.pallas_call(
        main_kernel,
        in_specs=[pl.BlockSpec(memory_space=pltpu.SMEM)] + [vmem] * 6 + [hbm] * 8,
        out_specs=[hbm] * 3,
        out_shape=[
            jax.ShapeDtypeStruct((HD, 7168), BF16),
            jax.ShapeDtypeStruct((2, NEW, KVR), BF16),
            jax.ShapeDtypeStruct((2, LOC, NEW), BF16),
        ],
        scratch_shapes=[
            pltpu.VMEM((2, LOC, LAT_W), BF16),
            pltpu.VMEM((HD, QR), F32),
            pltpu.VMEM((HD, 576), F32),
            pltpu.VMEM((2, 3, LOC, LAT_W), BF16),
            pltpu.VMEM((QR, NEW), BF16),
            pltpu.VMEM((2, NEW, KVR), BF16),
            pltpu.VMEM((NEW, HD), BF16),
            pltpu.VMEM((2, LOC, NEW), BF16),
            pltpu.VMEM((PREFIX + NEW, HD), BF16),
            pltpu.VMEM((PREFIX, HD), BF16),
            pltpu.VMEM((PREFIX, KVR), BF16),
            pltpu.VMEM((PREFIX + NEW, WID), BF16),
            pltpu.VMEM((WID, PREFIX + NEW), BF16),
            pltpu.VMEM((KVR, WID), BF16),
            pltpu.VMEM((WID, KVR), BF16),
            pltpu.VMEM((3, 2, 192, QR), BF16),
            pltpu.VMEM((16, NEW, NEW), BF16),
            pltpu.VMEM((2, NEW, NEW), BF16),
            pltpu.VMEM((PREFIX + NEW, NEW), F32),
            pltpu.VMEM((8, NEW), F32),
            pltpu.VMEM((2, NEW, WID), BF16),
            pltpu.VMEM((NEW, WID), BF16),
            pltpu.VMEM((3, WID, CHUNK), BF16),
            pltpu.VMEM((4, 2, LOC, CHUNK), F32),
            *[pltpu.VMEM((2, CHUNKS, LOC, CHUNK), F32)] * 3,
            pltpu.VMEM((2, 2, LOC, CHUNK), F32),
            pltpu.VMEM((4, HD, CHUNK), BF16),
            *[dma((2, 3))] * 2,
            *[dma((4,))] * 2,
            dma,
            dma((4,)),
            dma((8,)),
            dma((4,)),
            dma((3,)),
            dma((7,)),
            dma((2,)),
            dma((4,)),
            dma((4,)),
            *[dma((2, CHUNKS))] * 3,
            pltpu.SemaphoreType.REGULAR,
        ],
        compiler_params=pltpu.CompilerParams(vmem_limit_bytes=VMEM_ALL, collective_id=0, has_side_effects=True),
        cost_estimate=cost(1e11, 200 * MIB),
        name="main",
    )(lengths, *arrays)


def solution(mesh):
    def local_step(hidden, lengths, rope_cos, rope_sin, cache_lat, cache_pe, norm_in, w_dq, norm_q, w_dkv, norm_kv, w_uq, w_uk, w_uv, w_out):
        pe_t = jnp.swapaxes(cache_pe, 1, 2)
        y, c_new, k_newt = main_call(
            lengths,
            jnp.swapaxes(rope_cos, 1, 2),
            jnp.swapaxes(rope_sin, 1, 2),
            pe_t,
            norm_in[None],
            norm_q[None],
            norm_kv[None],
            hidden.reshape(HD, 7168),
            w_dq,
            w_dkv.T,
            cache_lat,
            w_uk.reshape(8192, HD),
            w_uv.reshape(8192, HD),
            jnp.transpose(w_uq, (1, 2, 0)),
            w_out,
        )
        lat_new, pe_new = update_caches(lengths, cache_lat, pe_t, c_new, k_newt)
        return y.reshape(hidden.shape), lat_new, jnp.swapaxes(pe_new, 1, 2)

    spec_tok = P("dp", "tp", None)
    spec_len = P("dp")
    spec_seq = P("dp", None, None)
    spec_vec = P(None)
    spec_mat = P(None, None)
    spec_head = P(None, "tp", None)
    spec_rows = P("tp", None)
    in_specs = (spec_tok, spec_len, spec_seq, spec_seq, spec_seq, spec_seq, spec_vec, spec_mat, spec_vec, spec_mat, spec_vec, spec_head, spec_head, spec_head, spec_rows)
    return jax.shard_map(local_step, mesh=mesh, in_specs=in_specs, out_specs=(spec_tok, spec_seq, spec_seq), check_vma=False)
```

```python
import functools

import jax
import jax.numpy as jnp
from jax import lax
from jax.experimental import pallas as pl
from jax.experimental.pallas import tpu as pltpu
from jax.sharding import PartitionSpec as P

F32 = jnp.float32
BF16 = jnp.bfloat16
EPS = 1e-6
MIB = 1 << 20
VMEM_ALL = 67043328
MESH = pl.DeviceIdType.MESH
LAT_W = 2176
PREFIX = 2048
ROW_BLK = 512
CHUNK = 512
DEPTH = 512
CHUNKS = 7168 // CHUNK
C2 = 192.0 ** -0.5 * 1.4426950408889634
NEG = -1e30
LOC = 64
HD = 128
NEW = 256
QR = 1536
WID = 2048
CB = 768
KVR = 512
NT = (((1,), (1,)), ((), ()))


def dot(lhs, rhs):
    return jnp.dot(lhs, rhs, preferred_element_type=F32)


def dot_nt(lhs, rhs):
    return lax.dot_general(lhs, rhs, NT, preferred_element_type=F32)


def cost(flops, nbytes):
    return pl.CostEstimate(flops=int(flops), bytes_accessed=int(nbytes), transcendentals=0)


def cache_kernel(len_ref, y_hbm, c_hbm, pe_hbm, cn_hbm, kn_hbm, yo_hbm, co_hbm, po_hbm, y, rows, cols, cn, kn, in_sem, out_sem, side_sem, y_sem):
    blocks = rows.shape[1] // NEW
    span = lambda r: pl.ds(r * NEW, NEW)
    lat_in = lambda b, r: pltpu.make_async_copy(c_hbm.at[b, span(r)], rows.at[b, span(r)], in_sem.at[b, r])
    lat_out = lambda b, r: pltpu.make_async_copy(rows.at[b, span(r)], co_hbm.at[b, span(r)], out_sem.at[b, r])
    pe_in = lambda b: pltpu.make_async_copy(pe_hbm.at[b], cols.at[b], in_sem.at[b, blocks])
    pe_out = lambda b: pltpu.make_async_copy(cols.at[b], po_hbm.at[b], out_sem.at[b, blocks])
    new_in = [pltpu.make_async_copy(cn_hbm, cn, side_sem.at[0]), pltpu.make_async_copy(kn_hbm, kn, side_sem.at[1])]
    part = lambda k: pl.ds(32 * k, 32)
    y_in = [pltpu.make_async_copy(y_hbm.at[part(k)], y.at[part(k)], y_sem.at[k]) for k in range(4)]
    y_out = [pltpu.make_async_copy(y.at[part(k)], yo_hbm.at[part(k)], y_sem.at[4 + k]) for k in range(4)]
    places = [(b, r) for b in range(2) for r in range(blocks)]
    for copy in new_in:
        copy.start()
    for b, r in places:
        lat_in(b, r).start()
    for b in range(2):
        pe_in(b).start()
    for copy in y_in:
        copy.start()
    for copy in new_in:
        copy.wait()
    for b, r in places:
        shift = r * NEW - len_ref[b]
        lat_in(b, r).wait()

        @pl.when((shift < NEW) & (shift > -NEW))
        def _():
            row = lax.broadcasted_iota(jnp.int32, (NEW, NEW), 0) + shift
            hot = (row == lax.broadcasted_iota(jnp.int32, (NEW, NEW), 1)).astype(F32).astype(BF16)
            row = lax.broadcasted_iota(jnp.int32, (NEW, KVR), 0) + shift
            old = rows[b, span(r), :].astype(F32)
            rows[b, span(r), :] = jnp.where((row >= 0) & (row < NEW), dot(hot, cn[b]), old).astype(BF16)

        lat_out(b, r).start()
    for b in range(2):
        pe_in(b).wait()
        for r in range(blocks):
            shift = r * NEW - len_ref[b]

            @pl.when((shift < NEW) & (shift > -NEW))
            def _():
                row = lax.broadcasted_iota(jnp.int32, (NEW, NEW), 0) + shift
                hot = (row == lax.broadcasted_iota(jnp.int32, (NEW, NEW), 1)).astype(F32).astype(BF16)
                col = lax.broadcasted_iota(jnp.int32, (LOC, NEW), 1) + shift
                old = cols[b, :, span(r)].astype(F32)
                cols[b, :, span(r)] = jnp.where((col >= 0) & (col < NEW), dot_nt(kn[b], hot), old).astype(BF16)

        pe_out(b).start()
    for k in range(4):
        y_in[k].wait()
        y_out[k].start()
    for b, r in places:
        lat_out(b, r).wait()
    for copy in y_out:
        copy.wait()
    for b in range(2):
        pe_out(b).wait()


def update_caches(lengths, y, cache_lat, pe_t, c_new, k_newt):
    hbm = pl.BlockSpec(memory_space=pl.ANY)
    sems = pltpu.SemaphoreType.DMA((2, cache_lat.shape[1] // NEW + 1))
    return pl.pallas_call(
        cache_kernel,
        in_specs=[pl.BlockSpec(memory_space=pltpu.SMEM)] + [hbm] * 5,
        out_specs=[hbm] * 3,
        out_shape=[jax.ShapeDtypeStruct(v.shape, BF16) for v in (y, cache_lat, pe_t)],
        scratch_shapes=[*[pltpu.VMEM(v.shape, BF16) for v in (y, cache_lat, pe_t, c_new, k_newt)], sems, sems, pltpu.SemaphoreType.DMA((2,)), pltpu.SemaphoreType.DMA((8,))],
        compiler_params=pltpu.CompilerParams(vmem_limit_bytes=VMEM_ALL),
        cost_estimate=cost(4e9, 12 * MIB),
        name="caches",
    )(lengths, y, cache_lat, pe_t, c_new, k_newt)


def at(start, size):
    return pl.ds(pl.multiple_of(start, size), size)


def main_kernel(len_ref, cos, sin, pet, g1, gq, gkv, x_hbm, wdq_hbm, wdkvt_hbm, c_hbm, wuk_hbm, wuv_hbm, wq_hbm, wo_hbm,
                y_hbm, cnew_hbm, knewt_hbm,
                lat, qa, kva, latb, cqt, cn, kn, knt, pe, mask, cbuf, kb, vtb, wkb, wvtb, wqb, q_lo, q_hi, sb, mb, ob, lhsb, wob,
                stage_d, xbuf, stage_x, rbuf, ownb, ybuf,
                lat_send, lat_recv, dq_sem, dkv_sem, c_sem, wk_sem, wvt_sem, wq_sem, wo_sem, x_sem, out_sem, y_sem,
                d_send, d_recv, i_send, i_recv, free_sem):
    me = lax.axis_index("tp")
    chip = me // 2
    core = me % 2
    sib = 2 * chip + (1 - core)
    far = 2 * (1 - chip) + core
    diag = 2 * (1 - chip) + (1 - core)

    def remote(src, dst, send, recv, peer):
        return pltpu.make_async_remote_copy(src_ref=src, dst_ref=dst, send_sem=send, recv_sem=recv, device_id={"tp": peer}, device_id_type=MESH)

    def fetch_rows(src, dst, sem, parts):
        size = dst.shape[0] // parts
        for k in range(parts):
            rows = pl.ds(k * size, size)
            pltpu.make_async_copy(src.at[rows], dst.at[rows], sem).start()

    def c_refs(b):
        return c_hbm.at[b, pl.ds(0, PREFIX), :], cbuf, c_sem

    def wq_refs(h):
        return wq_hbm.at[pl.ds(2 * h, 2)], wqb.at[h % 3], wq_sem.at[h % 3]

    def fetch_wq(i):
        src, dst, sem = wq_refs(i)
        for k in range(2):
            fetch_rows(src.at[k], dst.at[k], sem, 2)

    def wo_refs(g, n):
        return wo_hbm.at[:, at(n * CHUNK, CHUNK)], wob.at[g % 3], wo_sem.at[g % 3]

    def dq_refs(n):
        return wdq_hbm.at[at(n * DEPTH, DEPTH), :], kb.at[at((n % 4) * DEPTH, DEPTH), pl.ds(0, QR)], dq_sem.at[n % 4]

    def dkv_refs(n):
        return wdkvt_hbm.at[:, at(n * DEPTH, DEPTH)], vtb.at[pl.ds(0, 576), at((n % 4) * DEPTH, DEPTH)], dkv_sem.at[n % 4]

    def uk_copy(j):
        return pltpu.make_async_copy(wuk_hbm.at[at(WID * j, WID), :], kb.at[pl.ds(0, WID), at(QR + HD * j, HD)], wk_sem.at[j])

    def uv_copy(j):
        return pltpu.make_async_copy(wuv_hbm.at[at(1024 * j, 1024), :], vtb.at[pl.ds(1024, 1024), at(HD * j, HD)], wvt_sem.at[j])

    def piece(j):
        return at(HD * (j + 8), HD), pl.ds(1024, 1024)

    def x_copy(j):
        return pltpu.make_async_copy(x_hbm.at[:, at(1024 * j, 1024)], vtb.at[piece(j)], x_sem.at[j])

    def x_again(j):
        return pltpu.make_async_copy(x_hbm.at[:, at(1024 * j, 1024)], kb.at[at(HD * j, HD), pl.ds(0, 1024)], x_sem.at[j])

    for j in range(7):
        x_copy(j).start()
    for n in range(4):
        fetch_rows(*dq_refs(n), 2)
        fetch_rows(*dkv_refs(n), 2)

    barrier = pltpu.get_barrier_semaphore()
    for peer in (sib, far):
        pl.semaphore_signal(barrier, inc=1, device_id={"tp": peer}, device_id_type=MESH)

    aug = jnp.where(lax.broadcasted_iota(jnp.int32, (LOC, NEW), 0) == 0, 1.0, 0.0).astype(BF16)
    causal = lax.broadcasted_iota(jnp.int32, (NEW, NEW), 0) <= lax.broadcasted_iota(jnp.int32, (NEW, NEW), 1)
    for b in range(2):
        sb[pl.ds(NEW * b, NEW), :32] = cos[b].T
        sb[pl.ds(KVR + NEW * b, NEW), :32] = sin[b].T
    qa[...] = jnp.zeros_like(qa)
    kva[...] = jnp.zeros_like(kva)
    for j in range(7):
        x_copy(j).wait()

    def squares(j, acc):
        v = vtb[piece(j)].astype(F32)
        v = v * v
        return acc + sum(v[:, HD * k:HD * k + HD] for k in range(8))

    total = lax.fori_loop(0, 7, squares, jnp.zeros((HD, HD), F32))
    inv_x = lax.rsqrt(jnp.sum(total, axis=-1, keepdims=True) / 7168.0 + EPS)

    def scaled(j, carry):
        vtb[piece(j)] = (vtb[piece(j)].astype(F32) * inv_x * g1[:, at(1024 * j, 1024)]).astype(BF16)
        return carry

    lax.fori_loop(0, 7, scaled, 0)

    def project(n, carry):
        @pl.when((n >= 1) & (n + 3 < CHUNKS))
        def _():
            fetch_rows(*dq_refs(n + 3), 2)
            fetch_rows(*dkv_refs(n + 3), 2)

        pltpu.make_async_copy(*dq_refs(n)).wait()
        pltpu.make_async_copy(*dkv_refs(n)).wait()

        @pl.when(n == 4)
        def _():
            for j in range(4):
                uk_copy(j).start()
            for j in range(8):
                uv_copy(j).start()

        a = vtb[at(HD * (n // 2 + 8), HD), at(1024 + DEPTH * (n % 2), DEPTH)]
        slot = at((n % 4) * DEPTH, DEPTH)
        qa[...] += dot(a, kb[slot, :QR])
        kva[...] += dot_nt(a, vtb[:576, slot])

        @pl.when(n >= CHUNKS - 4)
        def _():
            j = n - (CHUNKS - 4)
            uk_copy(j).wait()
            wkb[at(HD * j, HD), :] = kb[:WID, at(QR + HD * j, HD)].reshape(HD, WID)
            halves = []
            for k in range(2):
                uv_copy(2 * j + k).wait()
                halves.append(vtb[1024:WID, at(HD * (2 * j + k), HD)].reshape(LOC, WID))
            wvtb[:, at(HD * j, HD)] = jnp.concatenate(halves, axis=0).T

        return carry

    lax.fori_loop(0, CHUNKS, project, 0)
    fetch_rows(*c_refs(0), 4)
    for b in range(2):
        rows = slice(LOC * b, LOC * b + LOC)
        q = qa[rows, :]
        inv_q = lax.rsqrt(jnp.mean(q * q, axis=-1, keepdims=True) + EPS)
        lat[b, :, :QR] = (q * inv_q * gq[...]).astype(BF16)
        c = kva[rows, :KVR]
        inv_c = lax.rsqrt(jnp.mean(c * c, axis=-1, keepdims=True) + EPS)
        lat[b, :, QR:WID] = (c * inv_c * gkv[...]).astype(BF16)
        v1 = kva[rows, KVR:544]
        v2 = kva[rows, 544:576]
        own_cos = sb[at(NEW * b + me * LOC, LOC), :32]
        own_sin = sb[at(KVR + NEW * b + me * LOC, LOC), :32]
        rot = jnp.concatenate([v1 * own_cos - v2 * own_sin, v2 * own_cos + v1 * own_sin, jnp.zeros((LOC, LOC), F32)], axis=1)
        lat[b, :, WID:] = rot.astype(BF16)

    pl.semaphore_wait(barrier, 2)
    to_far = [remote(lat.at[b], latb.at[b, 1], lat_send.at[b, 1], lat_recv.at[b, 1], far) for b in range(2)]
    to_sib = [remote(lat.at[b], latb.at[b, 0], lat_send.at[b, 0], lat_recv.at[b, 0], sib) for b in range(2)]
    onward = [remote(latb.at[b, 1], latb.at[b, 2], lat_send.at[b, 2], lat_recv.at[b, 2], sib) for b in range(2)]
    to_far[0].start()
    to_sib[0].start()
    to_far[1].start()
    to_sib[1].start()
    fetch_wq(0)
    fetch_wq(1)
    for n in range(3):
        fetch_rows(*wo_refs(n, n), 4)
    def kv_start(b):
        length = len_ref[b]
        row = lax.broadcasted_iota(jnp.int32, (PREFIX, HD), 0)
        lane = lax.broadcasted_iota(jnp.int32, (PREFIX, HD), 1)
        old = row < length
        mask[...] = jnp.where(old, 1.0, 0.0).astype(BF16)
        rot = pet[b, :, :PREFIX].astype(F32).T
        rot = jnp.concatenate([rot, jnp.zeros_like(rot)], axis=1)
        pe[:PREFIX, :] = jnp.where(old, rot, jnp.where(lane == LOC, NEG, 0.0)).astype(BF16)
        pltpu.make_async_copy(*c_refs(b)).wait()

    def kv_block(r):
        rows = at(r * NEW, NEW)
        m = mask[rows, :]
        c = cbuf[rows, :] * jnp.concatenate([m, m, m, m], axis=1)
        kb[rows, :] = dot(c, wkb[...]).astype(BF16)
        vtb[:, rows] = dot_nt(wvtb[...], c).astype(BF16)

    def assemble(b):
        for src, owner in ((lat.at[b], me), (latb.at[b, 0], sib), (latb.at[b, 1], far), (latb.at[b, 2], diag)):
            rows = at(owner * LOC, LOC)
            lhsb[rows, :QR] = src[:, :QR]
            cn[b, rows, :] = src[:, QR:WID]
            kn[rows, :] = src[:, WID:]
        cqt[...] = lhsb[:, :QR].T
        knt[b] = kn[...].T[:LOC]
        pe[PREFIX:, :] = kn[...]
        kb[PREFIX:, :] = dot(cn[b], wkb[...]).astype(BF16)
        vtb[:, PREFIX:] = dot_nt(wvtb[...], cn[b]).astype(BF16)

    def queries(b):
        def pair(i, carry):
            @pl.when(i + 2 < 8)
            def _():
                fetch_wq(i + 2)

            pltpu.make_async_copy(*wq_refs(i)).wait()
            cos_b = cos[b]
            sin_b = sin[b]
            for k in range(2):
                q = dot(wqb[i % 3, k], cqt[...])
                v1 = q[HD:160]
                v2 = q[160:]
                qt = jnp.concatenate([q[:HD].astype(BF16), (v1 * cos_b - v2 * sin_b).astype(BF16), (v2 * cos_b + v1 * sin_b).astype(BF16), aug], axis=0)
                q_lo[2 * i + k] = qt
            return carry

        lax.fori_loop(0, 8, pair, 0)
        q_hi[0] = q_lo[0]

    def attend(b):
        halves = ((q_lo, range(5)), (q_hi, range(5, 9)))
        order = [(side, c) for c in range(5) for side, (_, blocks) in enumerate(halves) if c < len(blocks)]

        def head(h, carry):
            d = at(h * HD, HD)
            best = [jnp.full((8, NEW), NEG, F32)] * 2
            for side, k in order:
                c = halves[side][1][k]
                rows = pl.ds(c * NEW, NEW)
                s = dot(jnp.concatenate([kb[rows, d], pe[rows, :]], axis=1), halves[side][0][(h, h % 2)[side]])
                if c == 8:
                    s = jnp.where(causal, s, NEG)
                sb[rows, :] = s
                best[side] = jnp.maximum(best[side], jnp.max(s.reshape(32, 8, NEW), axis=0))
            mb[...] = jnp.maximum(*best)

            @pl.when(h >= 0)
            def _():
                m = jnp.max(mb[...], axis=0, keepdims=True) * C2
                l8 = jnp.zeros((8, NEW), F32)
                for c in range(9):
                    rows = pl.ds(c * NEW, NEW)
                    p = jnp.exp2(sb[rows, :] * C2 - m)
                    sb[rows, :] = p
                    l8 = l8 + jnp.sum(p.reshape(32, 8, NEW), axis=0)
                inv = 1.0 / jnp.sum(l8, axis=0, keepdims=True)
                acc = [jnp.zeros((HD, NEW), F32)] * 2
                for side, k in order:
                    rows = pl.ds(halves[side][1][k] * NEW, NEW)
                    acc[side] = acc[side] + dot(vtb[d, rows], (sb[rows, :] * inv).astype(BF16))
                ob[b, :, d] = (acc[0] + acc[1]).T.astype(BF16)
                q_hi[(h + 1) % 2] = q_lo[jnp.minimum(h + 1, 15)]

            return carry

        lax.fori_loop(0, 16, head, 0)

    def to_sibling(b, n):
        return remote(stage_d.at[n % 4, 0], xbuf.at[b, n], d_send.at[n % 4], d_recv.at[b, n], sib)

    def over_link(b, n):
        return remote(stage_x.at[b, n], rbuf.at[b, n], i_send.at[b, n], i_recv.at[b, n], far)

    def put_y(n):
        return pltpu.make_async_copy(ybuf.at[n % 4], y_hbm.at[:, at(n * CHUNK, CHUNK)], y_sem.at[n % 4])

    def product(rows, g, n):
        pltpu.make_async_copy(*wo_refs(g, n)).wait()
        return dot(lhsb[:rows, :], wob[g % 3])

    def next_wo(g):
        @pl.when(g + 3 < 3 * CHUNKS)
        def _():
            fetch_rows(*wo_refs(g + 3, (g + 3) % CHUNKS), 4)

    def load_lhs(k, b, owner):
        lhsb[LOC * k:LOC * k + LOC, :] = ob[b, at(owner * LOC, LOC), :]

    def pass_on(b, n):
        to_sibling(b, n).wait_recv()
        stage_x[b, n] = stage_x[b, n] + xbuf[b, n]
        over_link(b, n).start()

    def far_start(b):
        load_lhs(0, b, far)
        load_lhs(1, b, diag)

    def far_chunk(b, n):
        g = b * CHUNKS + n
        y = product(HD, g, n)

        @pl.when(n >= 4)
        def _():
            to_sibling(b, n - 4).wait_send()

        stage_d[n % 4, 0] = y[LOC:]
        stage_x[b, n] = y[:LOC]
        to_sibling(b, n).start()
        next_wo(g)

        @pl.when(n >= 1)
        def _():
            pass_on(b, n - 1)

    def far_end(b):
        pass_on(b, CHUNKS - 1)
        for n in range(CHUNKS - 4, CHUNKS):
            to_sibling(b, n).wait_send()

    def own_unit(unit):
        for b in range(2):
            load_lhs(b, b, me)
            load_lhs(2 + b, b, sib)

        def both(n):
            return remote(stage_d.at[n % 4], xbuf.at[:, n], d_send.at[n % 4], d_recv.at[0, n], sib)

        def finish(n):
            both(n).wait_recv()

            @pl.when(n >= 4)
            def _():
                put_y(n - 4).wait()

            for b in range(2):
                over_link(b, n).wait_recv()
                total = ownb[n % 2, b] + xbuf[b, n] + rbuf[b, n]
                x = kb[at(HD * (n // 2) + LOC * b, LOC), at(CHUNK * (n % 2), CHUNK)]
                ybuf[n % 4, pl.ds(LOC * b, LOC), :] = (x.astype(F32) + total).astype(BF16)
            put_y(n).start()

        def chunk(n, carry):
            g = unit * CHUNKS + n
            y = product(NEW, g, n)

            @pl.when(n >= 4)
            def _():
                both(n - 4).wait_send()

            for b in range(2):
                ownb[n % 2, b] = y[LOC * b:LOC * b + LOC]
                stage_d[n % 4, b] = y[HD + LOC * b:192 + LOC * b]
            both(n).start()
            next_wo(g)

            @pl.when(n >= 1)
            def _():
                finish(n - 1)

            return carry

        lax.fori_loop(0, CHUNKS, chunk, 0)
        finish(CHUNKS - 1)
        for n in range(CHUNKS - 4, CHUNKS):
            both(n).wait_send()
            put_y(n).wait()

    def first_block(r, carry):
        @pl.when(r == 6)
        def _():
            to_far[0].wait_recv()
            onward[0].start()

        kv_block(r)
        return carry

    def second_block(r, carry):
        @pl.when((r >= 1) & (2 * r < CHUNKS))
        def _():
            far_chunk(0, 2 * r)
            far_chunk(0, 2 * r + 1)

        kv_block(r)
        return carry

    def far_only(b, n, carry):
        far_chunk(b, n)
        return carry

    kv_start(0)
    lax.fori_loop(0, 8, first_block, 0)
    fetch_rows(*c_refs(1), 4)
    to_sib[0].wait_recv()
    onward[0].wait_recv()
    assemble(0)
    queries(0)
    fetch_wq(0)
    fetch_wq(1)
    attend(0)
    to_far[1].wait_recv()
    onward[1].start()
    far_start(0)
    lax.fori_loop(0, 2, functools.partial(far_only, 0), 0)
    kv_start(1)
    lax.fori_loop(0, 8, second_block, 0)
    far_end(0)
    to_sib[1].wait_recv()
    onward[1].wait_recv()
    assemble(1)
    put_c = pltpu.make_async_copy(cn, cnew_hbm, out_sem.at[0])
    put_k = pltpu.make_async_copy(knt, knewt_hbm, out_sem.at[1])
    put_c.start()
    put_k.start()
    queries(1)
    attend(1)
    for j in range(7):
        x_again(j).start()
    far_start(1)
    lax.fori_loop(0, CHUNKS, functools.partial(far_only, 1), 0)
    far_end(1)
    pl.semaphore_signal(free_sem, inc=1, device_id={"tp": sib}, device_id_type=MESH)
    pl.semaphore_wait(free_sem, 1)
    for j in range(7):
        x_again(j).wait()
    own_unit(2)
    for b in range(2):
        to_far[b].wait_send()
        to_sib[b].wait_send()
        onward[b].wait_send()

        def drain(n, carry):
            over_link(b, n).wait_send()
            return carry

        lax.fori_loop(0, CHUNKS, drain, 0)
    put_c.wait()
    put_k.wait()


def main_call(lengths, *arrays):
    vmem = pl.BlockSpec(memory_space=pltpu.VMEM)
    hbm = pl.BlockSpec(memory_space=pl.ANY)
    dma = pltpu.SemaphoreType.DMA
    return pl.pallas_call(
        main_kernel,
        in_specs=[pl.BlockSpec(memory_space=pltpu.SMEM)] + [vmem] * 6 + [hbm] * 8,
        out_specs=[hbm] * 3,
        out_shape=[
            jax.ShapeDtypeStruct((HD, 7168), BF16),
            jax.ShapeDtypeStruct((2, NEW, KVR), BF16),
            jax.ShapeDtypeStruct((2, LOC, NEW), BF16),
        ],
        scratch_shapes=[
            pltpu.VMEM((2, LOC, LAT_W), BF16),
            pltpu.VMEM((HD, QR), F32),
            pltpu.VMEM((HD, 576), F32),
            pltpu.VMEM((2, 3, LOC, LAT_W), BF16),
            pltpu.VMEM((QR, NEW), BF16),
            pltpu.VMEM((2, NEW, KVR), BF16),
            pltpu.VMEM((NEW, HD), BF16),
            pltpu.VMEM((2, LOC, NEW), BF16),
            pltpu.VMEM((PREFIX + NEW, HD), BF16),
            pltpu.VMEM((PREFIX, HD), BF16),
            pltpu.VMEM((PREFIX, KVR), BF16),
            pltpu.VMEM((PREFIX + NEW, WID), BF16),
            pltpu.VMEM((WID, PREFIX + NEW), BF16),
            pltpu.VMEM((KVR, WID), BF16),
            pltpu.VMEM((WID, KVR), BF16),
            pltpu.VMEM((3, 2, 192, QR), BF16),
            pltpu.VMEM((16, NEW, NEW), BF16),
            pltpu.VMEM((2, NEW, NEW), BF16),
            pltpu.VMEM((PREFIX + NEW, NEW), F32),
            pltpu.VMEM((8, NEW), F32),
            pltpu.VMEM((2, NEW, WID), BF16),
            pltpu.VMEM((NEW, WID), BF16),
            pltpu.VMEM((3, WID, CHUNK), BF16),
            pltpu.VMEM((4, 2, LOC, CHUNK), F32),
            *[pltpu.VMEM((2, CHUNKS, LOC, CHUNK), F32)] * 3,
            pltpu.VMEM((2, 2, LOC, CHUNK), F32),
            pltpu.VMEM((4, HD, CHUNK), BF16),
            *[dma((2, 3))] * 2,
            *[dma((4,))] * 2,
            dma,
            dma((4,)),
            dma((8,)),
            dma((4,)),
            dma((3,)),
            dma((7,)),
            dma((2,)),
            dma((4,)),
            dma((4,)),
            *[dma((2, CHUNKS))] * 3,
            pltpu.SemaphoreType.REGULAR,
        ],
        compiler_params=pltpu.CompilerParams(vmem_limit_bytes=VMEM_ALL, collective_id=0, has_side_effects=True),
        cost_estimate=cost(1e11, 200 * MIB),
        name="main",
    )(lengths, *arrays)


def solution(mesh):
    def local_step(hidden, lengths, rope_cos, rope_sin, cache_lat, cache_pe, norm_in, w_dq, norm_q, w_dkv, norm_kv, w_uq, w_uk, w_uv, w_out):
        pe_t = jnp.swapaxes(cache_pe, 1, 2)
        y, c_new, k_newt = main_call(
            lengths,
            jnp.swapaxes(rope_cos, 1, 2),
            jnp.swapaxes(rope_sin, 1, 2),
            pe_t,
            norm_in[None],
            norm_q,
            norm_kv[None],
            hidden.reshape(HD, 7168),
            w_dq,
            w_dkv.T,
            cache_lat,
            w_uk.reshape(8192, HD),
            w_uv.reshape(8192, HD),
            jnp.transpose(w_uq, (1, 2, 0)),
            w_out,
        )
        y, lat_new, pe_new = update_caches(lengths, y, cache_lat, pe_t, c_new, k_newt)
        return y.reshape(hidden.shape), lat_new, jnp.swapaxes(pe_new, 1, 2)

    spec_tok = P("dp", "tp", None)
    spec_len = P("dp")
    spec_seq = P("dp", None, None)
    spec_vec = P(None)
    spec_mat = P(None, None)
    spec_head = P(None, "tp", None)
    spec_rows = P("tp", None)
    in_specs = (spec_tok, spec_len, spec_seq, spec_seq, spec_seq, spec_seq, spec_vec, spec_mat, spec_vec, spec_mat, spec_vec, spec_head, spec_head, spec_head, spec_rows)
    return jax.shard_map(local_step, mesh=mesh, in_specs=in_specs, out_specs=(spec_tok, spec_seq, spec_seq), check_vma=False)
```

```python
import functools

import jax
import jax.numpy as jnp
from jax import lax
from jax.experimental import pallas as pl
from jax.experimental.pallas import tpu as pltpu
from jax.sharding import PartitionSpec as P

F32 = jnp.float32
BF16 = jnp.bfloat16
EPS = 1e-6
MIB = 1 << 20
VMEM_ALL = 67043328
MESH = pl.DeviceIdType.MESH
LAT_W = 2176
PREFIX = 2048
ROW_BLK = 512
CHUNK = 512
DEPTH = 512
CHUNKS = 7168 // CHUNK
C2 = 192.0 ** -0.5 * 1.4426950408889634
NEG = -1e30
LOC = 64
HD = 128
NEW = 256
QR = 1536
WID = 2048
CB = 768
KVR = 512
NT = (((1,), (1,)), ((), ()))


def dot(lhs, rhs):
    return jnp.dot(lhs, rhs, preferred_element_type=F32)


def dot_nt(lhs, rhs):
    return lax.dot_general(lhs, rhs, NT, preferred_element_type=F32)


def cost(flops, nbytes):
    return pl.CostEstimate(flops=int(flops), bytes_accessed=int(nbytes), transcendentals=0)


def cache_kernel(len_ref, y_hbm, c_hbm, pe_hbm, cn_hbm, kn_hbm, yo_hbm, co_hbm, po_hbm, y, rows, cols, cn, kn, in_sem, out_sem, side_sem, y_sem):
    blocks = rows.shape[1] // NEW
    span = lambda r: pl.ds(r * NEW, NEW)
    lat_in = lambda b, r: pltpu.make_async_copy(c_hbm.at[b, span(r)], rows.at[b, span(r)], in_sem.at[b, r])
    lat_out = lambda b, r: pltpu.make_async_copy(rows.at[b, span(r)], co_hbm.at[b, span(r)], out_sem.at[b, r])
    pe_in = lambda b: pltpu.make_async_copy(pe_hbm.at[b], cols.at[b], in_sem.at[b, blocks])
    pe_out = lambda b: pltpu.make_async_copy(cols.at[b], po_hbm.at[b], out_sem.at[b, blocks])
    new_in = [pltpu.make_async_copy(cn_hbm, cn, side_sem.at[0]), pltpu.make_async_copy(kn_hbm, kn, side_sem.at[1])]
    part = lambda k: pl.ds(32 * k, 32)
    y_in = [pltpu.make_async_copy(y_hbm.at[part(k)], y.at[part(k)], y_sem.at[k]) for k in range(4)]
    y_out = [pltpu.make_async_copy(y.at[part(k)], yo_hbm.at[part(k)], y_sem.at[4 + k]) for k in range(4)]
    places = [(b, r) for b in range(2) for r in range(blocks)]
    for copy in new_in:
        copy.start()
    for b, r in places:
        lat_in(b, r).start()
    for b in range(2):
        pe_in(b).start()
    for copy in y_in:
        copy.start()
    for copy in new_in:
        copy.wait()
    for b, r in places:
        shift = r * NEW - len_ref[b]
        lat_in(b, r).wait()

        @pl.when((shift < NEW) & (shift > -NEW))
        def _():
            row = lax.broadcasted_iota(jnp.int32, (NEW, NEW), 0) + shift
            hot = (row == lax.broadcasted_iota(jnp.int32, (NEW, NEW), 1)).astype(F32).astype(BF16)
            row = lax.broadcasted_iota(jnp.int32, (NEW, KVR), 0) + shift
            old = rows[b, span(r), :].astype(F32)
            rows[b, span(r), :] = jnp.where((row >= 0) & (row < NEW), dot(hot, cn[b]), old).astype(BF16)

        lat_out(b, r).start()
    for b in range(2):
        pe_in(b).wait()
        for r in range(blocks):
            shift = r * NEW - len_ref[b]

            @pl.when((shift < NEW) & (shift > -NEW))
            def _():
                row = lax.broadcasted_iota(jnp.int32, (NEW, NEW), 0) + shift
                hot = (row == lax.broadcasted_iota(jnp.int32, (NEW, NEW), 1)).astype(F32).astype(BF16)
                col = lax.broadcasted_iota(jnp.int32, (LOC, NEW), 1) + shift
                old = cols[b, :, span(r)].astype(F32)
                cols[b, :, span(r)] = jnp.where((col >= 0) & (col < NEW), dot_nt(kn[b], hot), old).astype(BF16)

        pe_out(b).start()
    for k in range(4):
        y_in[k].wait()
        y_out[k].start()
    for b, r in places:
        lat_out(b, r).wait()
    for copy in y_out:
        copy.wait()
    for b in range(2):
        pe_out(b).wait()


def update_caches(lengths, y, cache_lat, pe_t, c_new, k_newt):
    hbm = pl.BlockSpec(memory_space=pl.ANY)
    sems = pltpu.SemaphoreType.DMA((2, cache_lat.shape[1] // NEW + 1))
    return pl.pallas_call(
        cache_kernel,
        in_specs=[pl.BlockSpec(memory_space=pltpu.SMEM)] + [hbm] * 5,
        out_specs=[hbm] * 3,
        out_shape=[jax.ShapeDtypeStruct(v.shape, BF16) for v in (y, cache_lat, pe_t)],
        scratch_shapes=[*[pltpu.VMEM(v.shape, BF16) for v in (y, cache_lat, pe_t, c_new, k_newt)], sems, sems, pltpu.SemaphoreType.DMA((2,)), pltpu.SemaphoreType.DMA((8,))],
        compiler_params=pltpu.CompilerParams(vmem_limit_bytes=VMEM_ALL),
        cost_estimate=cost(4e9, 12 * MIB),
        name="caches",
    )(lengths, y, cache_lat, pe_t, c_new, k_newt)


def at(start, size):
    return pl.ds(pl.multiple_of(start, size), size)


def main_kernel(len_ref, cos, sin, pet, g1, gq, gkv, x_hbm, wdq_hbm, wdkvt_hbm, c_hbm, wuk_hbm, wuv_hbm, wq_hbm, wo_hbm,
                y_hbm, cnew_hbm, knewt_hbm,
                lat, qa, kva, latb, cqt, cn, kn, knt, pe, cbuf, kb, vtb, wkb, wvtb, wqb, q_lo, q_hi, sb_a, sb_b, mb, ob, lhsb, wob,
                stage_d, xbuf, stage_x, rbuf, ybuf,
                lat_send, lat_recv, dq_sem, dkv_sem, c_sem, wk_sem, wvt_sem, wq_sem, wo_sem, x_sem, out_sem, y_sem,
                d_send, d_recv, i_send, i_recv, free_sem):
    sb = (sb_a, sb_b)
    me = lax.axis_index("tp")
    chip = me // 2
    core = me % 2
    sib = 2 * chip + (1 - core)
    far = 2 * (1 - chip) + core
    diag = 2 * (1 - chip) + (1 - core)

    def remote(src, dst, send, recv, peer):
        return pltpu.make_async_remote_copy(src_ref=src, dst_ref=dst, send_sem=send, recv_sem=recv, device_id={"tp": peer}, device_id_type=MESH)

    def fetch_rows(src, dst, sem, parts):
        size = dst.shape[0] // parts
        for k in range(parts):
            rows = pl.ds(k * size, size)
            pltpu.make_async_copy(src.at[rows], dst.at[rows], sem).start()

    def c_refs(b):
        return c_hbm.at[b, pl.ds(0, PREFIX), :], cbuf, c_sem

    def wq_refs(h):
        return wq_hbm.at[pl.ds(2 * h, 2)], wqb.at[h % 3], wq_sem.at[h % 3]

    def fetch_wq(i):
        src, dst, sem = wq_refs(i)
        for k in range(2):
            fetch_rows(src.at[k], dst.at[k], sem, 2)

    def wo_refs(g, n):
        return wo_hbm.at[:, at(n * CHUNK, CHUNK)], wob.at[g % 3], wo_sem.at[g % 3]

    def dq_refs(n):
        return wdq_hbm.at[at(n * DEPTH, DEPTH), :], kb.at[at((n % 4) * DEPTH, DEPTH), pl.ds(0, QR)], dq_sem.at[n % 4]

    def dkv_refs(n):
        return wdkvt_hbm.at[:, at(n * DEPTH, DEPTH)], vtb.at[pl.ds(0, 576), at((n % 4) * DEPTH, DEPTH)], dkv_sem.at[n % 4]

    def uk_copy(j):
        return pltpu.make_async_copy(wuk_hbm.at[at(WID * j, WID), :], kb.at[pl.ds(0, WID), at(QR + HD * j, HD)], wk_sem.at[j])

    def uv_copy(j):
        return pltpu.make_async_copy(wuv_hbm.at[at(1024 * j, 1024), :], vtb.at[pl.ds(1024, 1024), at(HD * j, HD)], wvt_sem.at[j])

    def piece(j):
        return at(HD * (j + 8), HD), pl.ds(1024, 1024)

    def x_copy(j):
        return pltpu.make_async_copy(x_hbm.at[:, at(1024 * j, 1024)], vtb.at[piece(j)], x_sem.at[j])

    def x_again(j):
        return pltpu.make_async_copy(x_hbm.at[:, at(1024 * j, 1024)], kb.at[at(HD * j, HD), pl.ds(0, 1024)], x_sem.at[j])

    for j in range(7):
        x_copy(j).start()
    for n in range(4):
        fetch_rows(*dq_refs(n), 2)
        fetch_rows(*dkv_refs(n), 2)

    barrier = pltpu.get_barrier_semaphore()
    for peer in (sib, far):
        pl.semaphore_signal(barrier, inc=1, device_id={"tp": peer}, device_id_type=MESH)

    aug = jnp.where(lax.broadcasted_iota(jnp.int32, (LOC, NEW), 0) == 0, 1.0, 0.0).astype(BF16)
    causal = lax.broadcasted_iota(jnp.int32, (NEW, NEW), 0) <= lax.broadcasted_iota(jnp.int32, (NEW, NEW), 1)
    for b in range(2):
        sb_a[pl.ds(NEW * b, NEW), :32] = cos[b].T
        sb_a[pl.ds(KVR + NEW * b, NEW), :32] = sin[b].T
    qa[...] = jnp.zeros_like(qa)
    kva[...] = jnp.zeros_like(kva)
    for j in range(7):
        x_copy(j).wait()

    def squares(j, acc):
        v = vtb[piece(j)].astype(F32)
        v = v * v
        return acc + sum(v[:, HD * k:HD * k + HD] for k in range(8))

    total = lax.fori_loop(0, 7, squares, jnp.zeros((HD, HD), F32))
    inv_x = lax.rsqrt(jnp.sum(total, axis=-1, keepdims=True) / 7168.0 + EPS)

    def scaled(j, carry):
        vtb[piece(j)] = (vtb[piece(j)].astype(F32) * inv_x * g1[:, at(1024 * j, 1024)]).astype(BF16)
        return carry

    lax.fori_loop(0, 7, scaled, 0)

    def project(n, carry):
        @pl.when((n >= 1) & (n + 3 < CHUNKS))
        def _():
            fetch_rows(*dq_refs(n + 3), 2)
            fetch_rows(*dkv_refs(n + 3), 2)

        pltpu.make_async_copy(*dq_refs(n)).wait()
        pltpu.make_async_copy(*dkv_refs(n)).wait()

        @pl.when(n == 4)
        def _():
            for j in range(4):
                uk_copy(j).start()
            for j in range(8):
                uv_copy(j).start()

        a = vtb[at(HD * (n // 2 + 8), HD), at(1024 + DEPTH * (n % 2), DEPTH)]
        slot = at((n % 4) * DEPTH, DEPTH)
        qa[...] += dot(a, kb[slot, :QR])
        kva[...] += dot_nt(a, vtb[:576, slot])

        @pl.when(n >= CHUNKS - 4)
        def _():
            j = n - (CHUNKS - 4)
            uk_copy(j).wait()
            wkb[at(HD * j, HD), :] = kb[:WID, at(QR + HD * j, HD)].reshape(HD, WID)
            halves = []
            for k in range(2):
                uv_copy(2 * j + k).wait()
                halves.append(vtb[1024:WID, at(HD * (2 * j + k), HD)].reshape(LOC, WID))
            wvtb[:, at(HD * j, HD)] = jnp.concatenate(halves, axis=0).T

        return carry

    lax.fori_loop(0, CHUNKS, project, 0)
    fetch_rows(*c_refs(0), 4)
    for b in range(2):
        rows = slice(LOC * b, LOC * b + LOC)
        q = qa[rows, :]
        inv_q = lax.rsqrt(jnp.mean(q * q, axis=-1, keepdims=True) + EPS)
        lat[b, :, :QR] = (q * inv_q * gq[...]).astype(BF16)
        c = kva[rows, :KVR]
        inv_c = lax.rsqrt(jnp.mean(c * c, axis=-1, keepdims=True) + EPS)
        lat[b, :, QR:WID] = (c * inv_c * gkv[...]).astype(BF16)
        v1 = kva[rows, KVR:544]
        v2 = kva[rows, 544:576]
        own_cos = sb_a[at(NEW * b + me * LOC, LOC), :32]
        own_sin = sb_a[at(KVR + NEW * b + me * LOC, LOC), :32]
        rot = jnp.concatenate([v1 * own_cos - v2 * own_sin, v2 * own_cos + v1 * own_sin, jnp.zeros((LOC, LOC), F32)], axis=1)
        lat[b, :, WID:] = rot.astype(BF16)

    pl.semaphore_wait(barrier, 2)
    to_far = [remote(lat.at[b], latb.at[b, 1], lat_send.at[b, 1], lat_recv.at[b, 1], far) for b in range(2)]
    to_sib = [remote(lat.at[b], latb.at[b, 0], lat_send.at[b, 0], lat_recv.at[b, 0], sib) for b in range(2)]
    onward = [remote(latb.at[b, 1], latb.at[b, 2], lat_send.at[b, 2], lat_recv.at[b, 2], sib) for b in range(2)]
    to_far[0].start()
    to_sib[0].start()
    to_far[1].start()
    to_sib[1].start()
    for i in range(3):
        fetch_wq(i)
    for n in range(3):
        fetch_rows(*wo_refs(n, n), 4)
    def kv_start(b):
        length = len_ref[b]
        row = lax.broadcasted_iota(jnp.int32, (PREFIX, HD), 0)
        lane = lax.broadcasted_iota(jnp.int32, (PREFIX, HD), 1)
        old = row < length
        rot = pet[b, :, :PREFIX].astype(F32).T
        rot = jnp.concatenate([rot, jnp.zeros_like(rot)], axis=1)
        pe[:PREFIX, :] = jnp.where(old, rot, jnp.where(lane == LOC, NEG, 0.0)).astype(BF16)
        pltpu.make_async_copy(*c_refs(b)).wait()

    def kv_block(b, r, size):
        rows = at(r * size, size)
        row = lax.broadcasted_iota(jnp.int32, (size, HD), 0) + r * size
        m = jnp.where(row < len_ref[b], 1.0, 0.0).astype(BF16)
        c = cbuf[rows, :] * jnp.concatenate([m, m, m, m], axis=1)
        kb[rows, :] = dot(c, wkb[...]).astype(BF16)
        vtb[:, rows] = dot_nt(wvtb[...], c).astype(BF16)

    def assemble(b):
        cqa = ob.at[1]
        for src, owner in ((lat.at[b], me), (latb.at[b, 0], sib), (latb.at[b, 1], far), (latb.at[b, 2], diag)):
            rows = at(owner * LOC, LOC)
            cqa[rows, :QR] = src[:, :QR]
            cn[b, rows, :] = src[:, QR:WID]
            kn[rows, :] = src[:, WID:]
        cqt[...] = cqa[:, :QR].T
        knt[b] = kn[...].T[:LOC]
        pe[PREFIX:, :] = kn[...]
        kb[PREFIX:, :] = dot(cn[b], wkb[...]).astype(BF16)
        vtb[:, PREFIX:] = dot_nt(wvtb[...], cn[b]).astype(BF16)

    def query_pair(b, i):
        pltpu.make_async_copy(*wq_refs(i)).wait()
        cos_b = cos[b]
        sin_b = sin[b]
        for k in range(2):
            q = dot(wqb[i % 3, k], cqt[...])
            v1 = q[HD:160]
            v2 = q[160:]
            qt = jnp.concatenate([q[:HD].astype(BF16), (v1 * cos_b - v2 * sin_b).astype(BF16), (v2 * cos_b + v1 * sin_b).astype(BF16), aug], axis=0)
            q_lo[2 * i + k] = qt

        @pl.when(i + 3 < 8)
        def _():
            fetch_wq(i + 3)

    def first_queries(i, carry):
        query_pair(0, i)
        return carry

    def attend(b):
        halves = ((q_lo, range(5)), (q_hi, range(5, 9)))
        order = [(side, c) for c in range(5) for side, (_, blocks) in enumerate(halves) if c < len(blocks)]

        def score(h, k):
            d = at(h * HD, HD)
            best = [jnp.full((8, NEW), NEG, F32)] * 2
            for side, j in order:
                c = halves[side][1][j]
                rows = pl.ds(c * NEW, NEW)
                t = dot(jnp.concatenate([kb[rows, d], pe[rows, :]], axis=1), halves[side][0][(h, k)[side]])
                if c == 8:
                    t = jnp.where(causal, t, NEG)
                sb[k][rows, :] = t
                best[side] = jnp.maximum(best[side], jnp.max(t.reshape(32, 8, NEW), axis=0))
                yield
            mb[k] = jnp.maximum(*best)

        def finish(h, k):
            d = at(h * HD, HD)
            m = jnp.max(mb[k], axis=0, keepdims=True) * C2
            l8 = jnp.zeros((8, NEW), F32)
            for c in range(9):
                rows = pl.ds(c * NEW, NEW)
                p = jnp.exp2(sb[k][rows, :] * C2 - m)
                sb[k][rows, :] = p
                l8 = l8 + jnp.sum(p.reshape(32, 8, NEW), axis=0)
                yield
            inv = 1.0 / jnp.sum(l8, axis=0, keepdims=True)
            acc = [jnp.zeros((HD, NEW), F32)] * 2
            for side, j in order:
                rows = pl.ds(halves[side][1][j] * NEW, NEW)
                acc[side] = acc[side] + dot(vtb[d, rows], (sb[k][rows, :] * inv).astype(BF16))
                yield
            ob[b, :, d] = (acc[0] + acc[1]).T.astype(BF16)

        def weave(*parts):
            live = list(parts)
            while live:
                live = [part for part in live if next(part, live) is None]

        for k in range(2):
            q_hi[k] = q_lo[k]

        @pl.when(me >= 0)
        def _():
            weave(score(0, 0))

        def pair(i, carry):
            h = 2 * i

            @pl.when(i >= 0)
            def _():
                weave(score(h + 1, 1), finish(h, 0))
                q_hi[0] = q_lo[jnp.minimum(h + 2, 15)]

            @pl.when(i < 8)
            def _():
                weave(score(jnp.minimum(h + 2, 15), 0), finish(h + 1, 1))
                q_hi[1] = q_lo[jnp.minimum(h + 3, 15)]

            return carry

        lax.fori_loop(0, 8, pair, 0)

    def to_sibling(b, n):
        return remote(stage_d.at[n % 4, 0], xbuf.at[b, n], d_send.at[n % 4], d_recv.at[b, n], sib)

    def over_link(b, n):
        return remote(stage_x.at[b, n], rbuf.at[b, n], i_send.at[b, n], i_recv.at[b, n], far)

    def put_y(n):
        return pltpu.make_async_copy(ybuf.at[n % 4], y_hbm.at[:, at(n * CHUNK, CHUNK)], y_sem.at[n % 4])

    def product(rows, g, n):
        pltpu.make_async_copy(*wo_refs(g, n)).wait()
        return dot(lhsb[:rows, :], wob[g % 3])

    def next_wo(g):
        @pl.when(g + 3 < 3 * CHUNKS)
        def _():
            fetch_rows(*wo_refs(g + 3, (g + 3) % CHUNKS), 4)

    def load_lhs(k, b, owner):
        lhsb[LOC * k:LOC * k + LOC, :] = ob[b, at(owner * LOC, LOC), :]

    def pass_on(b, n):
        to_sibling(b, n).wait_recv()
        stage_x[b, n] = stage_x[b, n] + xbuf[b, n]
        over_link(b, n).start()

    def far_start(b):
        load_lhs(0, b, far)
        load_lhs(1, b, diag)

    def far_chunk(b, n):
        g = b * CHUNKS + n
        y = product(HD, g, n)

        @pl.when(n >= 4)
        def _():
            to_sibling(b, n - 4).wait_send()

        stage_d[n % 4, 0] = y[LOC:]
        stage_x[b, n] = y[:LOC]
        to_sibling(b, n).start()
        next_wo(g)

        @pl.when(n == 1)
        def _():
            pass_on(b, 0)

        @pl.when(n >= 3)
        def _():
            pass_on(b, n - 2)

    def far_end(b):
        pass_on(b, CHUNKS - 2)
        pass_on(b, CHUNKS - 1)
        for n in range(CHUNKS - 4, CHUNKS):
            to_sibling(b, n).wait_send()

    def own_unit(unit):
        for n in range(4):
            over_link(0, n).wait_send()
        for b in range(2):
            load_lhs(b, b, me)
            load_lhs(2 + b, b, sib)

        def both(n):
            return remote(stage_d.at[n % 4], xbuf.at[:, n], d_send.at[n % 4], d_recv.at[0, n], sib)

        def finish(n):
            both(n).wait_recv()

            @pl.when(n >= 4)
            def _():
                put_y(n - 4).wait()

            for b in range(2):
                over_link(b, n).wait_recv()
                total = stage_x[0, 2 * (n % 2) + b] + xbuf[b, n] + rbuf[b, n]
                x = kb[at(HD * (n // 2) + LOC * b, LOC), at(CHUNK * (n % 2), CHUNK)]
                ybuf[n % 4, pl.ds(LOC * b, LOC), :] = (x.astype(F32) + total).astype(BF16)
            put_y(n).start()

        def chunk(n, carry):
            g = unit * CHUNKS + n
            y = product(NEW, g, n)

            @pl.when(n >= 4)
            def _():
                both(n - 4).wait_send()

            for b in range(2):
                stage_x[0, 2 * (n % 2) + b] = y[LOC * b:LOC * b + LOC]
                stage_d[n % 4, b] = y[HD + LOC * b:192 + LOC * b]
            both(n).start()
            next_wo(g)

            @pl.when(n >= 1)
            def _():
                finish(n - 1)

            return carry

        lax.fori_loop(0, CHUNKS, chunk, 0)
        finish(CHUNKS - 1)
        for n in range(CHUNKS - 4, CHUNKS):
            both(n).wait_send()
            put_y(n).wait()

    def first_block(r, carry):
        @pl.when(r == 3)
        def _():
            to_far[0].wait_recv()
            onward[0].start()

        kv_block(0, r, ROW_BLK)
        return carry

    def second_block(r, carry):
        @pl.when((r >= 1) & (2 * r < CHUNKS))
        def _():
            far_chunk(0, 2 * r)
            far_chunk(0, 2 * r + 1)

        kv_block(1, r, NEW)
        query_pair(1, r)
        return carry

    def far_only(b, n, carry):
        far_chunk(b, n)
        return carry

    kv_start(0)
    lax.fori_loop(0, PREFIX // ROW_BLK, first_block, 0)
    fetch_rows(*c_refs(1), 4)
    to_sib[0].wait_recv()
    onward[0].wait_recv()
    assemble(0)
    lax.fori_loop(0, 8, first_queries, 0)
    for i in range(3):
        fetch_wq(i)
    attend(0)
    to_far[1].wait_recv()
    onward[1].start()
    far_start(0)
    lax.fori_loop(0, 2, functools.partial(far_only, 0), 0)
    kv_start(1)
    to_sib[1].wait_recv()
    onward[1].wait_recv()
    assemble(1)
    lax.fori_loop(0, 8, second_block, 0)
    far_end(0)
    put_c = pltpu.make_async_copy(cn, cnew_hbm, out_sem.at[0])
    put_k = pltpu.make_async_copy(knt, knewt_hbm, out_sem.at[1])
    put_c.start()
    put_k.start()
    attend(1)
    for j in range(7):
        x_again(j).start()
    far_start(1)
    lax.fori_loop(0, CHUNKS, functools.partial(far_only, 1), 0)
    far_end(1)
    pl.semaphore_signal(free_sem, inc=1, device_id={"tp": sib}, device_id_type=MESH)
    pl.semaphore_wait(free_sem, 1)
    for j in range(7):
        x_again(j).wait()
    own_unit(2)
    for b in range(2):
        to_far[b].wait_send()
        to_sib[b].wait_send()
        onward[b].wait_send()

        def drain(n, carry):
            over_link(b, n).wait_send()
            return carry

        lax.fori_loop((4, 0)[b], CHUNKS, drain, 0)
    put_c.wait()
    put_k.wait()


def main_call(lengths, *arrays):
    vmem = pl.BlockSpec(memory_space=pltpu.VMEM)
    hbm = pl.BlockSpec(memory_space=pl.ANY)
    dma = pltpu.SemaphoreType.DMA
    return pl.pallas_call(
        main_kernel,
        in_specs=[pl.BlockSpec(memory_space=pltpu.SMEM)] + [vmem] * 6 + [hbm] * 8,
        out_specs=[hbm] * 3,
        out_shape=[
            jax.ShapeDtypeStruct((HD, 7168), BF16),
            jax.ShapeDtypeStruct((2, NEW, KVR), BF16),
            jax.ShapeDtypeStruct((2, LOC, NEW), BF16),
        ],
        scratch_shapes=[
            pltpu.VMEM((2, LOC, LAT_W), BF16),
            pltpu.VMEM((HD, QR), F32),
            pltpu.VMEM((HD, 576), F32),
            pltpu.VMEM((2, 3, LOC, LAT_W), BF16),
            pltpu.VMEM((QR, NEW), BF16),
            pltpu.VMEM((2, NEW, KVR), BF16),
            pltpu.VMEM((NEW, HD), BF16),
            pltpu.VMEM((2, LOC, NEW), BF16),
            pltpu.VMEM((PREFIX + NEW, HD), BF16),
            pltpu.VMEM((PREFIX, KVR), BF16),
            pltpu.VMEM((PREFIX + NEW, WID), BF16),
            pltpu.VMEM((WID, PREFIX + NEW), BF16),
            pltpu.VMEM((KVR, WID), BF16),
            pltpu.VMEM((WID, KVR), BF16),
            pltpu.VMEM((3, 2, 192, QR), BF16),
            pltpu.VMEM((16, NEW, NEW), BF16),
            pltpu.VMEM((2, NEW, NEW), BF16),
            *[pltpu.VMEM((PREFIX + NEW, NEW), F32)] * 2,
            pltpu.VMEM((2, 8, NEW), F32),
            pltpu.VMEM((2, NEW, WID), BF16),
            pltpu.VMEM((NEW, WID), BF16),
            pltpu.VMEM((3, WID, CHUNK), BF16),
            pltpu.VMEM((4, 2, LOC, CHUNK), F32),
            *[pltpu.VMEM((2, CHUNKS, LOC, CHUNK), F32)] * 3,
            pltpu.VMEM((4, HD, CHUNK), BF16),
            *[dma((2, 3))] * 2,
            *[dma((4,))] * 2,
            dma,
            dma((4,)),
            dma((8,)),
            dma((4,)),
            dma((3,)),
            dma((7,)),
            dma((2,)),
            dma((4,)),
            dma((4,)),
            *[dma((2, CHUNKS))] * 3,
            pltpu.SemaphoreType.REGULAR,
        ],
        compiler_params=pltpu.CompilerParams(vmem_limit_bytes=VMEM_ALL, collective_id=0, has_side_effects=True),
        cost_estimate=cost(1e11, 200 * MIB),
        name="main",
    )(lengths, *arrays)


def solution(mesh):
    def local_step(hidden, lengths, rope_cos, rope_sin, cache_lat, cache_pe, norm_in, w_dq, norm_q, w_dkv, norm_kv, w_uq, w_uk, w_uv, w_out):
        pe_t = jnp.swapaxes(cache_pe, 1, 2)
        y, c_new, k_newt = main_call(
            lengths,
            jnp.swapaxes(rope_cos, 1, 2),
            jnp.swapaxes(rope_sin, 1, 2),
            pe_t,
            norm_in[None],
            norm_q,
            norm_kv[None],
            hidden.reshape(HD, 7168),
            w_dq,
            w_dkv.T,
            cache_lat,
            w_uk.reshape(8192, HD),
            w_uv.reshape(8192, HD),
            jnp.transpose(w_uq, (1, 2, 0)),
            w_out,
        )
        y, lat_new, pe_new = update_caches(lengths, y, cache_lat, pe_t, c_new, k_newt)
        return y.reshape(hidden.shape), lat_new, jnp.swapaxes(pe_new, 1, 2)

    spec_tok = P("dp", "tp", None)
    spec_len = P("dp")
    spec_seq = P("dp", None, None)
    spec_vec = P(None)
    spec_mat = P(None, None)
    spec_head = P(None, "tp", None)
    spec_rows = P("tp", None)
    in_specs = (spec_tok, spec_len, spec_seq, spec_seq, spec_seq, spec_seq, spec_vec, spec_mat, spec_vec, spec_mat, spec_vec, spec_head, spec_head, spec_head, spec_rows)
    return jax.shard_map(local_step, mesh=mesh, in_specs=in_specs, out_specs=(spec_tok, spec_seq, spec_seq), check_vma=False)
```

```python
import functools

import jax
import jax.numpy as jnp
from jax import lax
from jax.experimental import pallas as pl
from jax.experimental.pallas import tpu as pltpu
from jax.sharding import PartitionSpec as P

F32 = jnp.float32
BF16 = jnp.bfloat16
EPS = 1e-6
MIB = 1 << 20
VMEM_ALL = 67043328
MESH = pl.DeviceIdType.MESH
LAT_W = 2176
PREFIX = 2048
ROW_BLK = 512
CHUNK = 512
DEPTH = 512
CHUNKS = 7168 // CHUNK
C2 = 192.0 ** -0.5 * 1.4426950408889634
NEG = -1e30
LOC = 64
HD = 128
NEW = 256
QR = 1536
WID = 2048
CB = 768
KVR = 512
NT = (((1,), (1,)), ((), ()))


def dot(lhs, rhs):
    return jnp.dot(lhs, rhs, preferred_element_type=F32)


def dot_nt(lhs, rhs):
    return lax.dot_general(lhs, rhs, NT, preferred_element_type=F32)


def cost(flops, nbytes):
    return pl.CostEstimate(flops=int(flops), bytes_accessed=int(nbytes), transcendentals=0)


def cache_kernel(len_ref, y_hbm, c_hbm, pe_hbm, cn_hbm, kn_hbm, yo_hbm, co_hbm, po_hbm, y, rows, cols, cn, kn, in_sem, out_sem, side_sem, y_sem):
    blocks = rows.shape[1] // NEW
    span = lambda r: pl.ds(r * NEW, NEW)
    lat_in = lambda b, r: pltpu.make_async_copy(c_hbm.at[b, span(r)], rows.at[b, span(r)], in_sem.at[b, r])
    lat_out = lambda b, r: pltpu.make_async_copy(rows.at[b, span(r)], co_hbm.at[b, span(r)], out_sem.at[b, r])
    pe_in = lambda b: pltpu.make_async_copy(pe_hbm.at[b], cols.at[b], in_sem.at[b, blocks])
    pe_out = lambda b: pltpu.make_async_copy(cols.at[b], po_hbm.at[b], out_sem.at[b, blocks])
    new_in = [pltpu.make_async_copy(cn_hbm, cn, side_sem.at[0]), pltpu.make_async_copy(kn_hbm, kn, side_sem.at[1])]
    part = lambda k: pl.ds(32 * k, 32)
    y_in = [pltpu.make_async_copy(y_hbm.at[part(k)], y.at[part(k)], y_sem.at[k]) for k in range(4)]
    y_out = [pltpu.make_async_copy(y.at[part(k)], yo_hbm.at[part(k)], y_sem.at[4 + k]) for k in range(4)]
    places = [(b, r) for b in range(2) for r in range(blocks)]
    for copy in new_in:
        copy.start()
    for b, r in places:
        lat_in(b, r).start()
    for b in range(2):
        pe_in(b).start()
    for copy in y_in:
        copy.start()
    for copy in new_in:
        copy.wait()
    for b, r in places:
        shift = r * NEW - len_ref[b]
        lat_in(b, r).wait()

        @pl.when((shift < NEW) & (shift > -NEW))
        def _():
            row = lax.broadcasted_iota(jnp.int32, (NEW, NEW), 0) + shift
            hot = (row == lax.broadcasted_iota(jnp.int32, (NEW, NEW), 1)).astype(F32).astype(BF16)
            row = lax.broadcasted_iota(jnp.int32, (NEW, KVR), 0) + shift
            old = rows[b, span(r), :].astype(F32)
            rows[b, span(r), :] = jnp.where((row >= 0) & (row < NEW), dot(hot, cn[b]), old).astype(BF16)

        lat_out(b, r).start()
    for b in range(2):
        pe_in(b).wait()
        for r in range(blocks):
            shift = r * NEW - len_ref[b]

            @pl.when((shift < NEW) & (shift > -NEW))
            def _():
                row = lax.broadcasted_iota(jnp.int32, (NEW, NEW), 0) + shift
                hot = (row == lax.broadcasted_iota(jnp.int32, (NEW, NEW), 1)).astype(F32).astype(BF16)
                col = lax.broadcasted_iota(jnp.int32, (LOC, NEW), 1) + shift
                old = cols[b, :, span(r)].astype(F32)
                cols[b, :, span(r)] = jnp.where((col >= 0) & (col < NEW), dot_nt(kn[b], hot), old).astype(BF16)

        pe_out(b).start()
    for k in range(4):
        y_in[k].wait()
        y_out[k].start()
    for b, r in places:
        lat_out(b, r).wait()
    for copy in y_out:
        copy.wait()
    for b in range(2):
        pe_out(b).wait()


def update_caches(lengths, y, cache_lat, pe_t, c_new, k_newt):
    hbm = pl.BlockSpec(memory_space=pl.ANY)
    sems = pltpu.SemaphoreType.DMA((2, cache_lat.shape[1] // NEW + 1))
    return pl.pallas_call(
        cache_kernel,
        in_specs=[pl.BlockSpec(memory_space=pltpu.SMEM)] + [hbm] * 5,
        out_specs=[hbm] * 3,
        out_shape=[jax.ShapeDtypeStruct(v.shape, BF16) for v in (y, cache_lat, pe_t)],
        scratch_shapes=[*[pltpu.VMEM(v.shape, BF16) for v in (y, cache_lat, pe_t, c_new, k_newt)], sems, sems, pltpu.SemaphoreType.DMA((2,)), pltpu.SemaphoreType.DMA((8,))],
        compiler_params=pltpu.CompilerParams(vmem_limit_bytes=VMEM_ALL),
        cost_estimate=cost(4e9, 12 * MIB),
        name="caches",
    )(lengths, y, cache_lat, pe_t, c_new, k_newt)


def at(start, size):
    return pl.ds(pl.multiple_of(start, size), size)


def main_kernel(len_ref, cos, sin, pet, g1, gq, gkv, x_hbm, wdq_hbm, wdkvt_hbm, c_hbm, wuk_hbm, wuv_hbm, wq_hbm, wo_hbm,
                y_hbm, cnew_hbm, knewt_hbm,
                lat, qa, kva, latb, cqt, cn, kn, knt, pe, cbuf, kb, vtb, wkb, wvtb, wqb, q_lo, q_hi, sb_a, sb_b, mb, ob, lhsb, wob,
                stage_d, xbuf, stage_x, rbuf, ybuf,
                lat_send, lat_recv, dq_sem, dkv_sem, c_sem, wk_sem, wvt_sem, wq_sem, wo_sem, x_sem, out_sem, y_sem,
                d_send, d_recv, i_send, i_recv, free_sem):
    sb = (sb_a, sb_b)
    me = lax.axis_index("tp")
    chip = me // 2
    core = me % 2
    sib = 2 * chip + (1 - core)
    far = 2 * (1 - chip) + core
    diag = 2 * (1 - chip) + (1 - core)

    def remote(src, dst, send, recv, peer):
        return pltpu.make_async_remote_copy(src_ref=src, dst_ref=dst, send_sem=send, recv_sem=recv, device_id={"tp": peer}, device_id_type=MESH)

    def fetch_rows(src, dst, sem, parts):
        size = dst.shape[0] // parts
        for k in range(parts):
            rows = pl.ds(k * size, size)
            pltpu.make_async_copy(src.at[rows], dst.at[rows], sem).start()

    def c_refs(b):
        return c_hbm.at[b, pl.ds(0, PREFIX), :], cbuf, c_sem

    def wq_refs(h):
        return wq_hbm.at[pl.ds(2 * h, 2)], wqb.at[h % 3], wq_sem.at[h % 3]

    def fetch_wq(i):
        src, dst, sem = wq_refs(i)
        for k in range(2):
            fetch_rows(src.at[k], dst.at[k], sem, 2)

    def wo_refs(g, n):
        return wo_hbm.at[:, at(n * CHUNK, CHUNK)], wob.at[g % 3], wo_sem.at[g % 3]

    def dq_refs(n):
        return wdq_hbm.at[at(n * DEPTH, DEPTH), :], kb.at[at((n % 4) * DEPTH, DEPTH), pl.ds(0, QR)], dq_sem.at[n % 4]

    def dkv_refs(n):
        return wdkvt_hbm.at[:, at(n * DEPTH, DEPTH)], vtb.at[pl.ds(0, 576), at((n % 4) * DEPTH, DEPTH)], dkv_sem.at[n % 4]

    def uk_copy(j):
        return pltpu.make_async_copy(wuk_hbm.at[at(WID * j, WID), :], kb.at[pl.ds(0, WID), at(QR + HD * j, HD)], wk_sem.at[j])

    def uv_copy(j):
        return pltpu.make_async_copy(wuv_hbm.at[at(1024 * j, 1024), :], vtb.at[pl.ds(1024, 1024), at(HD * j, HD)], wvt_sem.at[j])

    def piece(j):
        return at(HD * (j + 8), HD), pl.ds(1024, 1024)

    def x_copy(j):
        return pltpu.make_async_copy(x_hbm.at[:, at(1024 * j, 1024)], vtb.at[piece(j)], x_sem.at[j])

    def x_again(j):
        return pltpu.make_async_copy(x_hbm.at[:, at(1024 * j, 1024)], kb.at[at(HD * j, HD), pl.ds(0, 1024)], x_sem.at[j])

    for j in range(7):
        x_copy(j).start()
    for n in range(4):
        fetch_rows(*dq_refs(n), 2)
        fetch_rows(*dkv_refs(n), 2)

    barrier = pltpu.get_barrier_semaphore()
    for peer in (sib, far):
        pl.semaphore_signal(barrier, inc=1, device_id={"tp": peer}, device_id_type=MESH)

    aug = jnp.where(lax.broadcasted_iota(jnp.int32, (LOC, NEW), 0) == 0, 1.0, 0.0).astype(BF16)
    causal = lax.broadcasted_iota(jnp.int32, (NEW, NEW), 0) <= lax.broadcasted_iota(jnp.int32, (NEW, NEW), 1)
    for b in range(2):
        sb_a[pl.ds(NEW * b, NEW), :32] = cos[b].T
        sb_a[pl.ds(KVR + NEW * b, NEW), :32] = sin[b].T
    qa[...] = jnp.zeros_like(qa)
    kva[...] = jnp.zeros_like(kva)
    for j in range(7):
        x_copy(j).wait()

    def squares(j, acc):
        v = vtb[piece(j)].astype(F32)
        v = v * v
        return acc + sum(v[:, HD * k:HD * k + HD] for k in range(8))

    total = lax.fori_loop(0, 7, squares, jnp.zeros((HD, HD), F32))
    inv_x = lax.rsqrt(jnp.sum(total, axis=-1, keepdims=True) / 7168.0 + EPS)

    def scaled(j, carry):
        vtb[piece(j)] = (vtb[piece(j)].astype(F32) * inv_x * g1[:, at(1024 * j, 1024)]).astype(BF16)
        return carry

    lax.fori_loop(0, 7, scaled, 0)

    def project(n, carry):
        @pl.when((n >= 1) & (n + 3 < CHUNKS))
        def _():
            fetch_rows(*dq_refs(n + 3), 2)
            fetch_rows(*dkv_refs(n + 3), 2)

        pltpu.make_async_copy(*dq_refs(n)).wait()
        pltpu.make_async_copy(*dkv_refs(n)).wait()

        @pl.when(n == 4)
        def _():
            for j in range(4):
                uk_copy(j).start()
            for j in range(8):
                uv_copy(j).start()

        a = vtb[at(HD * (n // 2 + 8), HD), at(1024 + DEPTH * (n % 2), DEPTH)]
        slot = at((n % 4) * DEPTH, DEPTH)
        qa[...] += dot(a, kb[slot, :QR])
        kva[...] += dot_nt(a, vtb[:576, slot])

        @pl.when(n == CHUNKS - 3)
        def _():
            fetch_rows(*c_refs(0), 4)

        @pl.when(n >= CHUNKS - 4)
        def _():
            j = n - (CHUNKS - 4)
            uk_copy(j).wait()
            wkb[at(HD * j, HD), :] = kb[:WID, at(QR + HD * j, HD)].reshape(HD, WID)
            halves = []
            for k in range(2):
                uv_copy(2 * j + k).wait()
                halves.append(vtb[1024:WID, at(HD * (2 * j + k), HD)].reshape(LOC, WID))
            wvtb[:, at(HD * j, HD)] = jnp.concatenate(halves, axis=0).T

        return carry

    lax.fori_loop(0, CHUNKS, project, 0)
    for b in range(2):
        rows = slice(LOC * b, LOC * b + LOC)
        q = qa[rows, :]
        inv_q = lax.rsqrt(jnp.mean(q * q, axis=-1, keepdims=True) + EPS)
        lat[b, :, :QR] = (q * inv_q * gq[...]).astype(BF16)
        c = kva[rows, :KVR]
        inv_c = lax.rsqrt(jnp.mean(c * c, axis=-1, keepdims=True) + EPS)
        lat[b, :, QR:WID] = (c * inv_c * gkv[...]).astype(BF16)
        v1 = kva[rows, KVR:544]
        v2 = kva[rows, 544:576]
        own_cos = sb_a[at(NEW * b + me * LOC, LOC), :32]
        own_sin = sb_a[at(KVR + NEW * b + me * LOC, LOC), :32]
        rot = jnp.concatenate([v1 * own_cos - v2 * own_sin, v2 * own_cos + v1 * own_sin, jnp.zeros((LOC, LOC), F32)], axis=1)
        lat[b, :, WID:] = rot.astype(BF16)

    pl.semaphore_wait(barrier, 2)
    to_far = [remote(lat.at[b], latb.at[b, 1], lat_send.at[b, 1], lat_recv.at[b, 1], far) for b in range(2)]
    to_sib = [remote(lat.at[b], latb.at[b, 0], lat_send.at[b, 0], lat_recv.at[b, 0], sib) for b in range(2)]
    onward = [remote(latb.at[b, 1], latb.at[b, 2], lat_send.at[b, 2], lat_recv.at[b, 2], sib) for b in range(2)]
    to_far[0].start()
    to_sib[0].start()
    to_sib[1].start()
    for i in range(3):
        fetch_wq(i)
    for n in range(3):
        fetch_rows(*wo_refs(n, n), 4)
    def kv_start(b):
        length = len_ref[b]
        row = lax.broadcasted_iota(jnp.int32, (PREFIX, HD), 0)
        lane = lax.broadcasted_iota(jnp.int32, (PREFIX, HD), 1)
        old = row < length
        rot = pet[b, :, :PREFIX].astype(F32).T
        rot = jnp.concatenate([rot, jnp.zeros_like(rot)], axis=1)
        pe[:PREFIX, :] = jnp.where(old, rot, jnp.where(lane == LOC, NEG, 0.0)).astype(BF16)
        pltpu.make_async_copy(*c_refs(b)).wait()

    def kv_block(b, r, size):
        rows = at(r * size, size)
        row = lax.broadcasted_iota(jnp.int32, (size, HD), 0) + r * size
        m = jnp.where(row < len_ref[b], 1.0, 0.0).astype(BF16)
        c = cbuf[rows, :] * jnp.concatenate([m, m, m, m], axis=1)
        kb[rows, :] = dot(c, wkb[...]).astype(BF16)
        vtb[:, rows] = dot_nt(wvtb[...], c).astype(BF16)

    def assemble(b):
        cqa = ob.at[1]
        for src, owner in ((lat.at[b], me), (latb.at[b, 0], sib), (latb.at[b, 1], far), (latb.at[b, 2], diag)):
            rows = at(owner * LOC, LOC)
            cqa[rows, :QR] = src[:, :QR]
            cn[b, rows, :] = src[:, QR:WID]
            kn[rows, :] = src[:, WID:]
        cqt[...] = cqa[:, :QR].T
        knt[b] = kn[...].T[:LOC]
        pe[PREFIX:, :] = kn[...]
        kb[PREFIX:, :] = dot(cn[b], wkb[...]).astype(BF16)
        vtb[:, PREFIX:] = dot_nt(wvtb[...], cn[b]).astype(BF16)

    def query_pair(b, i):
        pltpu.make_async_copy(*wq_refs(i)).wait()
        cos_b = cos[b]
        sin_b = sin[b]
        for k in range(2):
            q = dot(wqb[i % 3, k, :, :CB], cqt[:CB, :]) + dot(wqb[i % 3, k, :, CB:], cqt[CB:, :])
            v1 = q[HD:160]
            v2 = q[160:]
            qt = jnp.concatenate([q[:HD].astype(BF16), (v1 * cos_b - v2 * sin_b).astype(BF16), (v2 * cos_b + v1 * sin_b).astype(BF16), aug], axis=0)
            q_lo[2 * i + k] = qt

        @pl.when(i + 3 < 8)
        def _():
            fetch_wq(i + 3)

    def attend(b, inside):
        if inside:
            query_pair(b, jnp.int32(0))

        halves = ((q_lo, range(5)), (q_hi, range(5, 9)))
        order = [(side, c) for c in range(5) for side, (_, blocks) in enumerate(halves) if c < len(blocks)]

        def score(h, k):
            d = at(h * HD, HD)
            best = [jnp.full((8, NEW), NEG, F32)] * 2
            for side, j in order:
                c = halves[side][1][j]
                rows = pl.ds(c * NEW, NEW)
                t = dot(jnp.concatenate([kb[rows, d], pe[rows, :]], axis=1), halves[side][0][(h, k)[side]])
                if c == 8:
                    t = jnp.where(causal, t, NEG)
                sb[k][rows, :] = t
                best[side] = jnp.maximum(best[side], jnp.max(t.reshape(32, 8, NEW), axis=0))
                yield
            mb[k] = jnp.maximum(*best)

        def finish(h, k):
            d = at(h * HD, HD)
            m = jnp.max(mb[k], axis=0, keepdims=True) * C2
            l8 = jnp.zeros((8, NEW), F32)
            for c in range(9):
                rows = pl.ds(c * NEW, NEW)
                p = jnp.exp2(sb[k][rows, :] * C2 - m)
                sb[k][rows, :] = p
                l8 = l8 + jnp.sum(p.reshape(32, 8, NEW), axis=0)
                yield
            inv = 1.0 / jnp.sum(l8, axis=0, keepdims=True)
            acc = [jnp.zeros((HD, NEW), F32)] * 2
            for side, j in order:
                rows = pl.ds(halves[side][1][j] * NEW, NEW)
                acc[side] = acc[side] + dot(vtb[d, rows], (sb[k][rows, :] * inv).astype(BF16))
                yield
            ob[b, :, d] = (acc[0] + acc[1]).T.astype(BF16)

        def weave(*parts):
            live = list(parts)
            while live:
                live = [part for part in live if next(part, live) is None]

        for k in range(2):
            q_hi[k] = q_lo[k]

        @pl.when(me >= 0)
        def _():
            weave(score(0, 0))

        def pair(i, carry):
            h = 2 * i
            if inside:
                @pl.when(i < 7)
                def _():
                    query_pair(b, i + 1)

            @pl.when(i >= 0)
            def _():
                weave(score(h + 1, 1), finish(h, 0))
                q_hi[0] = q_lo[jnp.minimum(h + 2, 15)]

            @pl.when(i < 8)
            def _():
                weave(score(jnp.minimum(h + 2, 15), 0), finish(h + 1, 1))
                q_hi[1] = q_lo[jnp.minimum(h + 3, 15)]

            return carry

        lax.fori_loop(0, 8, pair, 0)

    def to_sibling(b, n):
        return remote(stage_d.at[n % 4, 0], xbuf.at[b, n], d_send.at[n % 4], d_recv.at[b, n], sib)

    def over_link(b, n):
        return remote(stage_x.at[b, n], rbuf.at[b, n], i_send.at[b, n], i_recv.at[b, n], far)

    def put_y(n):
        return pltpu.make_async_copy(ybuf.at[n % 4], y_hbm.at[:, at(n * CHUNK, CHUNK)], y_sem.at[n % 4])

    def product(rows, g, n):
        pltpu.make_async_copy(*wo_refs(g, n)).wait()
        return dot(lhsb[:rows, :], wob[g % 3])

    def next_wo(g):
        @pl.when(g + 3 < 3 * CHUNKS)
        def _():
            fetch_rows(*wo_refs(g + 3, (g + 3) % CHUNKS), 4)

    def load_lhs(k, b, owner):
        lhsb[LOC * k:LOC * k + LOC, :] = ob[b, at(owner * LOC, LOC), :]

    def pass_on(b, n):
        to_sibling(b, n).wait_recv()
        stage_x[b, n] = stage_x[b, n] + xbuf[b, n]
        over_link(b, n).start()

    def far_start(b):
        load_lhs(0, b, far)
        load_lhs(1, b, diag)

    def far_chunk(b, n):
        g = b * CHUNKS + n
        y = product(HD, g, n)

        @pl.when(n >= 4)
        def _():
            to_sibling(b, n - 4).wait_send()

        stage_d[n % 4, 0] = y[LOC:]
        stage_x[b, n] = y[:LOC]
        to_sibling(b, n).start()
        next_wo(g)

        @pl.when(n == 1)
        def _():
            pass_on(b, 0)

        @pl.when(n >= 3)
        def _():
            pass_on(b, n - 2)

    def far_end(b):
        pass_on(b, CHUNKS - 2)
        pass_on(b, CHUNKS - 1)
        for n in range(CHUNKS - 4, CHUNKS):
            to_sibling(b, n).wait_send()

    def own_unit(unit):
        for n in range(4):
            over_link(0, n).wait_send()
        for b in range(2):
            load_lhs(b, b, me)
            load_lhs(2 + b, b, sib)

        def both(n):
            return remote(stage_d.at[n % 4], xbuf.at[:, n], d_send.at[n % 4], d_recv.at[0, n], sib)

        def finish(n):
            both(n).wait_recv()

            @pl.when(n >= 4)
            def _():
                put_y(n - 4).wait()

            for b in range(2):
                over_link(b, n).wait_recv()
                total = stage_x[0, 2 * (n % 2) + b] + xbuf[b, n] + rbuf[b, n]
                x = kb[at(HD * (n // 2) + LOC * b, LOC), at(CHUNK * (n % 2), CHUNK)]
                ybuf[n % 4, pl.ds(LOC * b, LOC), :] = (x.astype(F32) + total).astype(BF16)
            put_y(n).start()

        def chunk(n, carry):
            g = unit * CHUNKS + n
            y = product(NEW, g, n)

            @pl.when(n >= 4)
            def _():
                both(n - 4).wait_send()

            for b in range(2):
                stage_x[0, 2 * (n % 2) + b] = y[LOC * b:LOC * b + LOC]
                stage_d[n % 4, b] = y[HD + LOC * b:192 + LOC * b]
            both(n).start()
            next_wo(g)

            @pl.when(n >= 1)
            def _():
                finish(n - 1)

            return carry

        lax.fori_loop(0, CHUNKS, chunk, 0)
        finish(CHUNKS - 1)
        for n in range(CHUNKS - 4, CHUNKS):
            both(n).wait_send()
            put_y(n).wait()

    def first_block(r, carry):
        @pl.when(r == 3)
        def _():
            to_far[1].start()
            to_far[0].wait_recv()
            onward[0].start()

        kv_block(0, r, ROW_BLK)
        return carry

    def second_block(r, carry):
        n = 3 * r + 2
        far_chunk(0, n)
        query_pair(1, 2 * r)
        far_chunk(0, n + 1)
        query_pair(1, 2 * r + 1)
        far_chunk(0, n + 2)
        kv_block(1, r, ROW_BLK)
        return carry

    def far_only(b, n, carry):
        far_chunk(b, n)
        return carry

    kv_start(0)
    lax.fori_loop(0, PREFIX // ROW_BLK, first_block, 0)
    fetch_rows(*c_refs(1), 4)
    to_sib[0].wait_recv()
    onward[0].wait_recv()
    assemble(0)
    attend(0, True)
    for i in range(3):
        fetch_wq(i)
    to_far[1].wait_recv()
    onward[1].start()
    far_start(0)
    lax.fori_loop(0, 2, functools.partial(far_only, 0), 0)
    kv_start(1)
    to_sib[1].wait_recv()
    onward[1].wait_recv()
    assemble(1)
    lax.fori_loop(0, PREFIX // ROW_BLK, second_block, 0)
    far_end(0)
    put_c = pltpu.make_async_copy(cn, cnew_hbm, out_sem.at[0])
    put_k = pltpu.make_async_copy(knt, knewt_hbm, out_sem.at[1])
    put_c.start()
    put_k.start()
    attend(1, False)
    for j in range(7):
        x_again(j).start()
    far_start(1)
    lax.fori_loop(0, CHUNKS, functools.partial(far_only, 1), 0)
    far_end(1)
    pl.semaphore_signal(free_sem, inc=1, device_id={"tp": sib}, device_id_type=MESH)
    pl.semaphore_wait(free_sem, 1)
    for j in range(7):
        x_again(j).wait()
    own_unit(2)
    for b in range(2):
        to_far[b].wait_send()
        to_sib[b].wait_send()
        onward[b].wait_send()

        def drain(n, carry):
            over_link(b, n).wait_send()
            return carry

        lax.fori_loop((4, 0)[b], CHUNKS, drain, 0)
    put_c.wait()
    put_k.wait()


def main_call(lengths, *arrays):
    vmem = pl.BlockSpec(memory_space=pltpu.VMEM)
    hbm = pl.BlockSpec(memory_space=pl.ANY)
    dma = pltpu.SemaphoreType.DMA
    return pl.pallas_call(
        main_kernel,
        in_specs=[pl.BlockSpec(memory_space=pltpu.SMEM)] + [vmem] * 6 + [hbm] * 8,
        out_specs=[hbm] * 3,
        out_shape=[
            jax.ShapeDtypeStruct((HD, 7168), BF16),
            jax.ShapeDtypeStruct((2, NEW, KVR), BF16),
            jax.ShapeDtypeStruct((2, LOC, NEW), BF16),
        ],
        scratch_shapes=[
            pltpu.VMEM((2, LOC, LAT_W), BF16),
            pltpu.VMEM((HD, QR), F32),
            pltpu.VMEM((HD, 576), F32),
            pltpu.VMEM((2, 3, LOC, LAT_W), BF16),
            pltpu.VMEM((QR, NEW), BF16),
            pltpu.VMEM((2, NEW, KVR), BF16),
            pltpu.VMEM((NEW, HD), BF16),
            pltpu.VMEM((2, LOC, NEW), BF16),
            pltpu.VMEM((PREFIX + NEW, HD), BF16),
            pltpu.VMEM((PREFIX, KVR), BF16),
            pltpu.VMEM((PREFIX + NEW, WID), BF16),
            pltpu.VMEM((WID, PREFIX + NEW), BF16),
            pltpu.VMEM((KVR, WID), BF16),
            pltpu.VMEM((WID, KVR), BF16),
            pltpu.VMEM((3, 2, 192, QR), BF16),
            pltpu.VMEM((16, NEW, NEW), BF16),
            pltpu.VMEM((2, NEW, NEW), BF16),
            *[pltpu.VMEM((PREFIX + NEW, NEW), F32)] * 2,
            pltpu.VMEM((2, 8, NEW), F32),
            pltpu.VMEM((2, NEW, WID), BF16),
            pltpu.VMEM((NEW, WID), BF16),
            pltpu.VMEM((3, WID, CHUNK), BF16),
            pltpu.VMEM((4, 2, LOC, CHUNK), F32),
            *[pltpu.VMEM((2, CHUNKS, LOC, CHUNK), F32)] * 3,
            pltpu.VMEM((4, HD, CHUNK), BF16),
            *[dma((2, 3))] * 2,
            *[dma((4,))] * 2,
            dma,
            dma((4,)),
            dma((8,)),
            dma((4,)),
            dma((3,)),
            dma((7,)),
            dma((2,)),
            dma((4,)),
            dma((4,)),
            *[dma((2, CHUNKS))] * 3,
            pltpu.SemaphoreType.REGULAR,
        ],
        compiler_params=pltpu.CompilerParams(vmem_limit_bytes=VMEM_ALL, collective_id=0, has_side_effects=True),
        cost_estimate=cost(1e11, 200 * MIB),
        name="main",
    )(lengths, *arrays)


def solution(mesh):
    def local_step(hidden, lengths, rope_cos, rope_sin, cache_lat, cache_pe, norm_in, w_dq, norm_q, w_dkv, norm_kv, w_uq, w_uk, w_uv, w_out):
        pe_t = jnp.swapaxes(cache_pe, 1, 2)
        y, c_new, k_newt = main_call(
            lengths,
            jnp.swapaxes(rope_cos, 1, 2),
            jnp.swapaxes(rope_sin, 1, 2),
            pe_t,
            norm_in[None],
            norm_q,
            norm_kv[None],
            hidden.reshape(HD, 7168),
            w_dq,
            w_dkv.T,
            cache_lat,
            w_uk.reshape(8192, HD),
            w_uv.reshape(8192, HD),
            jnp.transpose(w_uq, (1, 2, 0)),
            w_out,
        )
        y, lat_new, pe_new = update_caches(lengths, y, cache_lat, pe_t, c_new, k_newt)
        return y.reshape(hidden.shape), lat_new, jnp.swapaxes(pe_new, 1, 2)

    spec_tok = P("dp", "tp", None)
    spec_len = P("dp")
    spec_seq = P("dp", None, None)
    spec_vec = P(None)
    spec_mat = P(None, None)
    spec_head = P(None, "tp", None)
    spec_rows = P("tp", None)
    in_specs = (spec_tok, spec_len, spec_seq, spec_seq, spec_seq, spec_seq, spec_vec, spec_mat, spec_vec, spec_mat, spec_vec, spec_head, spec_head, spec_head, spec_rows)
    return jax.shard_map(local_step, mesh=mesh, in_specs=in_specs, out_specs=(spec_tok, spec_seq, spec_seq), check_vma=False)
```

```python
import functools

import jax
import jax.numpy as jnp
from jax import lax
from jax.experimental import pallas as pl
from jax.experimental.pallas import tpu as pltpu
from jax.sharding import PartitionSpec as P

F32 = jnp.float32
BF16 = jnp.bfloat16
EPS = 1e-6
MIB = 1 << 20
VMEM_ALL = 67043328
MESH = pl.DeviceIdType.MESH
LAT_W = 2176
PREFIX = 2048
ROW_BLK = 512
CHUNK = 512
DEPTH = 512
CHUNKS = 7168 // CHUNK
C2 = 192.0 ** -0.5 * 1.4426950408889634
NEG = -1e30
LOC = 64
HD = 128
NEW = 256
QR = 1536
WID = 2048
CB = 768
KVR = 512
NT = (((1,), (1,)), ((), ()))


def dot(lhs, rhs):
    return jnp.dot(lhs, rhs, preferred_element_type=F32)


def dot_nt(lhs, rhs):
    return lax.dot_general(lhs, rhs, NT, preferred_element_type=F32)


def cost(flops, nbytes):
    return pl.CostEstimate(flops=int(flops), bytes_accessed=int(nbytes), transcendentals=0)


def cache_kernel(len_ref, y_hbm, c_hbm, pe_hbm, cn_hbm, kn_hbm, yo_hbm, co_hbm, po_hbm, y, rows, cols, cn, kn, in_sem, out_sem, side_sem, y_sem):
    blocks = rows.shape[1] // NEW
    span = lambda r: pl.ds(r * NEW, NEW)
    lat_in = lambda b, r: pltpu.make_async_copy(c_hbm.at[b, span(r)], rows.at[b, span(r)], in_sem.at[b, r])
    lat_out = lambda b, r: pltpu.make_async_copy(rows.at[b, span(r)], co_hbm.at[b, span(r)], out_sem.at[b, r])
    pe_in = lambda b: pltpu.make_async_copy(pe_hbm.at[b], cols.at[b], in_sem.at[b, blocks])
    pe_out = lambda b: pltpu.make_async_copy(cols.at[b], po_hbm.at[b], out_sem.at[b, blocks])
    new_in = [pltpu.make_async_copy(cn_hbm, cn, side_sem.at[0]), pltpu.make_async_copy(kn_hbm, kn, side_sem.at[1])]
    part = lambda k: pl.ds(32 * k, 32)
    y_in = [pltpu.make_async_copy(y_hbm.at[part(k)], y.at[part(k)], y_sem.at[k]) for k in range(4)]
    y_out = [pltpu.make_async_copy(y.at[part(k)], yo_hbm.at[part(k)], y_sem.at[4 + k]) for k in range(4)]
    places = [(b, r) for b in range(2) for r in range(blocks)]
    for copy in new_in:
        copy.start()
    for b, r in places:
        lat_in(b, r).start()
    for b in range(2):
        pe_in(b).start()
    for copy in y_in:
        copy.start()
    for copy in new_in:
        copy.wait()
    for b, r in places:
        shift = r * NEW - len_ref[b]
        lat_in(b, r).wait()

        @pl.when((shift < NEW) & (shift > -NEW))
        def _():
            row = lax.broadcasted_iota(jnp.int32, (NEW, NEW), 0) + shift
            hot = (row == lax.broadcasted_iota(jnp.int32, (NEW, NEW), 1)).astype(F32).astype(BF16)
            row = lax.broadcasted_iota(jnp.int32, (NEW, KVR), 0) + shift
            old = rows[b, span(r), :].astype(F32)
            rows[b, span(r), :] = jnp.where((row >= 0) & (row < NEW), dot(hot, cn[b]), old).astype(BF16)

        lat_out(b, r).start()
    for b in range(2):
        pe_in(b).wait()
        for r in range(blocks):
            shift = r * NEW - len_ref[b]

            @pl.when((shift < NEW) & (shift > -NEW))
            def _():
                row = lax.broadcasted_iota(jnp.int32, (NEW, NEW), 0) + shift
                hot = (row == lax.broadcasted_iota(jnp.int32, (NEW, NEW), 1)).astype(F32).astype(BF16)
                col = lax.broadcasted_iota(jnp.int32, (LOC, NEW), 1) + shift
                old = cols[b, :, span(r)].astype(F32)
                cols[b, :, span(r)] = jnp.where((col >= 0) & (col < NEW), dot_nt(kn[b], hot), old).astype(BF16)

        pe_out(b).start()
    for k in range(4):
        y_in[k].wait()
        y_out[k].start()
    for b, r in places:
        lat_out(b, r).wait()
    for copy in y_out:
        copy.wait()
    for b in range(2):
        pe_out(b).wait()


def update_caches(lengths, y, cache_lat, pe_t, c_new, k_newt):
    hbm = pl.BlockSpec(memory_space=pl.ANY)
    sems = pltpu.SemaphoreType.DMA((2, cache_lat.shape[1] // NEW + 1))
    return pl.pallas_call(
        cache_kernel,
        in_specs=[pl.BlockSpec(memory_space=pltpu.SMEM)] + [hbm] * 5,
        out_specs=[hbm] * 3,
        out_shape=[jax.ShapeDtypeStruct(v.shape, BF16) for v in (y, cache_lat, pe_t)],
        scratch_shapes=[*[pltpu.VMEM(v.shape, BF16) for v in (y, cache_lat, pe_t, c_new, k_newt)], sems, sems, pltpu.SemaphoreType.DMA((2,)), pltpu.SemaphoreType.DMA((8,))],
        compiler_params=pltpu.CompilerParams(vmem_limit_bytes=VMEM_ALL),
        cost_estimate=cost(4e9, 12 * MIB),
        name="caches",
    )(lengths, y, cache_lat, pe_t, c_new, k_newt)


def at(start, size):
    return pl.ds(pl.multiple_of(start, size), size)


def main_kernel(len_ref, cos, sin, pet, g1, gq, gkv, x_hbm, wdq_hbm, wdkvt_hbm, c_hbm, wuk_hbm, wuv_hbm, wq_hbm, wo_hbm,
                y_hbm, cnew_hbm, knewt_hbm,
                lat, qa, kva, latb, cqt, cn, kn, knt, pe, cbuf, kb, vtb, wkb, wvtb, wqb, q_lo, q_hi, sb_a, sb_b, mb, ob, lhsb, wob,
                stage_d, xbuf, stage_x, rbuf, ybuf,
                lat_send, lat_recv, dq_sem, dkv_sem, c_sem, wk_sem, wvt_sem, wq_sem, wo_sem, x_sem, out_sem, y_sem,
                d_send, d_recv, i_send, i_recv, free_sem):
    sb = (sb_a, sb_b)
    me = lax.axis_index("tp")
    chip = me // 2
    core = me % 2
    sib = 2 * chip + (1 - core)
    far = 2 * (1 - chip) + core
    diag = 2 * (1 - chip) + (1 - core)

    def remote(src, dst, send, recv, peer):
        return pltpu.make_async_remote_copy(src_ref=src, dst_ref=dst, send_sem=send, recv_sem=recv, device_id={"tp": peer}, device_id_type=MESH)

    def fetch_rows(src, dst, sem, parts):
        size = dst.shape[0] // parts
        for k in range(parts):
            rows = pl.ds(k * size, size)
            pltpu.make_async_copy(src.at[rows], dst.at[rows], sem).start()

    def c_refs(b):
        return c_hbm.at[b, pl.ds(0, PREFIX), :], cbuf, c_sem

    def wq_refs(h):
        return wq_hbm.at[pl.ds(2 * h, 2)], wqb.at[h % 3], wq_sem.at[h % 3]

    def fetch_wq(i):
        src, dst, sem = wq_refs(i)
        for k in range(2):
            fetch_rows(src.at[k], dst.at[k], sem, 2)

    def wo_refs(g, n):
        return wo_hbm.at[:, at(n * CHUNK, CHUNK)], wob.at[g % 3], wo_sem.at[g % 3]

    def dq_refs(n):
        return wdq_hbm.at[at(n * DEPTH, DEPTH), :], kb.at[at((n % 4) * DEPTH, DEPTH), pl.ds(0, QR)], dq_sem.at[n % 4]

    def dkv_refs(n):
        return wdkvt_hbm.at[:, at(n * DEPTH, DEPTH)], vtb.at[pl.ds(0, 576), at((n % 4) * DEPTH, DEPTH)], dkv_sem.at[n % 4]

    def uk_copy(j):
        return pltpu.make_async_copy(wuk_hbm.at[at(WID * j, WID), :], kb.at[pl.ds(0, WID), at(QR + HD * j, HD)], wk_sem.at[j])

    def uv_copy(j):
        return pltpu.make_async_copy(wuv_hbm.at[at(1024 * j, 1024), :], vtb.at[pl.ds(1024, 1024), at(HD * j, HD)], wvt_sem.at[j])

    def piece(j):
        return at(HD * (j + 8), HD), pl.ds(1024, 1024)

    def x_copy(j):
        return pltpu.make_async_copy(x_hbm.at[:, at(1024 * j, 1024)], vtb.at[piece(j)], x_sem.at[j])

    def x_again(j):
        return pltpu.make_async_copy(x_hbm.at[:, at(1024 * j, 1024)], kb.at[at(HD * j, HD), pl.ds(0, 1024)], x_sem.at[j])

    for j in range(7):
        x_copy(j).start()
    for n in range(4):
        fetch_rows(*dq_refs(n), 2)
        fetch_rows(*dkv_refs(n), 2)

    barrier = pltpu.get_barrier_semaphore()
    for peer in (sib, far):
        pl.semaphore_signal(barrier, inc=1, device_id={"tp": peer}, device_id_type=MESH)

    aug = jnp.where(lax.broadcasted_iota(jnp.int32, (LOC, NEW), 0) == 0, 1.0, 0.0).astype(BF16)
    causal = lax.broadcasted_iota(jnp.int32, (NEW, NEW), 0) <= lax.broadcasted_iota(jnp.int32, (NEW, NEW), 1)
    for b in range(2):
        sb_a[pl.ds(NEW * b, NEW), :32] = cos[b].T
        sb_a[pl.ds(KVR + NEW * b, NEW), :32] = sin[b].T
    qa[...] = jnp.zeros_like(qa)
    kva[...] = jnp.zeros_like(kva)
    for j in range(7):
        x_copy(j).wait()

    def squares(j, acc):
        v = vtb[piece(j)].astype(F32)
        v = v * v
        return acc + sum(v[:, HD * k:HD * k + HD] for k in range(8))

    total = lax.fori_loop(0, 7, squares, jnp.zeros((HD, HD), F32))
    inv_x = lax.rsqrt(jnp.sum(total, axis=-1, keepdims=True) / 7168.0 + EPS)

    def scaled(j, carry):
        vtb[piece(j)] = (vtb[piece(j)].astype(F32) * inv_x * g1[:, at(1024 * j, 1024)]).astype(BF16)
        return carry

    lax.fori_loop(0, 7, scaled, 0)

    def project(n, carry):
        @pl.when((n >= 1) & (n + 3 < CHUNKS))
        def _():
            fetch_rows(*dq_refs(n + 3), 2)
            fetch_rows(*dkv_refs(n + 3), 2)

        pltpu.make_async_copy(*dq_refs(n)).wait()
        pltpu.make_async_copy(*dkv_refs(n)).wait()

        @pl.when(n == 4)
        def _():
            for j in range(4):
                uk_copy(j).start()
            for j in range(8):
                uv_copy(j).start()

        a = vtb[at(HD * (n // 2 + 8), HD), at(1024 + DEPTH * (n % 2), DEPTH)]
        slot = at((n % 4) * DEPTH, DEPTH)
        qa[...] += dot(a, kb[slot, :QR])
        kva[...] += dot_nt(a, vtb[:576, slot])

        @pl.when(n == CHUNKS - 3)
        def _():
            fetch_rows(*c_refs(0), 4)

        @pl.when(n >= CHUNKS - 4)
        def _():
            j = n - (CHUNKS - 4)
            uk_copy(j).wait()
            wkb[at(HD * j, HD), :] = kb[:WID, at(QR + HD * j, HD)].reshape(HD, WID)
            halves = []
            for k in range(2):
                uv_copy(2 * j + k).wait()
                halves.append(vtb[1024:WID, at(HD * (2 * j + k), HD)].reshape(LOC, WID))
            wvtb[:, at(HD * j, HD)] = jnp.concatenate(halves, axis=0).T

        return carry

    lax.fori_loop(0, CHUNKS, project, 0)
    for b in range(2):
        rows = slice(LOC * b, LOC * b + LOC)
        q = qa[rows, :]
        inv_q = lax.rsqrt(jnp.mean(q * q, axis=-1, keepdims=True) + EPS)
        lat[b, :, :QR] = (q * inv_q * gq[...]).astype(BF16)
        c = kva[rows, :KVR]
        inv_c = lax.rsqrt(jnp.mean(c * c, axis=-1, keepdims=True) + EPS)
        lat[b, :, QR:WID] = (c * inv_c * gkv[...]).astype(BF16)
        v1 = kva[rows, KVR:544]
        v2 = kva[rows, 544:576]
        own_cos = sb_a[at(NEW * b + me * LOC, LOC), :32]
        own_sin = sb_a[at(KVR + NEW * b + me * LOC, LOC), :32]
        rot = jnp.concatenate([v1 * own_cos - v2 * own_sin, v2 * own_cos + v1 * own_sin, jnp.zeros((LOC, LOC), F32)], axis=1)
        lat[b, :, WID:] = rot.astype(BF16)

    pl.semaphore_wait(barrier, 2)
    to_far = [remote(lat.at[b], latb.at[b, 1], lat_send.at[b, 1], lat_recv.at[b, 1], far) for b in range(2)]
    to_sib = [remote(lat.at[b], latb.at[b, 0], lat_send.at[b, 0], lat_recv.at[b, 0], sib) for b in range(2)]
    onward = [remote(latb.at[b, 1], latb.at[b, 2], lat_send.at[b, 2], lat_recv.at[b, 2], sib) for b in range(2)]
    to_far[0].start()
    to_sib[0].start()
    to_sib[1].start()
    for i in range(3):
        fetch_wq(i)
    for n in range(3):
        fetch_rows(*wo_refs(n, n), 4)
    def kv_start(b):
        length = len_ref[b]
        row = lax.broadcasted_iota(jnp.int32, (PREFIX, HD), 0)
        lane = lax.broadcasted_iota(jnp.int32, (PREFIX, HD), 1)
        old = row < length
        rot = pet[b, :, :PREFIX].astype(F32).T
        rot = jnp.concatenate([rot, jnp.zeros_like(rot)], axis=1)
        pe[:PREFIX, :] = jnp.where(old, rot, jnp.where(lane == LOC, NEG, 0.0)).astype(BF16)
        pltpu.make_async_copy(*c_refs(b)).wait()

    def kv_block(b, r, size):
        rows = at(r * size, size)
        row = lax.broadcasted_iota(jnp.int32, (size, HD), 0) + r * size
        m = jnp.where(row < len_ref[b], 1.0, 0.0).astype(BF16)
        c = cbuf[rows, :] * jnp.concatenate([m, m, m, m], axis=1)
        kb[rows, :] = dot(c, wkb[...]).astype(BF16)
        vtb[:, rows] = dot_nt(wvtb[...], c).astype(BF16)

    def assemble(b):
        cqa = ob.at[1]
        for src, owner in ((lat.at[b], me), (latb.at[b, 0], sib), (latb.at[b, 1], far), (latb.at[b, 2], diag)):
            rows = at(owner * LOC, LOC)
            cqa[rows, :QR] = src[:, :QR]
            cn[b, rows, :] = src[:, QR:WID]
            kn[rows, :] = src[:, WID:]
        cqt[...] = cqa[:, :QR].T
        knt[b] = kn[...].T[:LOC]
        pe[PREFIX:, :] = kn[...]
        kb[PREFIX:, :] = dot(cn[b], wkb[...]).astype(BF16)
        vtb[:, PREFIX:] = dot_nt(wvtb[...], cn[b]).astype(BF16)

    def query(b, i):
        cos_b = cos[b]
        sin_b = sin[b]
        for k in range(2):
            q = dot(wqb[i % 3, k, :, :CB], cqt[:CB, :]) + dot(wqb[i % 3, k, :, CB:], cqt[CB:, :])
            v1 = q[HD:160]
            v2 = q[160:]
            qt = jnp.concatenate([q[:HD].astype(BF16), (v1 * cos_b - v2 * sin_b).astype(BF16), (v2 * cos_b + v1 * sin_b).astype(BF16), aug], axis=0)
            q_lo[2 * i + k] = qt
            if k == 0:
                q_hi[0] = qt
            yield

    def attend(b):
        def weave(*parts):
            live = list(parts)
            while live:
                live = [part for part in live if next(part, live) is None]

        pltpu.make_async_copy(*wq_refs(0)).wait()
        weave(query(b, jnp.int32(0)))
        fetch_wq(3)
        halves = ((q_lo, range(5)), (q_hi, range(5, 9)))
        order = [(side, c) for c in range(5) for side, (_, blocks) in enumerate(halves) if c < len(blocks)]

        def score(h, k):
            d = at(h * HD, HD)
            best = [jnp.full((8, NEW), NEG, F32)] * 2
            for side, j in order:
                c = halves[side][1][j]
                rows = pl.ds(c * NEW, NEW)
                t = dot(jnp.concatenate([kb[rows, d], pe[rows, :]], axis=1), halves[side][0][(h, k)[side]])
                if c == 8:
                    t = jnp.where(causal, t, NEG)
                sb[k][rows, :] = t
                best[side] = jnp.maximum(best[side], jnp.max(t.reshape(32, 8, NEW), axis=0))
                yield
            mb[k] = jnp.maximum(*best)

        def finish(h, k):
            d = at(h * HD, HD)
            m = jnp.max(mb[k], axis=0, keepdims=True) * C2
            l8 = jnp.zeros((8, NEW), F32)
            for c in range(9):
                rows = pl.ds(c * NEW, NEW)
                p = jnp.exp2(sb[k][rows, :] * C2 - m)
                sb[k][rows, :] = p
                l8 = l8 + jnp.sum(p.reshape(32, 8, NEW), axis=0)
                yield
            inv = 1.0 / jnp.sum(l8, axis=0, keepdims=True)
            acc = [jnp.zeros((HD, NEW), F32)] * 2
            for side, j in order:
                rows = pl.ds(halves[side][1][j] * NEW, NEW)
                acc[side] = acc[side] + dot(vtb[d, rows], (sb[k][rows, :] * inv).astype(BF16))
                yield
            ob[b, :, d] = (acc[0] + acc[1]).T.astype(BF16)

        @pl.when(me >= 0)
        def _():
            weave(score(0, 0))
            q_hi[1] = q_lo[1]

        def pair(i, carry):
            h = 2 * i
            later = jnp.minimum(i + 1, 7)

            @pl.when(i < 7)
            def _():
                pltpu.make_async_copy(*wq_refs(i + 1)).wait()

            weave(score(h + 1, 1), finish(h, 0), query(b, later))

            @pl.when(i + 4 < 8)
            def _():
                fetch_wq(i + 4)

            weave(score(2 * later, 0), finish(h + 1, 1))
            q_hi[1] = q_lo[2 * later + 1]
            return carry

        lax.fori_loop(0, 8, pair, 0)

    def to_sibling(b, n):
        return remote(stage_d.at[n % 4, 0], xbuf.at[b, n], d_send.at[n % 4], d_recv.at[b, n], sib)

    def over_link(b, n):
        return remote(stage_x.at[b, n], rbuf.at[b, n], i_send.at[b, n], i_recv.at[b, n], far)

    def put_y(n):
        return pltpu.make_async_copy(ybuf.at[n % 4], y_hbm.at[:, at(n * CHUNK, CHUNK)], y_sem.at[n % 4])

    def product(rows, g, n):
        pltpu.make_async_copy(*wo_refs(g, n)).wait()
        return dot(lhsb[:rows, :], wob[g % 3])

    def next_wo(g):
        @pl.when(g + 3 < 3 * CHUNKS)
        def _():
            fetch_rows(*wo_refs(g + 3, (g + 3) % CHUNKS), 4)

    def load_lhs(k, b, owner):
        lhsb[LOC * k:LOC * k + LOC, :] = ob[b, at(owner * LOC, LOC), :]

    def pass_on(b, n):
        to_sibling(b, n).wait_recv()
        stage_x[b, n] = stage_x[b, n] + xbuf[b, n]
        over_link(b, n).start()

    def far_start(b):
        load_lhs(0, b, far)
        load_lhs(1, b, diag)

    def far_chunk(b, n):
        g = b * CHUNKS + n
        y = product(HD, g, n)

        @pl.when(n >= 4)
        def _():
            to_sibling(b, n - 4).wait_send()

        stage_d[n % 4, 0] = y[LOC:]
        stage_x[b, n] = y[:LOC]
        to_sibling(b, n).start()
        next_wo(g)

        @pl.when(n == 1)
        def _():
            pass_on(b, 0)

        @pl.when(n >= 3)
        def _():
            pass_on(b, n - 2)

    def far_end(b):
        pass_on(b, CHUNKS - 2)
        pass_on(b, CHUNKS - 1)
        for n in range(CHUNKS - 4, CHUNKS):
            to_sibling(b, n).wait_send()

    def own_unit(unit):
        for n in range(4):
            over_link(0, n).wait_send()
        for b in range(2):
            load_lhs(b, b, me)
            load_lhs(2 + b, b, sib)

        def both(n):
            return remote(stage_d.at[n % 4], xbuf.at[:, n], d_send.at[n % 4], d_recv.at[0, n], sib)

        def finish(n):
            both(n).wait_recv()

            @pl.when(n >= 4)
            def _():
                put_y(n - 4).wait()

            for b in range(2):
                over_link(b, n).wait_recv()
                total = stage_x[0, 2 * (n % 2) + b] + xbuf[b, n] + rbuf[b, n]
                x = kb[at(HD * (n // 2) + LOC * b, LOC), at(CHUNK * (n % 2), CHUNK)]
                ybuf[n % 4, pl.ds(LOC * b, LOC), :] = (x.astype(F32) + total).astype(BF16)
            put_y(n).start()

        def chunk(n, carry):
            g = unit * CHUNKS + n
            y = product(NEW, g, n)

            @pl.when(n >= 4)
            def _():
                both(n - 4).wait_send()

            for b in range(2):
                stage_x[0, 2 * (n % 2) + b] = y[LOC * b:LOC * b + LOC]
                stage_d[n % 4, b] = y[HD + LOC * b:192 + LOC * b]
            both(n).start()
            next_wo(g)

            @pl.when(n >= 1)
            def _():
                finish(n - 1)

            return carry

        lax.fori_loop(0, CHUNKS, chunk, 0)
        finish(CHUNKS - 1)
        for n in range(CHUNKS - 4, CHUNKS):
            both(n).wait_send()
            put_y(n).wait()

    def first_block(r, carry):
        @pl.when(r == 3)
        def _():
            to_far[1].start()
            to_far[0].wait_recv()
            onward[0].start()

        kv_block(0, r, ROW_BLK)
        return carry

    def second_block(r, carry):
        n = 3 * r + 2
        far_chunk(0, n)
        far_chunk(0, n + 1)
        far_chunk(0, n + 2)
        kv_block(1, r, ROW_BLK)
        return carry

    def far_only(b, n, carry):
        far_chunk(b, n)
        return carry

    kv_start(0)
    lax.fori_loop(0, PREFIX // ROW_BLK, first_block, 0)
    fetch_rows(*c_refs(1), 4)
    to_sib[0].wait_recv()
    onward[0].wait_recv()
    assemble(0)
    attend(0)
    for i in range(3):
        fetch_wq(i)
    to_far[1].wait_recv()
    onward[1].start()
    far_start(0)
    lax.fori_loop(0, 2, functools.partial(far_only, 0), 0)
    kv_start(1)
    to_sib[1].wait_recv()
    onward[1].wait_recv()
    assemble(1)
    lax.fori_loop(0, PREFIX // ROW_BLK, second_block, 0)
    far_end(0)
    put_c = pltpu.make_async_copy(cn, cnew_hbm, out_sem.at[0])
    put_k = pltpu.make_async_copy(knt, knewt_hbm, out_sem.at[1])
    put_c.start()
    put_k.start()
    attend(1)
    for j in range(7):
        x_again(j).start()
    far_start(1)
    lax.fori_loop(0, CHUNKS, functools.partial(far_only, 1), 0)
    far_end(1)
    pl.semaphore_signal(free_sem, inc=1, device_id={"tp": sib}, device_id_type=MESH)
    pl.semaphore_wait(free_sem, 1)
    for j in range(7):
        x_again(j).wait()
    own_unit(2)
    for b in range(2):
        to_far[b].wait_send()
        to_sib[b].wait_send()
        onward[b].wait_send()

        def drain(n, carry):
            over_link(b, n).wait_send()
            return carry

        lax.fori_loop((4, 0)[b], CHUNKS, drain, 0)
    put_c.wait()
    put_k.wait()


def main_call(lengths, *arrays):
    vmem = pl.BlockSpec(memory_space=pltpu.VMEM)
    hbm = pl.BlockSpec(memory_space=pl.ANY)
    dma = pltpu.SemaphoreType.DMA
    return pl.pallas_call(
        main_kernel,
        in_specs=[pl.BlockSpec(memory_space=pltpu.SMEM)] + [vmem] * 6 + [hbm] * 8,
        out_specs=[hbm] * 3,
        out_shape=[
            jax.ShapeDtypeStruct((HD, 7168), BF16),
            jax.ShapeDtypeStruct((2, NEW, KVR), BF16),
            jax.ShapeDtypeStruct((2, LOC, NEW), BF16),
        ],
        scratch_shapes=[
            pltpu.VMEM((2, LOC, LAT_W), BF16),
            pltpu.VMEM((HD, QR), F32),
            pltpu.VMEM((HD, 576), F32),
            pltpu.VMEM((2, 3, LOC, LAT_W), BF16),
            pltpu.VMEM((QR, NEW), BF16),
            pltpu.VMEM((2, NEW, KVR), BF16),
            pltpu.VMEM((NEW, HD), BF16),
            pltpu.VMEM((2, LOC, NEW), BF16),
            pltpu.VMEM((PREFIX + NEW, HD), BF16),
            pltpu.VMEM((PREFIX, KVR), BF16),
            pltpu.VMEM((PREFIX + NEW, WID), BF16),
            pltpu.VMEM((WID, PREFIX + NEW), BF16),
            pltpu.VMEM((KVR, WID), BF16),
            pltpu.VMEM((WID, KVR), BF16),
            pltpu.VMEM((3, 2, 192, QR), BF16),
            pltpu.VMEM((16, NEW, NEW), BF16),
            pltpu.VMEM((2, NEW, NEW), BF16),
            *[pltpu.VMEM((PREFIX + NEW, NEW), F32)] * 2,
            pltpu.VMEM((2, 8, NEW), F32),
            pltpu.VMEM((2, NEW, WID), BF16),
            pltpu.VMEM((NEW, WID), BF16),
            pltpu.VMEM((3, WID, CHUNK), BF16),
            pltpu.VMEM((4, 2, LOC, CHUNK), F32),
            *[pltpu.VMEM((2, CHUNKS, LOC, CHUNK), F32)] * 3,
            pltpu.VMEM((4, HD, CHUNK), BF16),
            *[dma((2, 3))] * 2,
            *[dma((4,))] * 2,
            dma,
            dma((4,)),
            dma((8,)),
            dma((4,)),
            dma((3,)),
            dma((7,)),
            dma((2,)),
            dma((4,)),
            dma((4,)),
            *[dma((2, CHUNKS))] * 3,
            pltpu.SemaphoreType.REGULAR,
        ],
        compiler_params=pltpu.CompilerParams(vmem_limit_bytes=VMEM_ALL, collective_id=0, has_side_effects=True),
        cost_estimate=cost(1e11, 200 * MIB),
        name="main",
    )(lengths, *arrays)


def solution(mesh):
    def local_step(hidden, lengths, rope_cos, rope_sin, cache_lat, cache_pe, norm_in, w_dq, norm_q, w_dkv, norm_kv, w_uq, w_uk, w_uv, w_out):
        pe_t = jnp.swapaxes(cache_pe, 1, 2)
        y, c_new, k_newt = main_call(
            lengths,
            jnp.swapaxes(rope_cos, 1, 2),
            jnp.swapaxes(rope_sin, 1, 2),
            pe_t,
            norm_in[None],
            norm_q,
            norm_kv[None],
            hidden.reshape(HD, 7168),
            w_dq,
            w_dkv.T,
            cache_lat,
            w_uk.reshape(8192, HD),
            w_uv.reshape(8192, HD),
            jnp.transpose(w_uq, (1, 2, 0)),
            w_out,
        )
        y, lat_new, pe_new = update_caches(lengths, y, cache_lat, pe_t, c_new, k_newt)
        return y.reshape(hidden.shape), lat_new, jnp.swapaxes(pe_new, 1, 2)

    spec_tok = P("dp", "tp", None)
    spec_len = P("dp")
    spec_seq = P("dp", None, None)
    spec_vec = P(None)
    spec_mat = P(None, None)
    spec_head = P(None, "tp", None)
    spec_rows = P("tp", None)
    in_specs = (spec_tok, spec_len, spec_seq, spec_seq, spec_seq, spec_seq, spec_vec, spec_mat, spec_vec, spec_mat, spec_vec, spec_head, spec_head, spec_head, spec_rows)
    return jax.shard_map(local_step, mesh=mesh, in_specs=in_specs, out_specs=(spec_tok, spec_seq, spec_seq), check_vma=False)
```

```python
import functools

import jax
import jax.numpy as jnp
from jax import lax
from jax.experimental import pallas as pl
from jax.experimental.pallas import tpu as pltpu
from jax.sharding import PartitionSpec as P

F32 = jnp.float32
BF16 = jnp.bfloat16
EPS = 1e-6
MIB = 1 << 20
VMEM_ALL = 67043328
MESH = pl.DeviceIdType.MESH
LAT_W = 2176
PREFIX = 2048
ROW_BLK = 512
CHUNK = 512
DEPTH = 512
CHUNKS = 7168 // CHUNK
C2 = 192.0 ** -0.5 * 1.4426950408889634
NEG = -1e30
LOC = 64
HD = 128
NEW = 256
QR = 1536
WID = 2048
CB = 768
KVR = 512
NT = (((1,), (1,)), ((), ()))


def dot(lhs, rhs):
    return jnp.dot(lhs, rhs, preferred_element_type=F32)


def dot_nt(lhs, rhs):
    return lax.dot_general(lhs, rhs, NT, preferred_element_type=F32)


def cost(flops, nbytes):
    return pl.CostEstimate(flops=int(flops), bytes_accessed=int(nbytes), transcendentals=0)


def cache_kernel(len_ref, y_hbm, c_hbm, pe_hbm, cn_hbm, kn_hbm, yo_hbm, co_hbm, po_hbm, y, rows, cols, cn, kn, in_sem, out_sem, side_sem, y_sem):
    blocks = rows.shape[1] // NEW
    span = lambda r: pl.ds(r * NEW, NEW)
    lat_in = lambda b, r: pltpu.make_async_copy(c_hbm.at[b, span(r)], rows.at[b, span(r)], in_sem.at[b, r])
    lat_out = lambda b, r: pltpu.make_async_copy(rows.at[b, span(r)], co_hbm.at[b, span(r)], out_sem.at[b, r])
    pe_in = lambda b: pltpu.make_async_copy(pe_hbm.at[b], cols.at[b], in_sem.at[b, blocks])
    pe_out = lambda b: pltpu.make_async_copy(cols.at[b], po_hbm.at[b], out_sem.at[b, blocks])
    new_in = [pltpu.make_async_copy(cn_hbm, cn, side_sem.at[0]), pltpu.make_async_copy(kn_hbm, kn, side_sem.at[1])]
    part = lambda k: pl.ds(32 * k, 32)
    y_in = [pltpu.make_async_copy(y_hbm.at[part(k)], y.at[part(k)], y_sem.at[k]) for k in range(4)]
    y_out = [pltpu.make_async_copy(y.at[part(k)], yo_hbm.at[part(k)], y_sem.at[4 + k]) for k in range(4)]
    places = [(b, r) for b in range(2) for r in range(blocks)]
    for copy in new_in:
        copy.start()
    for copy in y_in:
        copy.start()
    for b, r in places:
        lat_in(b, r).start()
    for b in range(2):
        pe_in(b).start()
    for copy in new_in:
        copy.wait()
    for k in range(4):
        y_in[k].wait()
        y_out[k].start()
    for b, r in places:
        shift = r * NEW - len_ref[b]
        lat_in(b, r).wait()

        @pl.when((shift < NEW) & (shift > -NEW))
        def _():
            row = lax.broadcasted_iota(jnp.int32, (NEW, NEW), 0) + shift
            hot = (row == lax.broadcasted_iota(jnp.int32, (NEW, NEW), 1)).astype(F32).astype(BF16)
            row = lax.broadcasted_iota(jnp.int32, (NEW, KVR), 0) + shift
            old = rows[b, span(r), :].astype(F32)
            rows[b, span(r), :] = jnp.where((row >= 0) & (row < NEW), dot(hot, cn[b]), old).astype(BF16)

        lat_out(b, r).start()
    for b in range(2):
        pe_in(b).wait()
        for r in range(blocks):
            shift = r * NEW - len_ref[b]

            @pl.when((shift < NEW) & (shift > -NEW))
            def _():
                row = lax.broadcasted_iota(jnp.int32, (NEW, NEW), 0) + shift
                hot = (row == lax.broadcasted_iota(jnp.int32, (NEW, NEW), 1)).astype(F32).astype(BF16)
                col = lax.broadcasted_iota(jnp.int32, (LOC, NEW), 1) + shift
                old = cols[b, :, span(r)].astype(F32)
                cols[b, :, span(r)] = jnp.where((col >= 0) & (col < NEW), dot_nt(kn[b], hot), old).astype(BF16)

        pe_out(b).start()
    for b, r in places:
        lat_out(b, r).wait()
    for copy in y_out:
        copy.wait()
    for b in range(2):
        pe_out(b).wait()


def update_caches(lengths, y, cache_lat, pe_t, c_new, k_newt):
    hbm = pl.BlockSpec(memory_space=pl.ANY)
    sems = pltpu.SemaphoreType.DMA((2, cache_lat.shape[1] // NEW + 1))
    return pl.pallas_call(
        cache_kernel,
        in_specs=[pl.BlockSpec(memory_space=pltpu.SMEM)] + [hbm] * 5,
        out_specs=[hbm] * 3,
        out_shape=[jax.ShapeDtypeStruct(v.shape, BF16) for v in (y, cache_lat, pe_t)],
        scratch_shapes=[*[pltpu.VMEM(v.shape, BF16) for v in (y, cache_lat, pe_t, c_new, k_newt)], sems, sems, pltpu.SemaphoreType.DMA((2,)), pltpu.SemaphoreType.DMA((8,))],
        compiler_params=pltpu.CompilerParams(vmem_limit_bytes=VMEM_ALL),
        cost_estimate=cost(4e9, 12 * MIB),
        name="caches",
    )(lengths, y, cache_lat, pe_t, c_new, k_newt)


def at(start, size):
    return pl.ds(pl.multiple_of(start, size), size)


def main_kernel(len_ref, cos, sin, pet, g1, gq, gkv, x_hbm, wdq_hbm, wdkvt_hbm, c_hbm, wuk_hbm, wuv_hbm, wq_hbm, wo_hbm,
                y_hbm, cnew_hbm, knewt_hbm,
                lat, qa, kva, latb, cqt, cn, kn, knt, pe, cbuf, kb, vtb, wkb, wvtb, wqb, q_lo, q_hi, sb_a, sb_b, mb, ob, lhsb, wob,
                stage_d, xbuf, stage_x, rbuf, ybuf,
                lat_send, lat_recv, dq_sem, dkv_sem, c_sem, wk_sem, wvt_sem, wq_sem, wo_sem, x_sem, out_sem, y_sem,
                d_send, d_recv, i_send, i_recv, free_sem):
    sb = (sb_a, sb_b)
    me = lax.axis_index("tp")
    chip = me // 2
    core = me % 2
    sib = 2 * chip + (1 - core)
    far = 2 * (1 - chip) + core
    diag = 2 * (1 - chip) + (1 - core)

    def remote(src, dst, send, recv, peer):
        return pltpu.make_async_remote_copy(src_ref=src, dst_ref=dst, send_sem=send, recv_sem=recv, device_id={"tp": peer}, device_id_type=MESH)

    def fetch_rows(src, dst, sem, parts):
        size = dst.shape[0] // parts
        for k in range(parts):
            rows = pl.ds(k * size, size)
            pltpu.make_async_copy(src.at[rows], dst.at[rows], sem).start()

    def c_refs(b):
        return c_hbm.at[b, pl.ds(0, PREFIX), :], cbuf, c_sem

    def wq_refs(h):
        return wq_hbm.at[pl.ds(2 * h, 2)], wqb.at[h % 3], wq_sem.at[h % 3]

    def fetch_wq(i):
        src, dst, sem = wq_refs(i)
        for k in range(2):
            fetch_rows(src.at[k], dst.at[k], sem, 2)

    def wo_refs(g, n):
        return wo_hbm.at[:, at(n * CHUNK, CHUNK)], wob.at[g % 3], wo_sem.at[g % 3]

    def dq_refs(n):
        return wdq_hbm.at[at(n * DEPTH, DEPTH), :], kb.at[at((n % 4) * DEPTH, DEPTH), pl.ds(0, QR)], dq_sem.at[n % 4]

    def dkv_refs(n):
        return wdkvt_hbm.at[:, at(n * DEPTH, DEPTH)], vtb.at[pl.ds(0, 576), at((n % 4) * DEPTH, DEPTH)], dkv_sem.at[n % 4]

    def uk_copy(j):
        return pltpu.make_async_copy(wuk_hbm.at[at(WID * j, WID), :], kb.at[pl.ds(0, WID), at(QR + HD * j, HD)], wk_sem.at[j])

    def uv_copy(j):
        return pltpu.make_async_copy(wuv_hbm.at[at(1024 * j, 1024), :], vtb.at[pl.ds(1024, 1024), at(HD * j, HD)], wvt_sem.at[j])

    def piece(j):
        return at(HD * (j + 8), HD), pl.ds(1024, 1024)

    def x_copy(j):
        return pltpu.make_async_copy(x_hbm.at[:, at(1024 * j, 1024)], vtb.at[piece(j)], x_sem.at[j])

    def x_again(j):
        return pltpu.make_async_copy(x_hbm.at[:, at(1024 * j, 1024)], kb.at[at(HD * j, HD), pl.ds(0, 1024)], x_sem.at[j])

    for j in range(7):
        x_copy(j).start()
    for n in range(4):
        fetch_rows(*dq_refs(n), 2)
        fetch_rows(*dkv_refs(n), 2)

    barrier = pltpu.get_barrier_semaphore()
    for peer in (sib, far):
        pl.semaphore_signal(barrier, inc=1, device_id={"tp": peer}, device_id_type=MESH)

    aug = jnp.where(lax.broadcasted_iota(jnp.int32, (LOC, NEW), 0) == 0, 1.0, 0.0).astype(BF16)
    causal = lax.broadcasted_iota(jnp.int32, (NEW, NEW), 0) <= lax.broadcasted_iota(jnp.int32, (NEW, NEW), 1)
    for b in range(2):
        sb_a[pl.ds(NEW * b, NEW), :32] = cos[b].T
        sb_a[pl.ds(KVR + NEW * b, NEW), :32] = sin[b].T
    qa[...] = jnp.zeros_like(qa)
    kva[...] = jnp.zeros_like(kva)
    for j in range(7):
        x_copy(j).wait()

    def squares(j, acc):
        v = vtb[piece(j)].astype(F32)
        v = v * v
        return acc + sum(v[:, HD * k:HD * k + HD] for k in range(8))

    total = lax.fori_loop(0, 7, squares, jnp.zeros((HD, HD), F32))
    inv_x = lax.rsqrt(jnp.sum(total, axis=-1, keepdims=True) / 7168.0 + EPS)

    def scaled(j, carry):
        vtb[piece(j)] = (vtb[piece(j)].astype(F32) * inv_x * g1[:, at(1024 * j, 1024)]).astype(BF16)
        return carry

    lax.fori_loop(0, 7, scaled, 0)

    def project(n, carry):
        @pl.when((n >= 1) & (n + 3 < CHUNKS))
        def _():
            fetch_rows(*dq_refs(n + 3), 2)
            fetch_rows(*dkv_refs(n + 3), 2)

        pltpu.make_async_copy(*dq_refs(n)).wait()
        pltpu.make_async_copy(*dkv_refs(n)).wait()

        @pl.when(n == 4)
        def _():
            for j in range(4):
                uk_copy(j).start()
            for j in range(8):
                uv_copy(j).start()

        a = vtb[at(HD * (n // 2 + 8), HD), at(1024 + DEPTH * (n % 2), DEPTH)]
        slot = at((n % 4) * DEPTH, DEPTH)
        qa[...] += dot(a, kb[slot, :QR])
        kva[...] += dot_nt(a, vtb[:576, slot])

        @pl.when(n == CHUNKS - 3)
        def _():
            fetch_rows(*c_refs(0), 4)

        @pl.when(n >= CHUNKS - 4)
        def _():
            j = n - (CHUNKS - 4)
            uk_copy(j).wait()
            wkb[at(HD * j, HD), :] = kb[:WID, at(QR + HD * j, HD)].reshape(HD, WID)
            halves = []
            for k in range(2):
                uv_copy(2 * j + k).wait()
                halves.append(vtb[1024:WID, at(HD * (2 * j + k), HD)].reshape(LOC, WID))
            wvtb[:, at(HD * j, HD)] = jnp.concatenate(halves, axis=0).T

        return carry

    lax.fori_loop(0, CHUNKS, project, 0)
    for b in range(2):
        rows = slice(LOC * b, LOC * b + LOC)
        q = qa[rows, :]
        inv_q = lax.rsqrt(jnp.mean(q * q, axis=-1, keepdims=True) + EPS)
        lat[b, :, :QR] = (q * inv_q * gq[...]).astype(BF16)
        c = kva[rows, :KVR]
        inv_c = lax.rsqrt(jnp.mean(c * c, axis=-1, keepdims=True) + EPS)
        lat[b, :, QR:WID] = (c * inv_c * gkv[...]).astype(BF16)
        v1 = kva[rows, KVR:544]
        v2 = kva[rows, 544:576]
        own_cos = sb_a[at(NEW * b + me * LOC, LOC), :32]
        own_sin = sb_a[at(KVR + NEW * b + me * LOC, LOC), :32]
        rot = jnp.concatenate([v1 * own_cos - v2 * own_sin, v2 * own_cos + v1 * own_sin, jnp.zeros((LOC, LOC), F32)], axis=1)
        lat[b, :, WID:] = rot.astype(BF16)

    pl.semaphore_wait(barrier, 2)
    to_far = [remote(lat.at[b], latb.at[b, 1], lat_send.at[b, 1], lat_recv.at[b, 1], far) for b in range(2)]
    to_sib = [remote(lat.at[b], latb.at[b, 0], lat_send.at[b, 0], lat_recv.at[b, 0], sib) for b in range(2)]
    onward = [remote(latb.at[b, 1], latb.at[b, 2], lat_send.at[b, 2], lat_recv.at[b, 2], sib) for b in range(2)]
    to_far[0].start()
    to_sib[0].start()
    to_sib[1].start()
    for i in range(3):
        fetch_wq(i)
    for n in range(3):
        fetch_rows(*wo_refs(n, n), 4)
    def kv_start(b):
        length = len_ref[b]
        row = lax.broadcasted_iota(jnp.int32, (PREFIX, HD), 0)
        lane = lax.broadcasted_iota(jnp.int32, (PREFIX, HD), 1)
        old = row < length
        rot = pet[b, :, :PREFIX].astype(F32).T
        rot = jnp.concatenate([rot, jnp.zeros_like(rot)], axis=1)
        pe[:PREFIX, :] = jnp.where(old, rot, jnp.where(lane == LOC, NEG, 0.0)).astype(BF16)
        pltpu.make_async_copy(*c_refs(b)).wait()

    def kv_block(b, r, size):
        rows = at(r * size, size)
        row = lax.broadcasted_iota(jnp.int32, (size, HD), 0) + r * size
        m = jnp.where(row < len_ref[b], 1.0, 0.0).astype(BF16)
        c = cbuf[rows, :] * jnp.concatenate([m, m, m, m], axis=1)
        kb[rows, :] = dot(c, wkb[...]).astype(BF16)
        vtb[:, rows] = dot_nt(wvtb[...], c).astype(BF16)

    def assemble(b):
        cqa = ob.at[1]
        for src, owner in ((lat.at[b], me), (latb.at[b, 0], sib), (latb.at[b, 1], far), (latb.at[b, 2], diag)):
            rows = at(owner * LOC, LOC)
            cqa[rows, :QR] = src[:, :QR]
            cn[b, rows, :] = src[:, QR:WID]
            kn[rows, :] = src[:, WID:]
        cqt[...] = cqa[:, :QR].T
        knt[b] = kn[...].T[:LOC]
        pe[PREFIX:, :] = kn[...]
        kb[PREFIX:, :] = dot(cn[b], wkb[...]).astype(BF16)
        vtb[:, PREFIX:] = dot_nt(wvtb[...], cn[b]).astype(BF16)

    def query_pair(b, i):
        pltpu.make_async_copy(*wq_refs(i)).wait()
        cos_b = cos[b]
        sin_b = sin[b]
        for k in range(2):
            q = dot(wqb[i % 3, k, :, :CB], cqt[:CB, :]) + dot(wqb[i % 3, k, :, CB:], cqt[CB:, :])
            v1 = q[HD:160]
            v2 = q[160:]
            qt = jnp.concatenate([q[:HD].astype(BF16), (v1 * cos_b - v2 * sin_b).astype(BF16), (v2 * cos_b + v1 * sin_b).astype(BF16), aug], axis=0)
            q_lo[2 * i + k] = qt

        @pl.when(i + 3 < 8)
        def _():
            fetch_wq(i + 3)

    def attend(b, inside):
        if inside:
            query_pair(b, jnp.int32(0))

        halves = ((q_lo, range(5)), (q_hi, range(5, 9)))
        order = [(side, c) for c in range(5) for side, (_, blocks) in enumerate(halves) if c < len(blocks)]

        def score(h, k):
            d = at(h * HD, HD)
            best = [jnp.full((8, NEW), NEG, F32)] * 2
            for side, j in order:
                c = halves[side][1][j]
                rows = pl.ds(c * NEW, NEW)
                t = dot(jnp.concatenate([kb[rows, d], pe[rows, :]], axis=1), halves[side][0][(h, k)[side]]) * C2
                if c == 8:
                    t = jnp.where(causal, t, NEG)
                sb[k][rows, :] = t
                best[side] = jnp.maximum(best[side], jnp.max(t.reshape(32, 8, NEW), axis=0))
                yield
            mb[k] = jnp.maximum(*best)

        def finish(h, k):
            d = at(h * HD, HD)
            m = jnp.max(mb[k], axis=0, keepdims=True)
            l8 = jnp.zeros((8, NEW), F32)
            for c in range(9):
                rows = pl.ds(c * NEW, NEW)
                p = jnp.exp2(sb[k][rows, :] - m)
                sb[k][rows, :] = p
                l8 = l8 + jnp.sum(p.reshape(32, 8, NEW), axis=0)
                yield
            inv = 1.0 / jnp.sum(l8, axis=0, keepdims=True)
            acc = [jnp.zeros((HD, NEW), F32)] * 2
            for side, j in order:
                rows = pl.ds(halves[side][1][j] * NEW, NEW)
                acc[side] = acc[side] + dot(vtb[d, rows], (sb[k][rows, :] * inv).astype(BF16))
                yield
            ob[b, :, d] = (acc[0] + acc[1]).T.astype(BF16)

        def weave(*parts):
            live = list(parts)
            while live:
                live = [part for part in live if next(part, live) is None]

        for k in range(2):
            q_hi[k] = q_lo[k]

        @pl.when(me >= 0)
        def _():
            weave(score(0, 0))

        def pair(i, carry):
            h = 2 * i
            if inside:
                @pl.when(i < 7)
                def _():
                    query_pair(b, i + 1)

            @pl.when(i >= 0)
            def _():
                weave(score(h + 1, 1), finish(h, 0))
                q_hi[0] = q_lo[jnp.minimum(h + 2, 15)]

            @pl.when(i < 8)
            def _():
                weave(score(jnp.minimum(h + 2, 15), 0), finish(h + 1, 1))
                q_hi[1] = q_lo[jnp.minimum(h + 3, 15)]

            return carry

        lax.fori_loop(0, 8, pair, 0)

    def to_sibling(b, n):
        return remote(stage_d.at[n % 4, 0], xbuf.at[b, n], d_send.at[n % 4], d_recv.at[b, n], sib)

    def over_link(b, n):
        return remote(stage_x.at[b, n], rbuf.at[b, n], i_send.at[b, n], i_recv.at[b, n], far)

    def put_y(n):
        return pltpu.make_async_copy(ybuf.at[n % 4], y_hbm.at[:, at(n * CHUNK, CHUNK)], y_sem.at[n % 4])

    def product(rows, g, n):
        pltpu.make_async_copy(*wo_refs(g, n)).wait()
        return dot(lhsb[:rows, :], wob[g % 3])

    def next_wo(g):
        @pl.when(g + 3 < 3 * CHUNKS)
        def _():
            fetch_rows(*wo_refs(g + 3, (g + 3) % CHUNKS), 4)

    def load_lhs(k, b, owner):
        lhsb[LOC * k:LOC * k + LOC, :] = ob[b, at(owner * LOC, LOC), :]

    def pass_on(b, n):
        to_sibling(b, n).wait_recv()
        stage_x[b, n] = stage_x[b, n] + xbuf[b, n]
        over_link(b, n).start()

    def far_start(b):
        load_lhs(0, b, far)
        load_lhs(1, b, diag)

    def far_chunk(b, n):
        g = b * CHUNKS + n
        y = product(HD, g, n)

        @pl.when(n >= 4)
        def _():
            to_sibling(b, n - 4).wait_send()

        stage_d[n % 4, 0] = y[LOC:]
        stage_x[b, n] = y[:LOC]
        to_sibling(b, n).start()
        next_wo(g)

        @pl.when(n == 1)
        def _():
            pass_on(b, 0)

        @pl.when(n >= 3)
        def _():
            pass_on(b, n - 2)

    def far_end(b):
        pass_on(b, CHUNKS - 2)
        pass_on(b, CHUNKS - 1)
        for n in range(CHUNKS - 4, CHUNKS):
            to_sibling(b, n).wait_send()

    def own_unit(unit):
        for n in range(4):
            over_link(0, n).wait_send()
        for b in range(2):
            load_lhs(b, b, me)
            load_lhs(2 + b, b, sib)

        def both(n):
            return remote(stage_d.at[n % 4], xbuf.at[:, n], d_send.at[n % 4], d_recv.at[0, n], sib)

        def finish(n):
            both(n).wait_recv()

            @pl.when(n >= 4)
            def _():
                put_y(n - 4).wait()

            for b in range(2):
                over_link(b, n).wait_recv()
                total = stage_x[0, 2 * (n % 2) + b] + xbuf[b, n] + rbuf[b, n]
                x = kb[at(HD * (n // 2) + LOC * b, LOC), at(CHUNK * (n % 2), CHUNK)]
                ybuf[n % 4, pl.ds(LOC * b, LOC), :] = (x.astype(F32) + total).astype(BF16)
            put_y(n).start()

        def chunk(n, carry):
            g = unit * CHUNKS + n
            y = product(NEW, g, n)

            @pl.when(n >= 4)
            def _():
                both(n - 4).wait_send()

            for b in range(2):
                stage_x[0, 2 * (n % 2) + b] = y[LOC * b:LOC * b + LOC]
                stage_d[n % 4, b] = y[HD + LOC * b:192 + LOC * b]
            both(n).start()
            next_wo(g)

            @pl.when(n >= 1)
            def _():
                finish(n - 1)

            return carry

        lax.fori_loop(0, CHUNKS, chunk, 0)
        finish(CHUNKS - 1)
        for n in range(CHUNKS - 4, CHUNKS):
            both(n).wait_send()
            put_y(n).wait()

    def first_block(r, carry):
        @pl.when(r == 3)
        def _():
            to_far[1].start()
            to_far[0].wait_recv()
            onward[0].start()

        kv_block(0, r, ROW_BLK)
        return carry

    def second_block(r, carry):
        n = 3 * r + 2
        far_chunk(0, n)
        query_pair(1, 2 * r)
        far_chunk(0, n + 1)
        query_pair(1, 2 * r + 1)
        far_chunk(0, n + 2)
        kv_block(1, r, ROW_BLK)
        return carry

    def far_only(b, n, carry):
        far_chunk(b, n)
        return carry

    kv_start(0)
    lax.fori_loop(0, PREFIX // ROW_BLK, first_block, 0)
    fetch_rows(*c_refs(1), 4)
    to_sib[0].wait_recv()
    onward[0].wait_recv()
    assemble(0)
    attend(0, True)
    for i in range(3):
        fetch_wq(i)
    to_far[1].wait_recv()
    onward[1].start()
    far_start(0)
    lax.fori_loop(0, 2, functools.partial(far_only, 0), 0)
    kv_start(1)
    to_sib[1].wait_recv()
    onward[1].wait_recv()
    assemble(1)
    lax.fori_loop(0, PREFIX // ROW_BLK, second_block, 0)
    far_end(0)
    put_c = pltpu.make_async_copy(cn, cnew_hbm, out_sem.at[0])
    put_k = pltpu.make_async_copy(knt, knewt_hbm, out_sem.at[1])
    put_c.start()
    put_k.start()
    attend(1, False)
    for j in range(7):
        x_again(j).start()
    far_start(1)
    lax.fori_loop(0, CHUNKS, functools.partial(far_only, 1), 0)
    far_end(1)
    pl.semaphore_signal(free_sem, inc=1, device_id={"tp": sib}, device_id_type=MESH)
    pl.semaphore_wait(free_sem, 1)
    for j in range(7):
        x_again(j).wait()
    own_unit(2)
    for b in range(2):
        to_far[b].wait_send()
        to_sib[b].wait_send()
        onward[b].wait_send()

        def drain(n, carry):
            over_link(b, n).wait_send()
            return carry

        lax.fori_loop((4, 0)[b], CHUNKS, drain, 0)
    put_c.wait()
    put_k.wait()


def main_call(lengths, *arrays):
    vmem = pl.BlockSpec(memory_space=pltpu.VMEM)
    hbm = pl.BlockSpec(memory_space=pl.ANY)
    dma = pltpu.SemaphoreType.DMA
    return pl.pallas_call(
        main_kernel,
        in_specs=[pl.BlockSpec(memory_space=pltpu.SMEM)] + [vmem] * 6 + [hbm] * 8,
        out_specs=[hbm] * 3,
        out_shape=[
            jax.ShapeDtypeStruct((HD, 7168), BF16),
            jax.ShapeDtypeStruct((2, NEW, KVR), BF16),
            jax.ShapeDtypeStruct((2, LOC, NEW), BF16),
        ],
        scratch_shapes=[
            pltpu.VMEM((2, LOC, LAT_W), BF16),
            pltpu.VMEM((HD, QR), F32),
            pltpu.VMEM((HD, 576), F32),
            pltpu.VMEM((2, 3, LOC, LAT_W), BF16),
            pltpu.VMEM((QR, NEW), BF16),
            pltpu.VMEM((2, NEW, KVR), BF16),
            pltpu.VMEM((NEW, HD), BF16),
            pltpu.VMEM((2, LOC, NEW), BF16),
            pltpu.VMEM((PREFIX + NEW, HD), BF16),
            pltpu.VMEM((PREFIX, KVR), BF16),
            pltpu.VMEM((PREFIX + NEW, WID), BF16),
            pltpu.VMEM((WID, PREFIX + NEW), BF16),
            pltpu.VMEM((KVR, WID), BF16),
            pltpu.VMEM((WID, KVR), BF16),
            pltpu.VMEM((3, 2, 192, QR), BF16),
            pltpu.VMEM((16, NEW, NEW), BF16),
            pltpu.VMEM((2, NEW, NEW), BF16),
            *[pltpu.VMEM((PREFIX + NEW, NEW), F32)] * 2,
            pltpu.VMEM((2, 8, NEW), F32),
            pltpu.VMEM((2, NEW, WID), BF16),
            pltpu.VMEM((NEW, WID), BF16),
            pltpu.VMEM((3, WID, CHUNK), BF16),
            pltpu.VMEM((4, 2, LOC, CHUNK), F32),
            *[pltpu.VMEM((2, CHUNKS, LOC, CHUNK), F32)] * 3,
            pltpu.VMEM((4, HD, CHUNK), BF16),
            *[dma((2, 3))] * 2,
            *[dma((4,))] * 2,
            dma,
            dma((4,)),
            dma((8,)),
            dma((4,)),
            dma((3,)),
            dma((7,)),
            dma((2,)),
            dma((4,)),
            dma((4,)),
            *[dma((2, CHUNKS))] * 3,
            pltpu.SemaphoreType.REGULAR,
        ],
        compiler_params=pltpu.CompilerParams(vmem_limit_bytes=VMEM_ALL, collective_id=0, has_side_effects=True),
        cost_estimate=cost(1e11, 200 * MIB),
        name="main",
    )(lengths, *arrays)


def solution(mesh):
    def local_step(hidden, lengths, rope_cos, rope_sin, cache_lat, cache_pe, norm_in, w_dq, norm_q, w_dkv, norm_kv, w_uq, w_uk, w_uv, w_out):
        pe_t = jnp.swapaxes(cache_pe, 1, 2)
        y, c_new, k_newt = main_call(
            lengths,
            jnp.swapaxes(rope_cos, 1, 2),
            jnp.swapaxes(rope_sin, 1, 2),
            pe_t,
            norm_in[None],
            norm_q,
            norm_kv[None],
            hidden.reshape(HD, 7168),
            w_dq,
            w_dkv.T,
            cache_lat,
            w_uk.reshape(8192, HD),
            w_uv.reshape(8192, HD),
            jnp.transpose(w_uq, (1, 2, 0)),
            w_out,
        )
        y, lat_new, pe_new = update_caches(lengths, y, cache_lat, pe_t, c_new, k_newt)
        return y.reshape(hidden.shape), lat_new, jnp.swapaxes(pe_new, 1, 2)

    spec_tok = P("dp", "tp", None)
    spec_len = P("dp")
    spec_seq = P("dp", None, None)
    spec_vec = P(None)
    spec_mat = P(None, None)
    spec_head = P(None, "tp", None)
    spec_rows = P("tp", None)
    in_specs = (spec_tok, spec_len, spec_seq, spec_seq, spec_seq, spec_seq, spec_vec, spec_mat, spec_vec, spec_mat, spec_vec, spec_head, spec_head, spec_head, spec_rows)
    return jax.shard_map(local_step, mesh=mesh, in_specs=in_specs, out_specs=(spec_tok, spec_seq, spec_seq), check_vma=False)
```

```python
import functools

import jax
import jax.numpy as jnp
from jax import lax
from jax.experimental import pallas as pl
from jax.experimental.pallas import tpu as pltpu
from jax.sharding import PartitionSpec as P

F32 = jnp.float32
BF16 = jnp.bfloat16
EPS = 1e-6
MIB = 1 << 20
VMEM_ALL = 67043328
MESH = pl.DeviceIdType.MESH
LAT_W = 2176
PREFIX = 2048
ROW_BLK = 512
CHUNK = 512
DEPTH = 512
CHUNKS = 7168 // CHUNK
C2 = 192.0 ** -0.5 * 1.4426950408889634
NEG = -1e30
LOC = 64
HD = 128
NEW = 256
QR = 1536
WID = 2048
CB = 768
KVR = 512
NT = (((1,), (1,)), ((), ()))


def dot(lhs, rhs):
    return jnp.dot(lhs, rhs, preferred_element_type=F32)


def dot_nt(lhs, rhs):
    return lax.dot_general(lhs, rhs, NT, preferred_element_type=F32)


def cost(flops, nbytes):
    return pl.CostEstimate(flops=int(flops), bytes_accessed=int(nbytes), transcendentals=0)


def cache_kernel(len_ref, y_hbm, c_hbm, pe_hbm, cn_hbm, kn_hbm, yo_hbm, co_hbm, po_hbm, y, rows, cols, cn, kn, in_sem, out_sem, side_sem, y_sem):
    blocks = rows.shape[1] // NEW
    span = lambda r: pl.ds(r * NEW, NEW)
    lat_in = lambda b, r: pltpu.make_async_copy(c_hbm.at[b, span(r)], rows.at[b, span(r)], in_sem.at[b, r])
    lat_out = lambda b, r: pltpu.make_async_copy(rows.at[b, span(r)], co_hbm.at[b, span(r)], out_sem.at[b, r])
    pe_in = lambda b: pltpu.make_async_copy(pe_hbm.at[b], cols.at[b], in_sem.at[b, blocks])
    pe_out = lambda b: pltpu.make_async_copy(cols.at[b], po_hbm.at[b], out_sem.at[b, blocks])
    new_in = [pltpu.make_async_copy(cn_hbm, cn, side_sem.at[0]), pltpu.make_async_copy(kn_hbm, kn, side_sem.at[1])]
    part = lambda k: pl.ds(32 * k, 32)
    y_in = [pltpu.make_async_copy(y_hbm.at[part(k)], y.at[part(k)], y_sem.at[k]) for k in range(4)]
    y_out = [pltpu.make_async_copy(y.at[part(k)], yo_hbm.at[part(k)], y_sem.at[4 + k]) for k in range(4)]
    places = [(b, r) for b in range(2) for r in range(blocks)]
    for copy in new_in:
        copy.start()
    for copy in y_in:
        copy.start()
    for b, r in places:
        lat_in(b, r).start()
    for b in range(2):
        pe_in(b).start()
    for copy in new_in:
        copy.wait()
    for k in range(4):
        y_in[k].wait()
        y_out[k].start()
    for b, r in places:
        shift = r * NEW - len_ref[b]
        lat_in(b, r).wait()

        @pl.when((shift < NEW) & (shift > -NEW))
        def _():
            row = lax.broadcasted_iota(jnp.int32, (NEW, NEW), 0) + shift
            hot = (row == lax.broadcasted_iota(jnp.int32, (NEW, NEW), 1)).astype(F32).astype(BF16)
            row = lax.broadcasted_iota(jnp.int32, (NEW, KVR), 0) + shift
            old = rows[b, span(r), :].astype(F32)
            rows[b, span(r), :] = jnp.where((row >= 0) & (row < NEW), dot(hot, cn[b]), old).astype(BF16)

        lat_out(b, r).start()
    for b in range(2):
        pe_in(b).wait()
        for r in range(blocks):
            shift = r * NEW - len_ref[b]

            @pl.when((shift < NEW) & (shift > -NEW))
            def _():
                row = lax.broadcasted_iota(jnp.int32, (NEW, NEW), 0) + shift
                hot = (row == lax.broadcasted_iota(jnp.int32, (NEW, NEW), 1)).astype(F32).astype(BF16)
                col = lax.broadcasted_iota(jnp.int32, (LOC, NEW), 1) + shift
                old = cols[b, :, span(r)].astype(F32)
                cols[b, :, span(r)] = jnp.where((col >= 0) & (col < NEW), dot_nt(kn[b], hot), old).astype(BF16)

        pe_out(b).start()
    for b, r in places:
        lat_out(b, r).wait()
    for copy in y_out:
        copy.wait()
    for b in range(2):
        pe_out(b).wait()


def update_caches(lengths, y, cache_lat, pe_t, c_new, k_newt):
    hbm = pl.BlockSpec(memory_space=pl.ANY)
    sems = pltpu.SemaphoreType.DMA((2, cache_lat.shape[1] // NEW + 1))
    return pl.pallas_call(
        cache_kernel,
        in_specs=[pl.BlockSpec(memory_space=pltpu.SMEM)] + [hbm] * 5,
        out_specs=[hbm] * 3,
        out_shape=[jax.ShapeDtypeStruct(v.shape, BF16) for v in (y, cache_lat, pe_t)],
        scratch_shapes=[*[pltpu.VMEM(v.shape, BF16) for v in (y, cache_lat, pe_t, c_new, k_newt)], sems, sems, pltpu.SemaphoreType.DMA((2,)), pltpu.SemaphoreType.DMA((8,))],
        compiler_params=pltpu.CompilerParams(vmem_limit_bytes=VMEM_ALL),
        cost_estimate=cost(4e9, 12 * MIB),
        name="caches",
    )(lengths, y, cache_lat, pe_t, c_new, k_newt)


def at(start, size):
    return pl.ds(pl.multiple_of(start, size), size)


def main_kernel(len_ref, cos, sin, pet, g1, gq, gkv, x_hbm, wdq_hbm, wdkvt_hbm, c_hbm, wuk_hbm, wuv_hbm, wq_hbm, wo_hbm,
                y_hbm, cnew_hbm, knewt_hbm,
                lat, qa, kva, latb, cqt, cn, kn, knt, pe, cbuf, kb, vtb, wkb, wvtb, wqb, q_lo, q_hi, sb_a, sb_b, mb, ob, lhsb, wob,
                stage_d, xbuf, stage_x, rbuf, ybuf,
                lat_send, lat_recv, dq_sem, dkv_sem, c_sem, wk_sem, wvt_sem, wq_sem, wo_sem, x_sem, out_sem, y_sem,
                d_send, d_recv, i_send, i_recv, free_sem):
    sb = (sb_a, sb_b)
    me = lax.axis_index("tp")
    chip = me // 2
    core = me % 2
    sib = 2 * chip + (1 - core)
    far = 2 * (1 - chip) + core
    diag = 2 * (1 - chip) + (1 - core)

    def remote(src, dst, send, recv, peer):
        return pltpu.make_async_remote_copy(src_ref=src, dst_ref=dst, send_sem=send, recv_sem=recv, device_id={"tp": peer}, device_id_type=MESH)

    def fetch_rows(src, dst, sem, parts):
        size = dst.shape[0] // parts
        for k in range(parts):
            rows = pl.ds(k * size, size)
            pltpu.make_async_copy(src.at[rows], dst.at[rows], sem).start()

    def c_refs(b):
        return c_hbm.at[b, pl.ds(0, PREFIX), :], cbuf, c_sem

    def wq_refs(h):
        return wq_hbm.at[pl.ds(2 * h, 2)], wqb.at[h % 3], wq_sem.at[h % 3]

    def fetch_wq(i):
        src, dst, sem = wq_refs(i)
        for k in range(2):
            fetch_rows(src.at[k], dst.at[k], sem, 2)

    def wo_refs(g, n):
        return wo_hbm.at[:, at(n * CHUNK, CHUNK)], wob.at[g % 3], wo_sem.at[g % 3]

    def dq_refs(n):
        return wdq_hbm.at[at(n * DEPTH, DEPTH), :], kb.at[at((n % 4) * DEPTH, DEPTH), pl.ds(0, QR)], dq_sem.at[n % 4]

    def dkv_refs(n):
        return wdkvt_hbm.at[:, at(n * DEPTH, DEPTH)], vtb.at[pl.ds(0, 576), at((n % 4) * DEPTH, DEPTH)], dkv_sem.at[n % 4]

    def uk_copy(j):
        return pltpu.make_async_copy(wuk_hbm.at[at(WID * j, WID), :], kb.at[pl.ds(0, WID), at(QR + HD * j, HD)], wk_sem.at[j])

    def uv_copy(j):
        return pltpu.make_async_copy(wuv_hbm.at[at(1024 * j, 1024), :], vtb.at[pl.ds(1024, 1024), at(HD * j, HD)], wvt_sem.at[j])

    def piece(j):
        return at(HD * (j + 8), HD), pl.ds(1024, 1024)

    def x_copy(j):
        return pltpu.make_async_copy(x_hbm.at[:, at(1024 * j, 1024)], vtb.at[piece(j)], x_sem.at[j])

    def x_again(j):
        return pltpu.make_async_copy(x_hbm.at[:, at(1024 * j, 1024)], kb.at[at(HD * j, HD), pl.ds(0, 1024)], x_sem.at[j])

    for j in range(7):
        x_copy(j).start()
    for n in range(4):
        fetch_rows(*dq_refs(n), 2)
        fetch_rows(*dkv_refs(n), 2)
    for j in range(4):
        uk_copy(j).start()
    for j in range(8):
        uv_copy(j).start()

    barrier = pltpu.get_barrier_semaphore()
    for peer in (sib, far):
        pl.semaphore_signal(barrier, inc=1, device_id={"tp": peer}, device_id_type=MESH)

    aug = jnp.where(lax.broadcasted_iota(jnp.int32, (LOC, NEW), 0) == 0, 1.0, 0.0).astype(BF16)
    causal = lax.broadcasted_iota(jnp.int32, (NEW, NEW), 0) <= lax.broadcasted_iota(jnp.int32, (NEW, NEW), 1)
    for b in range(2):
        sb_a[pl.ds(NEW * b, NEW), :32] = cos[b].T
        sb_a[pl.ds(KVR + NEW * b, NEW), :32] = sin[b].T
    qa[...] = jnp.zeros_like(qa)
    kva[...] = jnp.zeros_like(kva)
    for j in range(7):
        x_copy(j).wait()

    def squares(j, acc):
        v = vtb[piece(j)].astype(F32)
        v = v * v
        return acc + sum(v[:, HD * k:HD * k + HD] for k in range(8))

    total = lax.fori_loop(0, 7, squares, jnp.zeros((HD, HD), F32))
    inv_x = lax.rsqrt(jnp.sum(total, axis=-1, keepdims=True) / 7168.0 + EPS)

    def scaled(j, carry):
        vtb[piece(j)] = (vtb[piece(j)].astype(F32) * inv_x * g1[:, at(1024 * j, 1024)]).astype(BF16)
        return carry

    lax.fori_loop(0, 7, scaled, 0)

    def project(n, carry):
        @pl.when((n >= 1) & (n + 3 < CHUNKS))
        def _():
            fetch_rows(*dq_refs(n + 3), 2)
            fetch_rows(*dkv_refs(n + 3), 2)

        pltpu.make_async_copy(*dq_refs(n)).wait()
        pltpu.make_async_copy(*dkv_refs(n)).wait()

        a = vtb[at(HD * (n // 2 + 8), HD), at(1024 + DEPTH * (n % 2), DEPTH)]
        slot = at((n % 4) * DEPTH, DEPTH)
        qa[...] += dot(a, kb[slot, :QR])
        kva[...] += dot_nt(a, vtb[:576, slot])

        @pl.when(n == CHUNKS - 3)
        def _():
            fetch_rows(*c_refs(0), 4)

        @pl.when(n >= CHUNKS - 4)
        def _():
            j = n - (CHUNKS - 4)
            uk_copy(j).wait()
            wkb[at(HD * j, HD), :] = kb[:WID, at(QR + HD * j, HD)].reshape(HD, WID)
            halves = []
            for k in range(2):
                uv_copy(2 * j + k).wait()
                halves.append(vtb[1024:WID, at(HD * (2 * j + k), HD)].reshape(LOC, WID))
            wvtb[:, at(HD * j, HD)] = jnp.concatenate(halves, axis=0).T

        return carry

    lax.fori_loop(0, CHUNKS, project, 0)
    for b in range(2):
        rows = slice(LOC * b, LOC * b + LOC)
        q = qa[rows, :]
        inv_q = lax.rsqrt(jnp.mean(q * q, axis=-1, keepdims=True) + EPS)
        lat[b, :, :QR] = (q * inv_q * gq[...]).astype(BF16)
        c = kva[rows, :KVR]
        inv_c = lax.rsqrt(jnp.mean(c * c, axis=-1, keepdims=True) + EPS)
        lat[b, :, QR:WID] = (c * inv_c * gkv[...]).astype(BF16)
        v1 = kva[rows, KVR:544]
        v2 = kva[rows, 544:576]
        own_cos = sb_a[at(NEW * b + me * LOC, LOC), :32]
        own_sin = sb_a[at(KVR + NEW * b + me * LOC, LOC), :32]
        rot = jnp.concatenate([v1 * own_cos - v2 * own_sin, v2 * own_cos + v1 * own_sin, jnp.zeros((LOC, LOC), F32)], axis=1)
        lat[b, :, WID:] = rot.astype(BF16)

    pl.semaphore_wait(barrier, 2)
    to_far = [remote(lat.at[b], latb.at[b, 1], lat_send.at[b, 1], lat_recv.at[b, 1], far) for b in range(2)]
    to_sib = [remote(lat.at[b], latb.at[b, 0], lat_send.at[b, 0], lat_recv.at[b, 0], sib) for b in range(2)]
    onward = [remote(latb.at[b, 1], latb.at[b, 2], lat_send.at[b, 2], lat_recv.at[b, 2], sib) for b in range(2)]
    to_far[0].start()
    to_sib[0].start()
    to_sib[1].start()
    for i in range(3):
        fetch_wq(i)
    for n in range(3):
        fetch_rows(*wo_refs(n, n), 4)
    def kv_start(b):
        length = len_ref[b]
        row = lax.broadcasted_iota(jnp.int32, (PREFIX, HD), 0)
        lane = lax.broadcasted_iota(jnp.int32, (PREFIX, HD), 1)
        old = row < length
        rot = pet[b, :, :PREFIX].astype(F32).T
        rot = jnp.concatenate([rot, jnp.zeros_like(rot)], axis=1)
        pe[:PREFIX, :] = jnp.where(old, rot, jnp.where(lane == LOC, NEG, 0.0)).astype(BF16)
        pltpu.make_async_copy(*c_refs(b)).wait()

    def kv_block(b, r, size):
        rows = at(r * size, size)
        row = lax.broadcasted_iota(jnp.int32, (size, HD), 0) + r * size
        m = jnp.where(row < len_ref[b], 1.0, 0.0).astype(BF16)
        c = cbuf[rows, :] * jnp.concatenate([m, m, m, m], axis=1)
        kb[rows, :] = dot(c, wkb[...]).astype(BF16)
        vtb[:, rows] = dot_nt(wvtb[...], c).astype(BF16)

    def assemble(b):
        cqa = ob.at[1]
        for src, owner in ((lat.at[b], me), (latb.at[b, 0], sib), (latb.at[b, 1], far), (latb.at[b, 2], diag)):
            rows = at(owner * LOC, LOC)
            cqa[rows, :QR] = src[:, :QR]
            cn[b, rows, :] = src[:, QR:WID]
            kn[rows, :] = src[:, WID:]
        cqt[...] = cqa[:, :QR].T
        knt[b] = kn[...].T[:LOC]
        pe[PREFIX:, :] = kn[...]
        kb[PREFIX:, :] = dot(cn[b], wkb[...]).astype(BF16)
        vtb[:, PREFIX:] = dot_nt(wvtb[...], cn[b]).astype(BF16)

    def query_pair(b, i):
        pltpu.make_async_copy(*wq_refs(i)).wait()
        cos_b = cos[b]
        sin_b = sin[b]
        for k in range(2):
            q = dot(wqb[i % 3, k, :, :CB], cqt[:CB, :]) + dot(wqb[i % 3, k, :, CB:], cqt[CB:, :])
            v1 = q[HD:160]
            v2 = q[160:]
            qt = jnp.concatenate([q[:HD].astype(BF16), (v1 * cos_b - v2 * sin_b).astype(BF16), (v2 * cos_b + v1 * sin_b).astype(BF16), aug], axis=0)
            q_lo[2 * i + k] = qt

        @pl.when(i + 3 < 8)
        def _():
            fetch_wq(i + 3)

    def attend(b, inside):
        if inside:
            query_pair(b, jnp.int32(0))

        halves = ((q_lo, range(5)), (q_hi, range(5, 9)))
        order = [(side, c) for c in range(5) for side, (_, blocks) in enumerate(halves) if c < len(blocks)]

        def score(h, k):
            d = at(h * HD, HD)
            best = [jnp.full((8, NEW), NEG, F32)] * 2
            for side, j in order:
                c = halves[side][1][j]
                rows = pl.ds(c * NEW, NEW)
                t = dot(jnp.concatenate([kb[rows, d], pe[rows, :]], axis=1), halves[side][0][(h, k)[side]]) * C2
                if c == 8:
                    t = jnp.where(causal, t, NEG)
                sb[k][rows, :] = t
                best[side] = jnp.maximum(best[side], jnp.max(t.reshape(32, 8, NEW), axis=0))
                yield
            mb[k] = jnp.maximum(*best)

        def finish(h, k):
            d = at(h * HD, HD)
            m = jnp.max(mb[k], axis=0, keepdims=True)
            l8 = jnp.zeros((8, NEW), F32)
            for c in range(9):
                rows = pl.ds(c * NEW, NEW)
                p = jnp.exp2(sb[k][rows, :] - m)
                sb[k][rows, :] = p
                l8 = l8 + jnp.sum(p.reshape(32, 8, NEW), axis=0)
                yield
            inv = 1.0 / jnp.sum(l8, axis=0, keepdims=True)
            acc = [jnp.zeros((HD, NEW), F32)] * 2
            for side, j in order:
                rows = pl.ds(halves[side][1][j] * NEW, NEW)
                acc[side] = acc[side] + dot(vtb[d, rows], (sb[k][rows, :] * inv).astype(BF16))
                yield
            ob[b, :, d] = (acc[0] + acc[1]).T.astype(BF16)

        def weave(*parts):
            live = list(parts)
            while live:
                live = [part for part in live if next(part, live) is None]

        for k in range(2):
            q_hi[k] = q_lo[k]

        @pl.when(me >= 0)
        def _():
            weave(score(0, 0))

        def pair(i, carry):
            h = 2 * i
            if inside:
                @pl.when(i < 7)
                def _():
                    query_pair(b, i + 1)

            @pl.when(i >= 0)
            def _():
                weave(score(h + 1, 1), finish(h, 0))
                q_hi[0] = q_lo[jnp.minimum(h + 2, 15)]

            @pl.when(i < 8)
            def _():
                weave(score(jnp.minimum(h + 2, 15), 0), finish(h + 1, 1))
                q_hi[1] = q_lo[jnp.minimum(h + 3, 15)]

            return carry

        lax.fori_loop(0, 8, pair, 0)

    def to_sibling(b, n):
        return remote(stage_d.at[n % 4, 0], xbuf.at[b, n], d_send.at[n % 4], d_recv.at[b, n], sib)

    def over_link(b, n):
        return remote(stage_x.at[b, n], rbuf.at[b, n], i_send.at[b, n], i_recv.at[b, n], far)

    def put_y(n):
        return pltpu.make_async_copy(ybuf.at[n % 4], y_hbm.at[:, at(n * CHUNK, CHUNK)], y_sem.at[n % 4])

    def product(rows, g, n):
        pltpu.make_async_copy(*wo_refs(g, n)).wait()
        return dot(lhsb[:rows, :], wob[g % 3])

    def next_wo(g):
        @pl.when(g + 3 < 3 * CHUNKS)
        def _():
            fetch_rows(*wo_refs(g + 3, (g + 3) % CHUNKS), 4)

    def load_lhs(k, b, owner):
        lhsb[LOC * k:LOC * k + LOC, :] = ob[b, at(owner * LOC, LOC), :]

    def pass_on(b, n):
        to_sibling(b, n).wait_recv()
        stage_x[b, n] = stage_x[b, n] + xbuf[b, n]
        over_link(b, n).start()

    def far_start(b):
        load_lhs(0, b, far)
        load_lhs(1, b, diag)

    def far_chunk(b, n):
        g = b * CHUNKS + n
        y = product(HD, g, n)

        @pl.when(n >= 4)
        def _():
            to_sibling(b, n - 4).wait_send()

        stage_d[n % 4, 0] = y[LOC:]
        stage_x[b, n] = y[:LOC]
        to_sibling(b, n).start()
        next_wo(g)

        @pl.when(n == 1)
        def _():
            pass_on(b, 0)

        @pl.when(n >= 3)
        def _():
            pass_on(b, n - 2)

    def far_end(b):
        pass_on(b, CHUNKS - 2)
        pass_on(b, CHUNKS - 1)
        for n in range(CHUNKS - 4, CHUNKS):
            to_sibling(b, n).wait_send()

    def own_unit(unit):
        for n in range(4):
            over_link(0, n).wait_send()
        for b in range(2):
            load_lhs(b, b, me)
            load_lhs(2 + b, b, sib)

        def both(n):
            return remote(stage_d.at[n % 4], xbuf.at[:, n], d_send.at[n % 4], d_recv.at[0, n], sib)

        def finish(n):
            both(n).wait_recv()

            @pl.when(n >= 4)
            def _():
                put_y(n - 4).wait()

            for b in range(2):
                over_link(b, n).wait_recv()
                total = stage_x[0, 2 * (n % 2) + b] + xbuf[b, n] + rbuf[b, n]
                x = kb[at(HD * (n // 2) + LOC * b, LOC), at(CHUNK * (n % 2), CHUNK)]
                ybuf[n % 4, pl.ds(LOC * b, LOC), :] = (x.astype(F32) + total).astype(BF16)
            put_y(n).start()

        def chunk(n, carry):
            g = unit * CHUNKS + n
            y = product(NEW, g, n)

            @pl.when(n >= 4)
            def _():
                both(n - 4).wait_send()

            for b in range(2):
                stage_x[0, 2 * (n % 2) + b] = y[LOC * b:LOC * b + LOC]
                stage_d[n % 4, b] = y[HD + LOC * b:192 + LOC * b]
            both(n).start()
            next_wo(g)

            @pl.when(n >= 1)
            def _():
                finish(n - 1)

            return carry

        lax.fori_loop(0, CHUNKS, chunk, 0)
        finish(CHUNKS - 1)
        for n in range(CHUNKS - 4, CHUNKS):
            both(n).wait_send()
            put_y(n).wait()

    def first_block(r, carry):
        @pl.when(r == 3)
        def _():
            to_far[1].start()
            to_far[0].wait_recv()
            onward[0].start()

        kv_block(0, r, ROW_BLK)
        return carry

    def second_block(r, carry):
        n = 3 * r + 2
        far_chunk(0, n)
        query_pair(1, 2 * r)
        far_chunk(0, n + 1)
        query_pair(1, 2 * r + 1)
        far_chunk(0, n + 2)
        kv_block(1, r, ROW_BLK)
        return carry

    def far_only(b, n, carry):
        far_chunk(b, n)
        return carry

    kv_start(0)
    lax.fori_loop(0, PREFIX // ROW_BLK, first_block, 0)
    fetch_rows(*c_refs(1), 4)
    to_sib[0].wait_recv()
    onward[0].wait_recv()
    assemble(0)
    attend(0, True)
    for i in range(3):
        fetch_wq(i)
    to_far[1].wait_recv()
    onward[1].start()
    far_start(0)
    lax.fori_loop(0, 2, functools.partial(far_only, 0), 0)
    kv_start(1)
    to_sib[1].wait_recv()
    onward[1].wait_recv()
    assemble(1)
    lax.fori_loop(0, PREFIX // ROW_BLK, second_block, 0)
    far_end(0)
    put_c = pltpu.make_async_copy(cn, cnew_hbm, out_sem.at[0])
    put_k = pltpu.make_async_copy(knt, knewt_hbm, out_sem.at[1])
    put_c.start()
    put_k.start()
    attend(1, False)
    for j in range(7):
        x_again(j).start()
    far_start(1)
    lax.fori_loop(0, CHUNKS, functools.partial(far_only, 1), 0)
    far_end(1)
    pl.semaphore_signal(free_sem, inc=1, device_id={"tp": sib}, device_id_type=MESH)
    pl.semaphore_wait(free_sem, 1)
    for j in range(7):
        x_again(j).wait()
    own_unit(2)
    for b in range(2):
        to_far[b].wait_send()
        to_sib[b].wait_send()
        onward[b].wait_send()

        def drain(n, carry):
            over_link(b, n).wait_send()
            return carry

        lax.fori_loop((4, 0)[b], CHUNKS, drain, 0)
    put_c.wait()
    put_k.wait()


def main_call(lengths, *arrays):
    vmem = pl.BlockSpec(memory_space=pltpu.VMEM)
    hbm = pl.BlockSpec(memory_space=pl.ANY)
    dma = pltpu.SemaphoreType.DMA
    return pl.pallas_call(
        main_kernel,
        in_specs=[pl.BlockSpec(memory_space=pltpu.SMEM)] + [vmem] * 6 + [hbm] * 8,
        out_specs=[hbm] * 3,
        out_shape=[
            jax.ShapeDtypeStruct((HD, 7168), BF16),
            jax.ShapeDtypeStruct((2, NEW, KVR), BF16),
            jax.ShapeDtypeStruct((2, LOC, NEW), BF16),
        ],
        scratch_shapes=[
            pltpu.VMEM((2, LOC, LAT_W), BF16),
            pltpu.VMEM((HD, QR), F32),
            pltpu.VMEM((HD, 576), F32),
            pltpu.VMEM((2, 3, LOC, LAT_W), BF16),
            pltpu.VMEM((QR, NEW), BF16),
            pltpu.VMEM((2, NEW, KVR), BF16),
            pltpu.VMEM((NEW, HD), BF16),
            pltpu.VMEM((2, LOC, NEW), BF16),
            pltpu.VMEM((PREFIX + NEW, HD), BF16),
            pltpu.VMEM((PREFIX, KVR), BF16),
            pltpu.VMEM((PREFIX + NEW, WID), BF16),
            pltpu.VMEM((WID, PREFIX + NEW), BF16),
            pltpu.VMEM((KVR, WID), BF16),
            pltpu.VMEM((WID, KVR), BF16),
            pltpu.VMEM((3, 2, 192, QR), BF16),
            pltpu.VMEM((16, NEW, NEW), BF16),
            pltpu.VMEM((2, NEW, NEW), BF16),
            *[pltpu.VMEM((PREFIX + NEW, NEW), F32)] * 2,
            pltpu.VMEM((2, 8, NEW), F32),
            pltpu.VMEM((2, NEW, WID), BF16),
            pltpu.VMEM((NEW, WID), BF16),
            pltpu.VMEM((3, WID, CHUNK), BF16),
            pltpu.VMEM((4, 2, LOC, CHUNK), F32),
            *[pltpu.VMEM((2, CHUNKS, LOC, CHUNK), F32)] * 3,
            pltpu.VMEM((4, HD, CHUNK), BF16),
            *[dma((2, 3))] * 2,
            *[dma((4,))] * 2,
            dma,
            dma((4,)),
            dma((8,)),
            dma((4,)),
            dma((3,)),
            dma((7,)),
            dma((2,)),
            dma((4,)),
            dma((4,)),
            *[dma((2, CHUNKS))] * 3,
            pltpu.SemaphoreType.REGULAR,
        ],
        compiler_params=pltpu.CompilerParams(vmem_limit_bytes=VMEM_ALL, collective_id=0, has_side_effects=True),
        cost_estimate=cost(1e11, 200 * MIB),
        name="main",
    )(lengths, *arrays)


def solution(mesh):
    def local_step(hidden, lengths, rope_cos, rope_sin, cache_lat, cache_pe, norm_in, w_dq, norm_q, w_dkv, norm_kv, w_uq, w_uk, w_uv, w_out):
        pe_t = jnp.swapaxes(cache_pe, 1, 2)
        y, c_new, k_newt = main_call(
            lengths,
            jnp.swapaxes(rope_cos, 1, 2),
            jnp.swapaxes(rope_sin, 1, 2),
            pe_t,
            norm_in[None],
            norm_q,
            norm_kv[None],
            hidden.reshape(HD, 7168),
            w_dq,
            w_dkv.T,
            cache_lat,
            w_uk.reshape(8192, HD),
            w_uv.reshape(8192, HD),
            jnp.transpose(w_uq, (1, 2, 0)),
            w_out,
        )
        y, lat_new, pe_new = update_caches(lengths, y, cache_lat, pe_t, c_new, k_newt)
        return y.reshape(hidden.shape), lat_new, jnp.swapaxes(pe_new, 1, 2)

    spec_tok = P("dp", "tp", None)
    spec_len = P("dp")
    spec_seq = P("dp", None, None)
    spec_vec = P(None)
    spec_mat = P(None, None)
    spec_head = P(None, "tp", None)
    spec_rows = P("tp", None)
    in_specs = (spec_tok, spec_len, spec_seq, spec_seq, spec_seq, spec_seq, spec_vec, spec_mat, spec_vec, spec_mat, spec_vec, spec_head, spec_head, spec_head, spec_rows)
    return jax.shard_map(local_step, mesh=mesh, in_specs=in_specs, out_specs=(spec_tok, spec_seq, spec_seq), check_vma=False)
```
